128 devices in a mesh: dp: 8 (over z, core), seq: 16 (over x, y).
Axes of the slice: x: 4, y: 4, z: 4, core: 2. Of those that a mesh axis runs over, the one named last changes fastest.
Arguments:
- loaded: bfloat16 [32768, 1024], P(('dp', 'seq')), may hold values from -6 to 6
- plan: int32 [128, 128], replicated, may hold values from 1 to 4, as said below
- segment_ids: int32 [16, 2048], P('dp'), may hold values from 0 to 31, never falling along the last dimension, each value on 1 to 1024 neighbouring positions
- in_weight: bfloat16 [1024, 2048], P('dp'), may hold values from -0.1875 to 0.1875
- out_weight: bfloat16 [1024, 1024], P('dp'), may hold values from -0.1875 to 0.1875
- depth_kernel: bfloat16 [1024, 31], P('dp'), may hold values from -2 to 2
- norm_gains: bfloat16 [1024, 2], P('dp'), may hold values from 0.25 to 1.75
- upstream: bfloat16 [16, 2048, 1024], P('dp', 'seq'), may hold values from -6 to 6
Outputs:
- encoded: bfloat16 [16, 2048, 1024], P('dp', 'seq')
- grad_frames: bfloat16 [16, 2048, 1024], P('dp', 'seq')
- grad_in_weight: float32 [1024, 2048], P('dp')
- grad_out_weight: float32 [1024, 1024], P('dp')
- grad_kernel: float32 [1024, 31], P('dp')
- grad_gains: float32 [1024, 2], P('dp')
The draws below stay inside these ranges and needn't reach their ends.
Inputs may be any that keep to these rules, and one draw needn't show every extreme that they name: Every row and every column of plan sums to 256; every row reaches 4.
All inputs are finite; a program needn't handle non-finite values.
Results may differ from the reference program's by a relative error of at most 0.006.
Values may be sent and summed in bfloat16 or wider, within the bound.
No kernel may reach another device: no remote copies, remote signals or barrier semaphores. Data moves between devices by JAX's collectives and lax.ppermute only.
A program may use at most 128 MiB of HBM per device.

```python
import math
import jax
import jax.numpy as jnp
import numpy as np
from jax import lax

D = 1024
KERNEL = 31
SLAB_DEV = 128
SLABS = 2
SLAB = 2048
SLABS_ALL = 16
ROWS_DEV = 256
FRAMES_ALL = 32768
N_DP = 8
N_SEQ = 16
DEVICES = 128


def one_hot_rows(targets, count):
    columns = jnp.arange(count, dtype=jnp.int32)
    return (columns[None, :] == targets[:, None]).astype(jnp.int32)


def draw_plan(key, part):
    key_order = jax.random.fold_in(key, 11)
    key_near = jax.random.fold_in(key, 12)
    key_far = jax.random.fold_in(key, 13)
    ordering = jax.random.permutation(key_order, DEVICES).astype(jnp.int32)
    near_shift = jax.random.randint(key_near, (), 1, DEVICES // 2, dtype=jnp.int32)
    far_shift = jax.random.randint(key_far, (), DEVICES // 2, DEVICES, dtype=jnp.int32)
    sources = jnp.arange(DEVICES, dtype=jnp.int32)
    peak_cols = ordering[sources]
    near_cols = ordering[(sources + near_shift) % DEVICES]
    far_cols = ordering[(sources + far_shift) % DEVICES]
    halfway = ROWS_DEV // DEVICES // 2
    moved = 2 * one_hot_rows(peak_cols, DEVICES) - one_hot_rows(near_cols, DEVICES) - one_hot_rows(far_cols, DEVICES)
    return (2 * halfway + halfway * moved).astype(jnp.int32)


def levels(key, dims, split, least, high):
    level, own = 1.0, jax.random.fold_in(key, 6)
    for axis_at, parts in split:
        steps = jnp.exp(jax.random.uniform(jax.random.fold_in(own, axis_at), (parts,), jnp.float32, least / len(split), high / len(split)))
        level = level * jnp.repeat(steps, dims[axis_at] // parts).reshape([-1 if axis == axis_at else 1 for axis in range(len(dims))])
    return level


def split_up(amount, total, limit, lean):
    weights = [(1 << 20) // math.isqrt(rank ** lean) + 1 for rank in range(2, amount + 1)]
    rest, holding = total - limit - (amount - 1), [1] * (amount - 1)
    while rest > 0:
        free = [i for i in range(amount - 1) if holding[i] < limit]
        pool, left = sum([weights[i] for i in free]), rest
        for i in free:
            extra = min(limit - holding[i], max(1, left * weights[i] // pool), rest)
            holding[i] = holding[i] + extra
            rest = rest - extra
    return np.array([limit] + holding)


def ragged(rng, amount, total, reach, skew):
    if amount == 2:
        one = jax.random.randint(rng, (), max(1, total - reach), min(reach, total - 1) + 1)
        return jnp.stack([one, total - one])
    sizes = jnp.asarray(split_up(amount, total, reach, skew), jnp.int32)
    couples = (amount - 1) // 2
    donor, receiver = sizes[1:1 + 2 * couples:2], sizes[2:2 + 2 * couples:2]
    room = jnp.minimum(donor - 1, reach - receiver)
    shifted = jax.random.randint(jax.random.fold_in(rng, 1), (couples,), 0, 1 << 20) % (room + 1)
    sizes = sizes.at[1:1 + 2 * couples:2].set(donor - shifted).at[2:2 + 2 * couples:2].set(receiver + shifted)
    return sizes[jax.random.permutation(jax.random.fold_in(rng, 2), amount)]


def gaussian(stream_key, extent, deviation, bound, shards=(), kind=jnp.bfloat16):
    entries = jax.random.normal(stream_key, extent, jnp.float32) * deviation
    if len(shards) > 0:
        entries = levels(stream_key, extent, shards, -0.22, 0.18) * entries
    return jnp.clip(entries, min=-bound, max=bound).astype(kind)


def setup_inputs(seed: int = 0) -> dict:
    key_list = jax.random.split(jax.random.key(seed), 9)
    return {
        "loaded": gaussian(key_list[0], (DEVICES * ROWS_DEV, D), 1.0, 6.0, ((0, 128),)),
        "plan": draw_plan(jax.random.fold_in(key_list[8], 71), 0),
        "segment_ids": jax.vmap(lambda own: jnp.searchsorted(jnp.cumsum(ragged(own, SLAB // 64, SLAB, SLAB // 2, 2)), jnp.arange(SLAB), side="right"))(jax.random.split(key_list[2], SLABS_ALL)).reshape((SLABS_ALL, SLAB)).astype(jnp.int32),
        "in_weight": gaussian(key_list[3], (D, 2 * D), D ** -0.5, 0.1875, ((0, 8),)),
        "out_weight": gaussian(key_list[4], (D, D), D ** -0.5, 0.1875, ((0, 8),)),
        "depth_kernel": gaussian(key_list[5], (D, KERNEL), (KERNEL // 4) ** -0.5, 2.0, ((0, 8),)),
        "norm_gains": jnp.clip(1.0 + 0.15 * jax.random.normal(key_list[6], (D, 2), jnp.float32), 0.25, 1.75).astype(jnp.bfloat16),
        "upstream": gaussian(key_list[7], (SLABS_ALL, SLAB, D), 1.0, 6.0, ((0, 8), (1, 16))),
    }


def norm_rows(values, gain):
    average = lax.optimization_barrier(jnp.mean(values, axis=-1, keepdims=True))
    centered = values - average
    spread = lax.optimization_barrier(jnp.mean(centered * centered, axis=-1, keepdims=True))
    return centered * lax.rsqrt(spread + 1e-05) * gain

def mid_section(values, gain):
    normed = norm_rows(values, gain)
    return normed * jax.nn.sigmoid(normed)

def repack(loaded, plan):
    send_end = jnp.cumsum(plan, axis=1).astype(jnp.int32)
    send_start = (send_end - plan).astype(jnp.int32)
    recv_start = (jnp.cumsum(plan, axis=0) - plan).astype(jnp.int32)
    row_index = jnp.arange(ROWS_DEV, dtype=jnp.int32)
    target_dev = lax.optimization_barrier(jnp.sum((send_end[:, None, :] <= row_index[None, :, None]).astype(jnp.int32), axis=2)).astype(jnp.int32)
    source_dev = jnp.broadcast_to(jnp.arange(DEVICES, dtype=jnp.int32)[:, None], target_dev.shape)
    within = row_index[None, :] - send_start[source_dev, target_dev]
    target = (target_dev * ROWS_DEV + recv_start[source_dev, target_dev] + within).astype(jnp.int32)
    placed = jnp.zeros_like(loaded).at[target.reshape(-1)].set(loaded)
    grid = placed.reshape(N_DP, N_SEQ, SLABS, SLAB_DEV, D)
    return jnp.transpose(grid, (0, 2, 1, 3, 4)).reshape(SLABS_ALL, SLAB, D)

def reference(loaded, plan, segment_ids, in_weight, out_weight, depth_kernel, norm_gains, upstream):
    margin = KERNEL // 2
    frames = repack(loaded, plan)
    frame_rows = frames.reshape(-1, D).astype(jnp.float32)
    gain_pre = norm_gains[:, 0].astype(jnp.float32)
    gain_mid = norm_gains[:, 1].astype(jnp.float32)
    taps = depth_kernel.astype(jnp.float32)
    normed_full, pull_pre = jax.vjp(norm_rows, frame_rows, gain_pre)
    normed = normed_full.astype(jnp.bfloat16)
    hidden = jnp.dot(normed, in_weight, preferred_element_type=jnp.float32)
    gate_lin = hidden[:, :D]
    gate_sig = jax.nn.sigmoid(hidden[:, D:])
    gated = (gate_lin * gate_sig).astype(jnp.bfloat16).reshape(SLABS_ALL, SLAB, D)
    gated_pad = jnp.pad(gated, ((0, 0), (margin, margin), (0, 0)))
    id_pad = jnp.pad(segment_ids, ((0, 0), (margin, margin)), constant_values=-1)
    mixing = jnp.zeros((SLABS_ALL, SLAB, D), jnp.float32)
    for tap_index in range(KERNEL):
        same = (id_pad[:, tap_index:tap_index + SLAB] == segment_ids)[..., None]
        mixing = mixing + jnp.where(same, gated_pad[:, tap_index:tap_index + SLAB].astype(jnp.float32) * taps[:, tap_index], 0.0)
    activated_full, pull_mid = jax.vjp(mid_section, mixing.reshape(-1, D), gain_mid)
    activated = activated_full.astype(jnp.bfloat16)
    projected = jnp.dot(activated, out_weight, preferred_element_type=jnp.float32)
    encoded = (frame_rows + projected).astype(jnp.bfloat16).reshape(SLABS_ALL, SLAB, D)
    upstream_rows = upstream.reshape(-1, D)
    grad_act = jnp.dot(upstream_rows, out_weight.T, preferred_element_type=jnp.float32)
    grad_out_w = jnp.dot(activated.T, upstream_rows, preferred_element_type=jnp.float32)
    grad_mixing, grad_gain_mid = pull_mid(grad_act)
    grad_cells = grad_mixing.reshape(SLABS_ALL, SLAB, D)
    grad_pad = jnp.pad(grad_cells, ((0, 0), (margin, margin), (0, 0)))
    grad_gated = jnp.zeros((SLABS_ALL, SLAB, D), jnp.float32)
    tap_grads = []
    for tap_index in range(KERNEL):
        same = (id_pad[:, tap_index:tap_index + SLAB] == segment_ids)[..., None]
        tap_grads.append(lax.optimization_barrier(jnp.sum(jnp.where(same, grad_cells * gated_pad[:, tap_index:tap_index + SLAB].astype(jnp.float32), 0.0), axis=(0, 1))))
        mirror = 2 * margin - tap_index
        back_same = (id_pad[:, mirror:mirror + SLAB] == segment_ids)[..., None]
        grad_gated = grad_gated + jnp.where(back_same, grad_pad[:, mirror:mirror + SLAB] * taps[:, tap_index], 0.0)
    grad_taps = jnp.stack(tap_grads, axis=1)
    grad_gated = grad_gated.reshape(-1, D)
    grad_hidden = jnp.concatenate([grad_gated * gate_sig, grad_gated * gate_lin * gate_sig * (1.0 - gate_sig)], axis=1).astype(jnp.bfloat16)
    grad_in_w = jnp.dot(normed.T, grad_hidden, preferred_element_type=jnp.float32)
    grad_normed = jnp.dot(grad_hidden, in_weight.T, preferred_element_type=jnp.float32)
    grad_rows, grad_gain_pre = pull_pre(grad_normed)
    grad_frames = (upstream_rows.astype(jnp.float32) + grad_rows).astype(jnp.bfloat16).reshape(SLABS_ALL, SLAB, D)
    grad_gain = jnp.stack([grad_gain_pre, grad_gain_mid], axis=1)
    scale = 1.0 / math.sqrt(FRAMES_ALL)
    return (encoded, grad_frames, grad_in_w * scale, grad_out_w * scale, grad_taps * scale, grad_gain * scale)
```

```python
import math

import jax
import jax.numpy as jnp
from jax import lax
from jax.experimental import pallas as pl
from jax.experimental.pallas import tpu as pltpu
from jax.sharding import Mesh, PartitionSpec as P

DP = ("z", "core")
SEQ = ("x", "y")
ZXY = ("z", "x", "y")
EDGE = 16
LANES = 128
ROWS_STEP = 32
EPS = 1e-05


def forward_kernel(
    gated_ref, low_ref, high_ref, ids_ref, taps_ref, gain_ref, grad_act_ref,
    act_ref, grad_mix_ref, grad_gain_ref, pad_ref, mix_ref,
):
    slabs, frames, width = gated_ref.shape
    blocks = width // LANES
    taps_count = taps_ref.shape[1] - 1
    shift = EDGE - taps_count // 2

    def one_slab(s, total):
        for b in range(blocks):
            cols = slice(b * LANES, (b + 1) * LANES)
            pad_ref[b, 0:EDGE] = low_ref[s, :, cols].astype(jnp.float32)
            pad_ref[b, EDGE : EDGE + frames] = gated_ref[s, :, cols].astype(jnp.float32)
            pad_ref[b, EDGE + frames :] = high_ref[s, :, cols].astype(jnp.float32)

        def conv_step(i, carry):
            row = pl.multiple_of((i // (blocks // 2)) * ROWS_STEP, ROWS_STEP)
            b = (i % (blocks // 2)) * 2
            center = ids_ref[s, pl.ds(row + EDGE, ROWS_STEP)]
            sums = [jnp.zeros((ROWS_STEP, LANES), jnp.float32) for _ in range(2)]
            for k in range(taps_count):
                same = ids_ref[s, pl.ds(row + k + shift, ROWS_STEP)] == center
                for j in range(2):
                    term = pad_ref[b + j, pl.ds(row + k + shift, ROWS_STEP)]
                    sums[j] = sums[j] + jnp.where(same, term, 0.0) * taps_ref[b + j, k : k + 1, :]
            for j in range(2):
                mix_ref[b + j, pl.ds(row, ROWS_STEP)] = sums[j]
            return carry

        lax.fori_loop(0, (frames // ROWS_STEP) * (blocks // 2), conv_step, 0)

        def row_step(i, total):
            row = pl.multiple_of(i * 16, 16)
            out_row = pl.multiple_of(s * frames + i * 16, 16)
            mixing = jnp.concatenate([mix_ref[b, pl.ds(row, 16)] for b in range(blocks)], axis=1)
            grad_act = grad_act_ref[pl.ds(out_row, 16), :]
            gain = gain_ref[0:1, :]
            centered = mixing - jnp.mean(mixing, axis=-1, keepdims=True)
            scale = lax.rsqrt(jnp.mean(centered * centered, axis=-1, keepdims=True) + EPS)
            normed = centered * scale
            value = normed * gain
            sig = jax.nn.sigmoid(value)
            act_ref[pl.ds(out_row, 16), :] = (value * sig).astype(act_ref.dtype)
            grad_value = grad_act * (sig * (1.0 + value * (1.0 - sig)))
            part = grad_value * normed
            total = total + part[0:8] + part[8:16]
            grad_normed = grad_value * gain
            first = jnp.mean(grad_normed, axis=-1, keepdims=True)
            second = jnp.mean(grad_normed * normed, axis=-1, keepdims=True)
            grad_mix_ref[s, pl.ds(row, 16), :] = (
                scale * (grad_normed - first - normed * second)
            ).astype(grad_mix_ref.dtype)
            return total

        return lax.fori_loop(0, frames // 16, row_step, total)

    grad_gain_ref[...] = lax.fori_loop(
        0, slabs, one_slab, jnp.zeros(grad_gain_ref.shape, jnp.float32)
    )


def backward_kernel(
    grad_mix_ref, low_ref, high_ref, gated_ref, ids_ref, taps_ref, hidden_ref,
    grad_hidden_ref, grad_taps_ref, pad_ref, sum_ref,
):
    slabs, frames, width = gated_ref.shape
    blocks = width // LANES
    taps_count = taps_ref.shape[1] - 1
    half = taps_count // 2
    sum_ref[...] = jnp.zeros(sum_ref.shape, jnp.float32)

    def one_slab(s, carry):
        for b in range(blocks):
            cols = slice(b * LANES, (b + 1) * LANES)
            pad_ref[b, 0:EDGE] = low_ref[s, :, cols].astype(jnp.float32)
            pad_ref[b, EDGE : EDGE + frames] = grad_mix_ref[s, :, cols].astype(jnp.float32)
            pad_ref[b, EDGE + frames :] = high_ref[s, :, cols].astype(jnp.float32)

        def conv_step(i, carry):
            row = pl.multiple_of((i // (blocks // 2)) * ROWS_STEP, ROWS_STEP)
            out_row = pl.multiple_of(s * frames + row, ROWS_STEP)
            b = (i % (blocks // 2)) * 2
            center = ids_ref[s, pl.ds(row + EDGE, ROWS_STEP)]
            sums = [jnp.zeros((ROWS_STEP, LANES), jnp.float32) for _ in range(2)]
            cols = [pl.ds(pl.multiple_of((b + j) * LANES, LANES), LANES) for j in range(2)]
            here = [gated_ref[s, pl.ds(row, ROWS_STEP), cols[j]].astype(jnp.float32) for j in range(2)]
            for k in range(taps_count):
                at = row + EDGE + half - k
                same = ids_ref[s, pl.ds(at, ROWS_STEP)] == center
                for j in range(2):
                    term = jnp.where(same, pad_ref[b + j, pl.ds(at, ROWS_STEP)], 0.0)
                    sums[j] = sums[j] + term * taps_ref[b + j, k : k + 1, :]
                    part = term * here[j]
                    sum_ref[b + j, k] = sum_ref[b + j, k] + (
                        (part[0:8] + part[8:16]) + (part[16:24] + part[24:32])
                    )
            for j in range(2):
                lin = hidden_ref[pl.ds(out_row, ROWS_STEP), cols[j]]
                sig = jax.nn.sigmoid(
                    hidden_ref[
                        pl.ds(out_row, ROWS_STEP),
                        pl.ds(pl.multiple_of(width + (b + j) * LANES, LANES), LANES),
                    ]
                )
                grad_lin = sums[j] * sig
                grad_hidden_ref[pl.ds(out_row, ROWS_STEP), cols[j]] = grad_lin.astype(jnp.bfloat16)
                grad_hidden_ref[
                    pl.ds(out_row, ROWS_STEP),
                    pl.ds(pl.multiple_of(width + (b + j) * LANES, LANES), LANES),
                ] = (grad_lin * lin * (1.0 - sig)).astype(jnp.bfloat16)
            return carry

        return lax.fori_loop(0, (frames // ROWS_STEP) * (blocks // 2), conv_step, carry)

    lax.fori_loop(0, slabs, one_slab, 0)
    for b in range(blocks):
        for k in range(taps_count):
            grad_taps_ref[k : k + 1, b * LANES : (b + 1) * LANES] = jnp.sum(
                sum_ref[b, k], axis=0, keepdims=True
            )
        grad_taps_ref[taps_count:, b * LANES : (b + 1) * LANES] = jnp.zeros(
            (grad_taps_ref.shape[0] - taps_count, LANES), jnp.float32
        )


def kernel_call(body, name, outs, scratch, flops, *args):
    moved = sum(a.size * a.dtype.itemsize for a in args)
    return pl.pallas_call(
        body,
        out_shape=outs,
        scratch_shapes=scratch,
        name=name,
        compiler_params=pltpu.CompilerParams(vmem_limit_bytes=48 * 1024 * 1024),
        cost_estimate=pl.CostEstimate(flops=flops, bytes_accessed=moved, transcendentals=0),
    )(*args)


def spread(shard, axes, count):
    return lax.all_to_all(
        jnp.broadcast_to(shard[None], (count, *shard.shape)), axes, 0, 0, tiled=True
    )


def edges(block, count):
    forward = [(i, i + 1) for i in range(count - 1)]
    backward = [(i + 1, i) for i in range(count - 1)]
    low = lax.ppermute(block[:, -EDGE:].astype(jnp.bfloat16), SEQ, forward)
    high = lax.ppermute(block[:, :EDGE].astype(jnp.bfloat16), SEQ, backward)
    return low, high


def norm_rows(values, gain):
    average = jnp.mean(values, axis=-1, keepdims=True)
    centered = values - average
    spread_ = jnp.mean(centered * centered, axis=-1, keepdims=True)
    return centered * lax.rsqrt(spread_ + EPS) * gain


def per_device(
    loaded, plan, segment_ids, in_weight, out_weight, depth_kernel, norm_gains, upstream
):
    rows_dev, width = loaded.shape
    devices = plan.shape[0]
    capacity = 2 * rows_dev // devices
    slabs, slab_len = segment_ids.shape
    n_seq = lax.axis_size(SEQ)
    n_z = lax.axis_size("z")
    frames_dev = slab_len // n_seq
    kernel_len = depth_kernel.shape[1]
    core = lax.axis_index("core")
    sender = lax.axis_index((*DP, *SEQ))
    swap = [(0, 1), (1, 0)]

    extras = jnp.pad(
        jnp.concatenate([depth_kernel, norm_gains], axis=1), ((0, 0), (0, LANES - kernel_len - 2))
    )
    in_full = lax.all_gather(in_weight, DP, axis=0, tiled=True)
    out_full = lax.all_gather(
        jnp.concatenate([out_weight, extras], axis=1), DP, axis=0, tiled=True
    )
    upstream_rows = upstream.reshape(rows_dev, width)
    upstream_other = lax.ppermute(upstream_rows, "core", swap)

    send_plan = lax.dynamic_index_in_dim(plan, sender, 0, keepdims=False)
    send_start = jnp.cumsum(send_plan) - send_plan
    slot_index = jnp.arange(capacity, dtype=jnp.int32)
    source_rows = send_start[:, None] + slot_index[None, :]
    outgoing = jnp.take(
        loaded, jnp.clip(source_rows, 0, rows_dev - 1).reshape(-1), axis=0
    ).reshape(devices, capacity, width)
    arrived = lax.all_to_all(
        outgoing, (*DP, *SEQ), split_axis=0, concat_axis=0, tiled=True
    ).reshape(devices * capacity, width)
    recv_plan = lax.dynamic_index_in_dim(plan, sender, 1, keepdims=False)
    recv_end = jnp.cumsum(recv_plan)
    frame_index = jnp.arange(rows_dev, dtype=jnp.int32)
    before = recv_end[None, :] <= frame_index[:, None]
    source_dev = jnp.sum(before.astype(jnp.int32), axis=1)
    start_of = jnp.sum(jnp.where(before, recv_plan[None, :], 0), axis=1)
    frames = jnp.take(arrived, source_dev * capacity + frame_index - start_of, axis=0)

    id_pad = jnp.pad(segment_ids, ((0, 0), (EDGE, EDGE)), constant_values=-1)
    window = lax.dynamic_slice_in_dim(
        id_pad, lax.axis_index(SEQ) * frames_dev, frames_dev + 2 * EDGE, 1
    )
    ids = jnp.broadcast_to(window[:, :, None], (*window.shape, LANES))

    side = out_full[:, width : width + kernel_len + 2].astype(jnp.float32).T
    gain_pre, gain_mid = side[kernel_len], side[kernel_len + 1]
    taps = jnp.pad(side[:kernel_len], ((0, 1), (0, 0)))
    taps = taps.reshape(kernel_len + 1, width // LANES, LANES).transpose(1, 0, 2)
    out_full = out_full[:, :width]

    frame_rows = frames.astype(jnp.float32)
    normed_full, pull_pre = jax.vjp(norm_rows, frame_rows, gain_pre)
    normed = normed_full.astype(jnp.bfloat16)
    hidden = jnp.dot(normed, in_full, preferred_element_type=jnp.float32)
    gated = (
        (hidden[:, :width] * jax.nn.sigmoid(hidden[:, width:]))
        .astype(jnp.bfloat16)
        .reshape(slabs, frames_dev, width)
    )
    low, high = edges(gated, n_seq)
    grad_act = jnp.dot(upstream_rows, out_full.T, preferred_element_type=jnp.float32)
    elements = rows_dev * width
    blocked = pltpu.VMEM((width // LANES, frames_dev + 2 * EDGE, LANES), jnp.float32)
    activated, grad_mixing, grad_gain_mid = kernel_call(
        forward_kernel,
        "mixing_forward",
        (
            jax.ShapeDtypeStruct((rows_dev, width), jnp.bfloat16),
            jax.ShapeDtypeStruct((slabs, frames_dev, width), jnp.float32),
            jax.ShapeDtypeStruct((8, width), jnp.float32),
        ),
        [blocked, pltpu.VMEM((width // LANES, frames_dev, LANES), jnp.float32)],
        elements * 3 * kernel_len,
        gated, low, high, ids, taps, gain_mid[None], grad_act,
    )
    grad_low, grad_high = edges(grad_mixing, n_seq)

    def for_core(rows, which):
        parts = rows.reshape(rows.shape[0], n_z, 2, LANES)
        return lax.dynamic_index_in_dim(parts, which, 2, keepdims=False).reshape(
            rows.shape[0], n_z * LANES
        )

    normed_other = lax.ppermute(for_core(normed, 1 - core), "core", swap)
    act_other = lax.ppermute(for_core(activated, 1 - core), "core", swap)
    projected = jnp.dot(activated, out_full, preferred_element_type=jnp.float32)
    encoded = (frame_rows + projected).astype(jnp.bfloat16).reshape(slabs, frames_dev, width)

    def weight_part(mine, other, right, right_other):
        left = jnp.concatenate([mine, other], axis=0)
        both = jnp.concatenate([right, right_other], axis=0)
        return lax.dot_general(
            left, both, (((0,), (0,)), ((), ())), preferred_element_type=jnp.float32
        ).astype(jnp.bfloat16)

    def summed(part):
        arrived_parts = lax.all_to_all(
            part.reshape(n_z * n_seq, LANES // n_seq, part.shape[1]), ZXY, 0, 0, tiled=True
        )
        return jnp.sum(arrived_parts.astype(jnp.float32), axis=0)

    scale = 1.0 / math.sqrt(devices * rows_dev)
    out_part = weight_part(for_core(activated, core), act_other, upstream_rows, upstream_other)
    out_sum = summed(out_part)

    grad_hidden, grad_taps = kernel_call(
        backward_kernel,
        "mixing_backward",
        (
            jax.ShapeDtypeStruct((rows_dev, 2 * width), jnp.bfloat16),
            jax.ShapeDtypeStruct((kernel_len + 1, width), jnp.float32),
        ),
        [blocked, pltpu.VMEM((width // LANES, kernel_len, 8, LANES), jnp.float32)],
        elements * 5 * kernel_len,
        grad_mixing, grad_low, grad_high, gated, ids, taps, hidden,
    )
    hidden_other = lax.ppermute(grad_hidden, "core", swap)
    grad_normed = lax.dot_general(
        grad_hidden, in_full, (((1,), (1,)), ((), ())), preferred_element_type=jnp.float32
    )
    grad_rows, grad_gain_pre = pull_pre(grad_normed)
    grad_frames = (
        (upstream_rows.astype(jnp.float32) + grad_rows)
        .astype(jnp.bfloat16)
        .reshape(slabs, frames_dev, width)
    )
    small = jnp.concatenate(
        [grad_taps[:kernel_len], grad_gain_pre[None], jnp.sum(grad_gain_mid, axis=0)[None]], axis=0
    )
    small_other = lax.ppermute(for_core(small, 1 - core), "core", swap)
    small_part = (for_core(small, core) + small_other).T.astype(jnp.bfloat16)
    small_part = jnp.pad(small_part, ((0, 0), (0, LANES - small_part.shape[1])))
    in_part = weight_part(for_core(normed, core), normed_other, grad_hidden, hidden_other)
    in_sum = summed(jnp.concatenate([in_part, small_part], axis=1))
    total = (jnp.concatenate([in_sum, out_sum], axis=1) * scale).astype(jnp.bfloat16)
    final = spread(total, SEQ, n_seq).reshape(LANES, total.shape[1]).astype(jnp.float32)
    return (
        encoded,
        grad_frames,
        final[:, : 2 * width],
        final[:, 2 * width + LANES :],
        final[:, 2 * width : 2 * width + kernel_len],
        final[:, 2 * width + kernel_len : 2 * width + kernel_len + 2],
    )


def solution(mesh):
    n_dp, n_seq = mesh.devices.shape
    side = math.isqrt(n_seq)
    split = Mesh(mesh.devices.reshape(n_dp // 2, 2, side, side), ("z", "core", "x", "y"))
    placed = (
        P((*DP, *SEQ), None),
        P(),
        P(DP, None),
        P(DP, None),
        P(DP, None),
        P(DP, None),
        P(DP, None),
        P(DP, SEQ, None),
    )
    return jax.shard_map(
        per_device,
        mesh=split,
        in_specs=placed,
        out_specs=(
            P(DP, SEQ, None),
            P(DP, SEQ, None),
            P(DP, None),
            P(DP, None),
            P(DP, None),
            P(DP, None),
        ),
        check_vma=False,
    )
```

```python
import math

import jax
import jax.numpy as jnp
from jax import lax
from jax.experimental import pallas as pl
from jax.experimental.pallas import tpu as pltpu
from jax.sharding import Mesh, PartitionSpec as P


DP = ("z", "core")
SEQ = ("x", "y")
ZXY = ("z", "x", "y")
EDGE = 16
LANES = 128
ROWS_STEP = 32
EPS = 1e-05


def forward_kernel(
    gated_ref, low_ref, high_ref, ids_ref, taps_ref, gain_ref,
    act_ref, normed_ref, scale_ref, pad_ref, mix_ref,
):
    slabs, frames, width = gated_ref.shape
    blocks = width // LANES
    taps_count = taps_ref.shape[1] - 1
    shift = EDGE - taps_count // 2

    def one_slab(s, carry):
        for b in range(blocks):
            cols = slice(b * LANES, (b + 1) * LANES)
            pad_ref[b, 0:EDGE] = low_ref[s, :, cols].astype(jnp.float32)
            pad_ref[b, EDGE : EDGE + frames] = gated_ref[s, :, cols].astype(jnp.float32)
            pad_ref[b, EDGE + frames :] = high_ref[s, :, cols].astype(jnp.float32)

        def conv_step(i, carry):
            row = pl.multiple_of((i // (blocks // 2)) * ROWS_STEP, ROWS_STEP)
            b = (i % (blocks // 2)) * 2
            center = ids_ref[s, pl.ds(row + EDGE, ROWS_STEP)]
            sums = [jnp.zeros((ROWS_STEP, LANES), jnp.float32) for _ in range(2)]
            for k in range(taps_count):
                same = ids_ref[s, pl.ds(row + k + shift, ROWS_STEP)] == center
                for j in range(2):
                    term = pad_ref[b + j, pl.ds(row + k + shift, ROWS_STEP)]
                    sums[j] = sums[j] + jnp.where(same, term, 0.0) * taps_ref[b + j, k : k + 1, :]
            for j in range(2):
                mix_ref[b + j, pl.ds(row, ROWS_STEP)] = sums[j]
            return carry

        lax.fori_loop(0, (frames // ROWS_STEP) * (blocks // 2), conv_step, 0)

        def row_step(i, carry):
            row = pl.multiple_of(i * 16, 16)
            out_row = pl.multiple_of(s * frames + i * 16, 16)
            mixing = jnp.concatenate([mix_ref[b, pl.ds(row, 16)] for b in range(blocks)], axis=1)
            centered = mixing - jnp.mean(mixing, axis=-1, keepdims=True)
            scale = lax.rsqrt(jnp.mean(centered * centered, axis=-1, keepdims=True) + EPS)
            normed = centered * scale
            value = normed * gain_ref[0:1, :]
            act_ref[pl.ds(out_row, 16), :] = (value * jax.nn.sigmoid(value)).astype(act_ref.dtype)
            normed_ref[pl.ds(out_row, 16), :] = normed
            scale_ref[pl.ds(out_row, 16), :] = jnp.broadcast_to(scale, (16, LANES))
            return carry

        return lax.fori_loop(0, frames // 16, row_step, carry)

    lax.fori_loop(0, slabs, one_slab, 0)


def middle_kernel(normed_ref, scale_ref, grad_act_ref, gain_ref, grad_mix_ref, grad_gain_ref):
    slabs, frames, _ = grad_mix_ref.shape
    steps = frames // 16

    def row_step(i, total):
        row = pl.multiple_of(i * 16, 16)
        normed = normed_ref[pl.ds(row, 16), :]
        scale = scale_ref[pl.ds(row, 16), 0:1]
        gain = gain_ref[0:1, :]
        value = normed * gain
        sig = jax.nn.sigmoid(value)
        grad_value = grad_act_ref[pl.ds(row, 16), :] * (sig * (1.0 + value * (1.0 - sig)))
        part = grad_value * normed
        total = total + (part[0:8] + part[8:16])
        grad_normed = grad_value * gain
        first = jnp.mean(grad_normed, axis=-1, keepdims=True)
        second = jnp.mean(grad_normed * normed, axis=-1, keepdims=True)
        grad_mix_ref[i // steps, pl.ds(pl.multiple_of((i % steps) * 16, 16), 16), :] = scale * (
            grad_normed - first - normed * second
        )
        return total

    grad_gain_ref[...] = lax.fori_loop(
        0, slabs * steps, row_step, jnp.zeros(grad_gain_ref.shape, jnp.float32)
    )


def backward_kernel(
    grad_mix_ref, low_ref, high_ref, gated_ref, ids_ref, taps_ref, hidden_ref,
    grad_hidden_ref, grad_taps_ref, pad_ref, sum_ref,
):
    slabs, frames, width = gated_ref.shape
    blocks = width // LANES
    taps_count = taps_ref.shape[1] - 1
    half = taps_count // 2
    sum_ref[...] = jnp.zeros(sum_ref.shape, jnp.float32)

    def one_slab(s, carry):
        for b in range(blocks):
            cols = slice(b * LANES, (b + 1) * LANES)
            pad_ref[b, 0:EDGE] = low_ref[s, :, cols].astype(jnp.float32)
            pad_ref[b, EDGE : EDGE + frames] = grad_mix_ref[s, :, cols].astype(jnp.float32)
            pad_ref[b, EDGE + frames :] = high_ref[s, :, cols].astype(jnp.float32)

        def conv_step(i, carry):
            row = pl.multiple_of((i // (blocks // 2)) * ROWS_STEP, ROWS_STEP)
            out_row = pl.multiple_of(s * frames + row, ROWS_STEP)
            b = (i % (blocks // 2)) * 2
            center = ids_ref[s, pl.ds(row + EDGE, ROWS_STEP)]
            sums = [jnp.zeros((ROWS_STEP, LANES), jnp.float32) for _ in range(2)]
            cols = [pl.ds(pl.multiple_of((b + j) * LANES, LANES), LANES) for j in range(2)]
            here = [gated_ref[s, pl.ds(row, ROWS_STEP), cols[j]].astype(jnp.float32) for j in range(2)]
            for k in range(taps_count):
                at = row + EDGE + half - k
                same = ids_ref[s, pl.ds(at, ROWS_STEP)] == center
                for j in range(2):
                    term = jnp.where(same, pad_ref[b + j, pl.ds(at, ROWS_STEP)], 0.0)
                    sums[j] = sums[j] + term * taps_ref[b + j, k : k + 1, :]
                    part = term * here[j]
                    sum_ref[b + j, k] = sum_ref[b + j, k] + (
                        (part[0:8] + part[8:16]) + (part[16:24] + part[24:32])
                    )
            for j in range(2):
                lin = hidden_ref[pl.ds(out_row, ROWS_STEP), cols[j]]
                sig = jax.nn.sigmoid(
                    hidden_ref[
                        pl.ds(out_row, ROWS_STEP),
                        pl.ds(pl.multiple_of(width + (b + j) * LANES, LANES), LANES),
                    ]
                )
                grad_lin = sums[j] * sig
                grad_hidden_ref[pl.ds(out_row, ROWS_STEP), cols[j]] = grad_lin.astype(jnp.bfloat16)
                grad_hidden_ref[
                    pl.ds(out_row, ROWS_STEP),
                    pl.ds(pl.multiple_of(width + (b + j) * LANES, LANES), LANES),
                ] = (grad_lin * lin * (1.0 - sig)).astype(jnp.bfloat16)
            return carry

        return lax.fori_loop(0, (frames // ROWS_STEP) * (blocks // 2), conv_step, carry)

    lax.fori_loop(0, slabs, one_slab, 0)
    for b in range(blocks):
        for k in range(taps_count):
            grad_taps_ref[k : k + 1, b * LANES : (b + 1) * LANES] = jnp.sum(
                sum_ref[b, k], axis=0, keepdims=True
            )
        grad_taps_ref[taps_count:, b * LANES : (b + 1) * LANES] = jnp.zeros(
            (grad_taps_ref.shape[0] - taps_count, LANES), jnp.float32
        )


def product_kernel(core_ref, left_ref, left_other_ref, right_ref, right_other_ref, *rest):
    out_ref = rest[-1]
    width = right_ref.shape[1]
    step = 512
    left, left_other = left_ref[...], left_other_ref[...]
    over_rows = (((0,), (0,)), ((), ()))
    for at in range(0, width, step):
        out_ref[:, at : at + step] = (
            lax.dot_general(
                left, right_ref[:, at : at + step], over_rows, preferred_element_type=jnp.float32
            )
            + lax.dot_general(
                left_other,
                right_other_ref[:, at : at + step],
                over_rows,
                preferred_element_type=jnp.float32,
            )
        ).astype(out_ref.dtype)
    if len(rest) > 1:
        small = rest[0][...] + rest[1][...]
        filled = jnp.concatenate(
            [small, jnp.zeros((LANES - small.shape[0], LANES), jnp.float32)], axis=0
        )
        out_ref[:, width:] = filled.T.astype(out_ref.dtype)


def weight_part(core, left, left_other, right, right_other, *small):
    rows, channels = left.shape
    mine = channels // LANES // 2
    width = right.shape[1]
    out_width = width + (LANES if small else 0)
    picked = lambda height: pl.BlockSpec((height, LANES), lambda z, c: (0, 2 * z + c[0]))
    whole = lambda a: pl.BlockSpec(a.shape, lambda z, c: (0, 0))
    return pl.pallas_call(
        product_kernel,
        out_shape=jax.ShapeDtypeStruct((mine * LANES, out_width), jnp.bfloat16),
        grid_spec=pltpu.PrefetchScalarGridSpec(
            num_scalar_prefetch=1,
            grid=(mine,),
            in_specs=[picked(rows), picked(rows), whole(right), whole(right_other)]
            + [picked(a.shape[0]) for a in small],
            out_specs=pl.BlockSpec((LANES, out_width), lambda z, c: (z, 0)),
        ),
        name="weight_part",
        compiler_params=pltpu.CompilerParams(vmem_limit_bytes=48 * 1024 * 1024),
        cost_estimate=pl.CostEstimate(
            flops=4 * rows * mine * LANES * width,
            bytes_accessed=4 * rows * (channels + width),
            transcendentals=0,
        ),
    )(core, left, left_other, right, right_other, *small)


def kernel_call(body, outs, scratch, flops, *args):
    moved = sum(a.size * a.dtype.itemsize for a in args)
    return pl.pallas_call(
        body,
        out_shape=outs,
        scratch_shapes=scratch,
        compiler_params=pltpu.CompilerParams(vmem_limit_bytes=48 * 1024 * 1024),
        cost_estimate=pl.CostEstimate(flops=flops, bytes_accessed=moved, transcendentals=0),
    )(*args)


def spread(shard, axes, count):
    return lax.all_to_all(
        jnp.broadcast_to(shard[None], (count, *shard.shape)), axes, 0, 0, tiled=True
    )


def edges(block, count):
    forward = [(i, i + 1) for i in range(count - 1)]
    backward = [(i + 1, i) for i in range(count - 1)]
    low = lax.ppermute(block[:, -EDGE:].astype(jnp.bfloat16), SEQ, forward)
    high = lax.ppermute(block[:, :EDGE].astype(jnp.bfloat16), SEQ, backward)
    return low, high


def norm_rows(values, gain):
    average = jnp.mean(values, axis=-1, keepdims=True)
    centered = values - average
    spread_ = jnp.mean(centered * centered, axis=-1, keepdims=True)
    return centered * lax.rsqrt(spread_ + EPS) * gain


def per_device(
    loaded, plan, segment_ids, in_weight, out_weight, depth_kernel, norm_gains, upstream
):
    rows_dev, width = loaded.shape
    devices = plan.shape[0]
    capacity = 2 * rows_dev // devices
    slabs, slab_len = segment_ids.shape
    n_seq = lax.axis_size(SEQ)
    n_z = lax.axis_size("z")
    frames_dev = slab_len // n_seq
    kernel_len = depth_kernel.shape[1]
    core = lax.axis_index("core")
    sender = lax.axis_index((*DP, *SEQ))
    swap = [(0, 1), (1, 0)]

    extras = jnp.pad(
        jnp.concatenate([depth_kernel, norm_gains], axis=1), ((0, 0), (0, LANES - kernel_len - 2))
    )
    in_all = lax.all_gather(jnp.concatenate([in_weight, extras], axis=1), DP, axis=0, tiled=True)
    out_full = lax.all_gather(out_weight, DP, axis=0, tiled=True)
    in_full = in_all[:, : 2 * width]

    send_plan = lax.dynamic_index_in_dim(plan, sender, 0, keepdims=False)
    send_start = jnp.cumsum(send_plan) - send_plan
    slot_index = jnp.arange(capacity, dtype=jnp.int32)
    source_rows = jnp.minimum(send_start[:, None] + slot_index[None, :], rows_dev - 1)
    outgoing = (
        loaded.at[source_rows.reshape(-1)]
        .get(mode="promise_in_bounds")
        .reshape(devices, capacity, width)
    )
    arrived = lax.all_to_all(
        outgoing, (*DP, *SEQ), split_axis=0, concat_axis=0, tiled=True
    ).reshape(devices * capacity, width)
    recv_plan = lax.dynamic_index_in_dim(plan, sender, 1, keepdims=False)
    recv_end = jnp.cumsum(recv_plan)
    frame_index = jnp.arange(rows_dev, dtype=jnp.int32)
    before = recv_end[None, :] <= frame_index[:, None]
    source_dev = jnp.sum(before.astype(jnp.int32), axis=1)
    start_of = jnp.sum(jnp.where(before, recv_plan[None, :], 0), axis=1)
    frames = arrived.at[source_dev * capacity + frame_index - start_of].get(
        mode="promise_in_bounds"
    )
    upstream_rows = upstream.reshape(rows_dev, width)
    upstream_other = lax.ppermute(upstream_rows, "core", swap)

    id_pad = jnp.pad(segment_ids, ((0, 0), (EDGE, EDGE)), constant_values=-1)
    window = lax.dynamic_slice_in_dim(
        id_pad, lax.axis_index(SEQ) * frames_dev, frames_dev + 2 * EDGE, 1
    )
    ids = jnp.broadcast_to(window[:, :, None], (*window.shape, LANES))

    side = in_all[:, 2 * width : 2 * width + kernel_len + 2].astype(jnp.float32).T
    gain_pre, gain_mid = side[kernel_len], side[kernel_len + 1]
    taps = jnp.pad(side[:kernel_len], ((0, 1), (0, 0)))
    taps = taps.reshape(kernel_len + 1, width // LANES, LANES).transpose(1, 0, 2)

    frame_rows = frames.astype(jnp.float32)
    normed_full, pull_pre = jax.vjp(norm_rows, frame_rows, gain_pre)
    normed = normed_full.astype(jnp.bfloat16)
    hidden = jnp.dot(normed, in_full, preferred_element_type=jnp.float32)
    gated = (
        (hidden[:, :width] * jax.nn.sigmoid(hidden[:, width:]))
        .astype(jnp.bfloat16)
        .reshape(slabs, frames_dev, width)
    )
    low, high = edges(gated, n_seq)
    elements = rows_dev * width
    blocked = pltpu.VMEM((width // LANES, frames_dev + 2 * EDGE, LANES), jnp.float32)
    activated, normed_mid, scale_mid = kernel_call(
        forward_kernel,
        (
            jax.ShapeDtypeStruct((rows_dev, width), jnp.bfloat16),
            jax.ShapeDtypeStruct((rows_dev, width), jnp.float32),
            jax.ShapeDtypeStruct((rows_dev, LANES), jnp.float32),
        ),
        [blocked, pltpu.VMEM((width // LANES, frames_dev, LANES), jnp.float32)],
        elements * 3 * kernel_len,
        gated, low, high, ids, taps, gain_mid[None],
    )
    act_other = lax.ppermute(activated, "core", swap)
    normed_other = lax.ppermute(normed, "core", swap)
    grad_act = jnp.dot(upstream_rows, out_full.T, preferred_element_type=jnp.float32)
    grad_mixing, grad_gain_mid = kernel_call(
        middle_kernel,
        (
            jax.ShapeDtypeStruct((slabs, frames_dev, width), jnp.float32),
            jax.ShapeDtypeStruct((8, width), jnp.float32),
        ),
        [],
        elements * 30,
        normed_mid, scale_mid, grad_act, gain_mid[None],
    )
    grad_low, grad_high = edges(grad_mixing, n_seq)

    def summed(part):
        arrived_parts = lax.all_to_all(
            part.reshape(n_z * n_seq, LANES // n_seq, part.shape[1]), ZXY, 0, 0, tiled=True
        )
        return jnp.sum(arrived_parts.astype(jnp.float32), axis=0)

    core_ref = core[None].astype(jnp.int32)
    out_part = weight_part(core_ref, activated, act_other, upstream_rows, upstream_other)
    out_sum = summed(out_part)
    projected = jnp.dot(activated, out_full, preferred_element_type=jnp.float32)
    encoded = (frame_rows + projected).astype(jnp.bfloat16).reshape(slabs, frames_dev, width)

    grad_hidden, grad_taps = kernel_call(
        backward_kernel,
        (
            jax.ShapeDtypeStruct((rows_dev, 2 * width), jnp.bfloat16),
            jax.ShapeDtypeStruct((kernel_len + 1, width), jnp.float32),
        ),
        [blocked, pltpu.VMEM((width // LANES, kernel_len, 8, LANES), jnp.float32)],
        elements * 5 * kernel_len,
        grad_mixing, grad_low, grad_high, gated, ids, taps, hidden,
    )
    hidden_other = lax.ppermute(grad_hidden, "core", swap)
    small = jnp.concatenate(
        [
            grad_taps,
            jnp.sum(grad_gain_mid, axis=0)[None],
            jnp.zeros((7, width), jnp.float32),
        ],
        axis=0,
    )
    small_other = lax.ppermute(small, "core", swap)
    in_part = weight_part(
        core_ref, normed, normed_other, grad_hidden, hidden_other, small, small_other
    )
    in_sum = summed(in_part)
    grad_normed = lax.dot_general(
        grad_hidden, in_full, (((1,), (1,)), ((), ())), preferred_element_type=jnp.float32
    )
    grad_rows, _ = pull_pre(grad_normed)
    grad_frames = (
        (upstream_rows.astype(jnp.float32) + grad_rows)
        .astype(jnp.bfloat16)
        .reshape(slabs, frames_dev, width)
    )
    share = LANES // n_seq
    first = lax.axis_index(SEQ) * share
    own_weight = lax.dynamic_slice_in_dim(in_weight, first, share, 0).astype(jnp.float32)
    own_gain = lax.dynamic_slice_in_dim(norm_gains, first, share, 0)[:, :1].astype(jnp.float32)
    grad_gain_pre = (
        jnp.sum(own_weight * in_sum[:, : 2 * width], axis=1, keepdims=True) / own_gain
    )
    place = jnp.arange(LANES) == kernel_len
    small_sum = jnp.where(place[None], grad_gain_pre, in_sum[:, 2 * width :])
    scale = 1.0 / math.sqrt(devices * rows_dev)
    total = (
        jnp.concatenate([in_sum[:, : 2 * width], small_sum, out_sum], axis=1) * scale
    ).astype(jnp.bfloat16)
    final = spread(total, SEQ, n_seq).reshape(LANES, total.shape[1]).astype(jnp.float32)
    return (
        encoded,
        grad_frames,
        final[:, : 2 * width],
        final[:, 2 * width + LANES :],
        final[:, 2 * width : 2 * width + kernel_len],
        final[:, 2 * width + kernel_len : 2 * width + kernel_len + 2],
    )


def solution(mesh):
    n_dp, n_seq = mesh.devices.shape
    side = math.isqrt(n_seq)
    split = Mesh(mesh.devices.reshape(n_dp // 2, 2, side, side), ("z", "core", "x", "y"))
    placed = (
        P((*DP, *SEQ), None),
        P(),
        P(DP, None),
        P(DP, None),
        P(DP, None),
        P(DP, None),
        P(DP, None),
        P(DP, SEQ, None),
    )
    return jax.shard_map(
        per_device,
        mesh=split,
        in_specs=placed,
        out_specs=(
            P(DP, SEQ, None),
            P(DP, SEQ, None),
            P(DP, None),
            P(DP, None),
            P(DP, None),
            P(DP, None),
        ),
        check_vma=False,
    )
```

```python
import math

import jax
import jax.numpy as jnp
from jax import lax
from jax.experimental import pallas as pl
from jax.experimental.pallas import tpu as pltpu
from jax.sharding import Mesh, PartitionSpec as P


DP = ("z", "core")
SEQ = ("x", "y")
ZXY = ("z", "x", "y")
EDGE = 16
LANES = 128
ROWS_STEP = 32
EPS = 1e-05


def forward_kernel(
    gated_ref, ids_ref, taps_ref, gain_ref,
    act_ref, normed_ref, scale_ref, pad_ref, mix_ref,
):
    slabs, padded, width = gated_ref.shape
    blocks = width // LANES
    taps_count = taps_ref.shape[1] - 1
    wide = padded - 2 * EDGE
    shift = EDGE - taps_count // 2

    def one_slab(s, carry):
        for b in range(blocks):
            pad_ref[b] = gated_ref[s, :, b * LANES : (b + 1) * LANES].astype(jnp.float32)

        def conv_step(i, carry):
            row = pl.multiple_of((i // (blocks // 2)) * ROWS_STEP, ROWS_STEP)
            b = (i % (blocks // 2)) * 2
            center = ids_ref[s, pl.ds(row + EDGE, ROWS_STEP)]
            sums = [jnp.zeros((ROWS_STEP, LANES), jnp.float32) for _ in range(2)]
            for k in range(taps_count):
                same = ids_ref[s, pl.ds(row + k + shift, ROWS_STEP)] == center
                for j in range(2):
                    term = pad_ref[b + j, pl.ds(row + k + shift, ROWS_STEP)]
                    sums[j] = sums[j] + jnp.where(same, term, 0.0) * taps_ref[b + j, k : k + 1, :]
            for j in range(2):
                mix_ref[b + j, pl.ds(row, ROWS_STEP)] = sums[j]
            return carry

        lax.fori_loop(0, (wide // ROWS_STEP) * (blocks // 2), conv_step, 0)

        def row_step(i, carry):
            row = pl.multiple_of(i * 16, 16)
            out_row = pl.multiple_of(s * wide + i * 16, 16)
            mixing = jnp.concatenate([mix_ref[b, pl.ds(row, 16)] for b in range(blocks)], axis=1)
            centered = mixing - jnp.mean(mixing, axis=-1, keepdims=True)
            scale = lax.rsqrt(jnp.mean(centered * centered, axis=-1, keepdims=True) + EPS)
            normed = centered * scale
            value = normed * gain_ref[0:1, :]
            act_ref[pl.ds(out_row, 16), :] = (value * jax.nn.sigmoid(value)).astype(act_ref.dtype)
            normed_ref[pl.ds(out_row, 16), :] = normed
            scale_ref[pl.ds(out_row, 16), :] = jnp.broadcast_to(scale, (16, LANES))
            return carry

        return lax.fori_loop(0, wide // 16, row_step, carry)

    lax.fori_loop(0, slabs, one_slab, 0)


def middle_kernel(normed_ref, scale_ref, grad_act_ref, gain_ref, grad_mix_ref, grad_gain_ref):
    slabs, frames, _ = grad_mix_ref.shape
    steps = frames // 16

    def row_step(i, total):
        row = pl.multiple_of(i * 16, 16)
        normed = normed_ref[pl.ds(row, 16), :]
        scale = scale_ref[pl.ds(row, 16), 0:1]
        gain = gain_ref[0:1, :]
        value = normed * gain
        sig = jax.nn.sigmoid(value)
        grad_value = grad_act_ref[pl.ds(row, 16), :] * (sig * (1.0 + value * (1.0 - sig)))
        part = grad_value * normed
        at = i % steps
        own = jnp.logical_and(at > 0, at < steps - 1)
        total = total + jnp.where(own, part[0:8] + part[8:16], 0.0)
        grad_normed = grad_value * gain
        first = jnp.mean(grad_normed, axis=-1, keepdims=True)
        second = jnp.mean(grad_normed * normed, axis=-1, keepdims=True)
        grad_mix_ref[i // steps, pl.ds(pl.multiple_of((i % steps) * 16, 16), 16), :] = scale * (
            grad_normed - first - normed * second
        )
        return total

    grad_gain_ref[...] = lax.fori_loop(
        0, slabs * steps, row_step, jnp.zeros(grad_gain_ref.shape, jnp.float32)
    )


def backward_kernel(
    grad_mix_ref, gated_ref, ids_ref, taps_ref, hidden_ref,
    grad_hidden_ref, grad_taps_ref, pad_ref, sum_ref,
):
    slabs, padded, width = gated_ref.shape
    frames = padded - 4 * EDGE
    blocks = width // LANES
    taps_count = taps_ref.shape[1] - 1
    half = taps_count // 2
    sum_ref[...] = jnp.zeros(sum_ref.shape, jnp.float32)

    def one_slab(s, carry):
        for b in range(blocks):
            pad_ref[b] = grad_mix_ref[s, :, b * LANES : (b + 1) * LANES]

        def conv_step(i, carry):
            row = pl.multiple_of((i // (blocks // 2)) * ROWS_STEP, ROWS_STEP)
            out_row = pl.multiple_of(s * frames + row, ROWS_STEP)
            b = (i % (blocks // 2)) * 2
            hid_row = pl.multiple_of(s * padded + 2 * EDGE + row, ROWS_STEP)
            center = ids_ref[s, pl.ds(row + 2 * EDGE, ROWS_STEP)]
            sums = [jnp.zeros((ROWS_STEP, LANES), jnp.float32) for _ in range(2)]
            cols = [pl.ds(pl.multiple_of((b + j) * LANES, LANES), LANES) for j in range(2)]
            here = [gated_ref[s, pl.ds(row + 2 * EDGE, ROWS_STEP), cols[j]].astype(jnp.float32) for j in range(2)]
            for k in range(taps_count):
                at = row + EDGE + half - k
                same = ids_ref[s, pl.ds(at + EDGE, ROWS_STEP)] == center
                for j in range(2):
                    term = jnp.where(same, pad_ref[b + j, pl.ds(at, ROWS_STEP)], 0.0)
                    sums[j] = sums[j] + term * taps_ref[b + j, k : k + 1, :]
                    part = term * here[j]
                    sum_ref[b + j, k] = sum_ref[b + j, k] + (
                        (part[0:8] + part[8:16]) + (part[16:24] + part[24:32])
                    )
            for j in range(2):
                lin = hidden_ref[pl.ds(hid_row, ROWS_STEP), cols[j]]
                sig = jax.nn.sigmoid(
                    hidden_ref[
                        pl.ds(hid_row, ROWS_STEP),
                        pl.ds(pl.multiple_of(width + (b + j) * LANES, LANES), LANES),
                    ]
                )
                grad_lin = sums[j] * sig
                grad_hidden_ref[pl.ds(out_row, ROWS_STEP), cols[j]] = grad_lin.astype(jnp.bfloat16)
                grad_hidden_ref[
                    pl.ds(out_row, ROWS_STEP),
                    pl.ds(pl.multiple_of(width + (b + j) * LANES, LANES), LANES),
                ] = (grad_lin * lin * (1.0 - sig)).astype(jnp.bfloat16)
            return carry

        return lax.fori_loop(0, (frames // ROWS_STEP) * (blocks // 2), conv_step, carry)

    lax.fori_loop(0, slabs, one_slab, 0)
    for b in range(blocks):
        for k in range(taps_count):
            grad_taps_ref[k : k + 1, b * LANES : (b + 1) * LANES] = jnp.sum(
                sum_ref[b, k], axis=0, keepdims=True
            )
        grad_taps_ref[taps_count:, b * LANES : (b + 1) * LANES] = jnp.zeros(
            (grad_taps_ref.shape[0] - taps_count, LANES), jnp.float32
        )


def send_kernel(index_ref, rows_ref, out_ref):
    rows, width = rows_ref.shape
    pick = (lax.broadcasted_iota(jnp.int32, (index_ref.shape[0], rows), 1) == index_ref[...])
    pick = pick.astype(jnp.float32).astype(jnp.bfloat16)
    for h in range(2):
        part = jnp.dot(
            pick,
            rows_ref[:, h * (width // 2) : (h + 1) * (width // 2)],
            preferred_element_type=jnp.float32,
        )
        slots = part.shape[0] // out_ref.shape[0]
        out_ref[:, h * slots : (h + 1) * slots, :] = part.astype(jnp.bfloat16).reshape(
            out_ref.shape[0], slots, width // 2
        )


def receive_kernel(index_ref, arrived_ref, out_ref):
    slots, half = arrived_ref.shape
    columns = lax.broadcasted_iota(jnp.int32, (index_ref.shape[0], slots), 1)
    for h in range(2):
        pick = (columns == index_ref[:, h : h + 1]).astype(jnp.float32).astype(jnp.bfloat16)
        out_ref[:, h * half : (h + 1) * half] = jnp.dot(
            pick, arrived_ref[...], preferred_element_type=jnp.float32
        ).astype(jnp.bfloat16)


def finish_kernel(final_ref, grad_in_ref, grad_out_ref, grad_taps_ref, grad_gains_ref):
    in_width, taps_count = grad_in_ref.shape[1], grad_taps_ref.shape[0]
    grad_in_ref[...] = final_ref[:, :in_width].astype(jnp.float32)
    grad_out_ref[...] = final_ref[:, in_width + LANES :].astype(jnp.float32)
    small = final_ref[:, in_width : in_width + LANES].astype(jnp.float32).T
    grad_taps_ref[...] = small[:taps_count]
    grad_gains_ref[...] = small[taps_count : taps_count + 2]


def product_kernel(core_ref, left_ref, left_other_ref, right_ref, right_other_ref, *rest):
    out_ref = rest[-1]
    width = right_ref.shape[1]
    step = 512
    left, left_other = left_ref[...], left_other_ref[...]
    over_rows = (((0,), (0,)), ((), ()))
    for at in range(0, width, step):
        out_ref[:, at : at + step] = (
            lax.dot_general(
                left, right_ref[:, at : at + step], over_rows, preferred_element_type=jnp.float32
            )
            + lax.dot_general(
                left_other,
                right_other_ref[:, at : at + step],
                over_rows,
                preferred_element_type=jnp.float32,
            )
        ).astype(out_ref.dtype)
    if len(rest) > 1:
        small = rest[0][...] + rest[1][...]
        filled = jnp.concatenate(
            [small, jnp.zeros((LANES - small.shape[0], LANES), jnp.float32)], axis=0
        )
        out_ref[:, width:] = filled.T.astype(out_ref.dtype)


def weight_part(core, left, left_other, right, right_other, *small):
    rows, channels = left.shape
    mine = channels // LANES // 2
    width = right.shape[1]
    out_width = width + (LANES if small else 0)
    picked = lambda height: pl.BlockSpec((height, LANES), lambda z, c: (0, 2 * z + c[0]))
    whole = lambda a: pl.BlockSpec(a.shape, lambda z, c: (0, 0))
    return pl.pallas_call(
        product_kernel,
        out_shape=jax.ShapeDtypeStruct((mine * LANES, out_width), jnp.bfloat16),
        grid_spec=pltpu.PrefetchScalarGridSpec(
            num_scalar_prefetch=1,
            grid=(mine,),
            in_specs=[picked(rows), picked(rows), whole(right), whole(right_other)]
            + [picked(a.shape[0]) for a in small],
            out_specs=pl.BlockSpec((LANES, out_width), lambda z, c: (z, 0)),
        ),
        name="weight_part",
        compiler_params=pltpu.CompilerParams(vmem_limit_bytes=48 * 1024 * 1024),
        cost_estimate=pl.CostEstimate(
            flops=4 * rows * mine * LANES * width,
            bytes_accessed=4 * rows * (channels + width),
            transcendentals=0,
        ),
    )(core, left, left_other, right, right_other, *small)


def kernel_call(body, outs, scratch, flops, *args):
    moved = sum(a.size * a.dtype.itemsize for a in args)
    return pl.pallas_call(
        body,
        out_shape=outs,
        scratch_shapes=scratch,
        compiler_params=pltpu.CompilerParams(vmem_limit_bytes=48 * 1024 * 1024),
        cost_estimate=pl.CostEstimate(flops=flops, bytes_accessed=moved, transcendentals=0),
    )(*args)


def spread(shard, axes, count):
    return lax.all_to_all(
        jnp.broadcast_to(shard[None], (count, *shard.shape)), axes, 0, 0, tiled=True
    )


def edges(block, count, reach):
    forward = [(i, i + 1) for i in range(count - 1)]
    backward = [(i + 1, i) for i in range(count - 1)]
    low = lax.ppermute(block[:, -reach:], SEQ, forward)
    high = lax.ppermute(block[:, :reach], SEQ, backward)
    return low, high


def norm_rows(values, gain):
    average = jnp.mean(values, axis=-1, keepdims=True)
    centered = values - average
    spread_ = jnp.mean(centered * centered, axis=-1, keepdims=True)
    return centered * lax.rsqrt(spread_ + EPS) * gain


def per_device(
    loaded, plan, segment_ids, in_weight, out_weight, depth_kernel, norm_gains, upstream
):
    rows_dev, width = loaded.shape
    devices = plan.shape[0]
    capacity = 2 * rows_dev // devices
    slabs, slab_len = segment_ids.shape
    n_seq = lax.axis_size(SEQ)
    n_z = lax.axis_size("z")
    frames_dev = slab_len // n_seq
    kernel_len = depth_kernel.shape[1]
    core = lax.axis_index("core")
    sender = lax.axis_index((*DP, *SEQ))
    swap = [(0, 1), (1, 0)]

    in_full = lax.all_gather(in_weight, DP, axis=0, tiled=True)
    out_full = lax.all_gather(out_weight, DP, axis=0, tiled=True)

    send_plan = lax.dynamic_index_in_dim(plan, sender, 0, keepdims=False)
    send_start = jnp.cumsum(send_plan) - send_plan
    slot_index = jnp.arange(capacity, dtype=jnp.int32)
    source_rows = jnp.minimum(send_start[:, None] + slot_index[None, :], rows_dev - 1)
    outgoing = kernel_call(
        send_kernel,
        jax.ShapeDtypeStruct((devices, 2 * capacity, width // 2), jnp.bfloat16),
        [],
        4 * devices * capacity * rows_dev * width,
        source_rows.reshape(-1, 1), loaded,
    )
    arrived = lax.all_to_all(
        outgoing, (*DP, *SEQ), split_axis=0, concat_axis=0, tiled=True
    ).reshape(devices * 2 * capacity, width // 2)
    recv_plan = lax.dynamic_index_in_dim(plan, sender, 1, keepdims=False)
    recv_end = jnp.cumsum(recv_plan)
    frame_index = jnp.arange(rows_dev, dtype=jnp.int32)
    before = recv_end[None, :] <= frame_index[:, None]
    source_dev = jnp.sum(before.astype(jnp.int32), axis=1)
    start_of = jnp.sum(jnp.where(before, recv_plan[None, :], 0), axis=1)
    place = source_dev * 2 * capacity + frame_index - start_of
    frames = kernel_call(
        receive_kernel,
        jax.ShapeDtypeStruct((rows_dev, width), jnp.bfloat16),
        [],
        4 * devices * capacity * rows_dev * width,
        jnp.stack([place, place + capacity], axis=1), arrived,
    )
    extras = jnp.pad(
        jnp.concatenate([depth_kernel, norm_gains], axis=1), ((0, 0), (0, LANES - kernel_len - 2))
    )
    extras, frames = lax.optimization_barrier((extras, frames))
    low, high = edges(frames.reshape(slabs, frames_dev, width), n_seq, 2 * EDGE)
    side_all = spread(extras, DP, n_z * 2)
    side = side_all.reshape(width, LANES)[:, : kernel_len + 2].astype(jnp.float32).T
    gain_pre, gain_mid = side[kernel_len], side[kernel_len + 1]
    taps = jnp.pad(side[:kernel_len], ((0, 1), (0, 0)))
    taps = taps.reshape(kernel_len + 1, width // LANES, LANES).transpose(1, 0, 2)

    upstream_rows = upstream.reshape(rows_dev, width)
    upstream_other = lax.ppermute(upstream_rows, "core", swap)
    up_low, up_high = edges(upstream, n_seq, EDGE)
    upstream_wide = jnp.concatenate([up_low, upstream, up_high], axis=1).reshape(-1, width)

    id_pad = jnp.pad(segment_ids, ((0, 0), (2 * EDGE, 2 * EDGE)), constant_values=-1)
    window = lax.dynamic_slice_in_dim(
        id_pad, lax.axis_index(SEQ) * frames_dev, frames_dev + 4 * EDGE, 1
    )
    ids = jnp.broadcast_to(window[:, :, None], (*window.shape, LANES))

    frame_rows = frames.astype(jnp.float32)
    _, pull_pre = jax.vjp(norm_rows, frame_rows, gain_pre)
    padded = frames_dev + 4 * EDGE
    frames_wide = jnp.concatenate(
        [low, frames.reshape(slabs, frames_dev, width), high], axis=1
    ).reshape(-1, width)
    normed_wide = norm_rows(frames_wide.astype(jnp.float32), gain_pre).astype(jnp.bfloat16)
    hidden = jnp.dot(normed_wide, in_full, preferred_element_type=jnp.float32)
    gated = (
        (hidden[:, :width] * jax.nn.sigmoid(hidden[:, width:]))
        .astype(jnp.bfloat16)
        .reshape(slabs, padded, width)
    )
    normed = normed_wide.reshape(slabs, padded, width)[:, 2 * EDGE : 2 * EDGE + frames_dev]
    normed = normed.reshape(rows_dev, width)
    elements = rows_dev * width
    wide = frames_dev + 2 * EDGE
    blocks = width // LANES
    act_wide, normed_mid, scale_mid = kernel_call(
        forward_kernel,
        (
            jax.ShapeDtypeStruct((slabs * wide, width), jnp.bfloat16),
            jax.ShapeDtypeStruct((slabs * wide, width), jnp.float32),
            jax.ShapeDtypeStruct((slabs * wide, LANES), jnp.float32),
        ),
        [
            pltpu.VMEM((blocks, padded, LANES), jnp.float32),
            pltpu.VMEM((blocks, wide, LANES), jnp.float32),
        ],
        elements * 3 * kernel_len,
        gated, ids, taps, gain_mid[None],
    )
    activated = act_wide.reshape(slabs, wide, width)[:, EDGE : EDGE + frames_dev]
    activated = activated.reshape(rows_dev, width)
    act_other = lax.ppermute(activated, "core", swap)
    normed_other = lax.ppermute(normed, "core", swap)
    grad_act = jnp.dot(upstream_wide, out_full.T, preferred_element_type=jnp.float32)
    grad_mixing, grad_gain_mid = kernel_call(
        middle_kernel,
        (
            jax.ShapeDtypeStruct((slabs, wide, width), jnp.float32),
            jax.ShapeDtypeStruct((8, width), jnp.float32),
        ),
        [],
        elements * 30,
        normed_mid, scale_mid, grad_act, gain_mid[None],
    )

    def summed(part):
        arrived_parts = lax.all_to_all(
            part.reshape(n_z * n_seq, LANES // n_seq, part.shape[1]), ZXY, 0, 0, tiled=True
        )
        return jnp.sum(arrived_parts.astype(jnp.float32), axis=0)

    core_ref = core[None].astype(jnp.int32)
    out_part = weight_part(core_ref, activated, act_other, upstream_rows, upstream_other)
    out_sum = summed(out_part)
    projected = jnp.dot(activated, out_full, preferred_element_type=jnp.float32)
    encoded = (frame_rows + projected).astype(jnp.bfloat16).reshape(slabs, frames_dev, width)

    grad_hidden, grad_taps = kernel_call(
        backward_kernel,
        (
            jax.ShapeDtypeStruct((rows_dev, 2 * width), jnp.bfloat16),
            jax.ShapeDtypeStruct((kernel_len + 1, width), jnp.float32),
        ),
        [
            pltpu.VMEM((blocks, wide, LANES), jnp.float32),
            pltpu.VMEM((blocks, kernel_len, 8, LANES), jnp.float32),
        ],
        elements * 5 * kernel_len,
        grad_mixing, gated, ids, taps, hidden,
    )
    hidden_other = lax.ppermute(grad_hidden, "core", swap)
    small = jnp.concatenate(
        [
            grad_taps,
            jnp.sum(grad_gain_mid, axis=0)[None],
            jnp.zeros((7, width), jnp.float32),
        ],
        axis=0,
    )
    small_other = lax.ppermute(small, "core", swap)
    in_part = weight_part(
        core_ref, normed, normed_other, grad_hidden, hidden_other, small, small_other
    )
    in_sum = summed(in_part)
    grad_normed = lax.dot_general(
        grad_hidden, in_full, (((1,), (1,)), ((), ())), preferred_element_type=jnp.float32
    )
    grad_rows, _ = pull_pre(grad_normed)
    grad_frames = (
        (upstream_rows.astype(jnp.float32) + grad_rows)
        .astype(jnp.bfloat16)
        .reshape(slabs, frames_dev, width)
    )
    share = LANES // n_seq
    first = lax.axis_index(SEQ) * share
    own_weight = lax.dynamic_slice_in_dim(in_weight, first, share, 0).astype(jnp.float32)
    own_gain = lax.dynamic_slice_in_dim(norm_gains, first, share, 0)[:, :1].astype(jnp.float32)
    grad_gain_pre = (
        jnp.sum(own_weight * in_sum[:, : 2 * width], axis=1, keepdims=True) / own_gain
    )
    place = jnp.arange(LANES) == kernel_len
    small_sum = jnp.where(place[None], grad_gain_pre, in_sum[:, 2 * width :])
    scale = 1.0 / math.sqrt(devices * rows_dev)
    total = (
        jnp.concatenate([in_sum[:, : 2 * width], small_sum, out_sum], axis=1) * scale
    ).astype(jnp.bfloat16)
    final = spread(total, SEQ, n_seq).reshape(LANES, total.shape[1])
    grad_in, grad_out, grad_kernel, grad_gains = kernel_call(
        finish_kernel,
        (
            jax.ShapeDtypeStruct((LANES, 2 * width), jnp.float32),
            jax.ShapeDtypeStruct((LANES, width), jnp.float32),
            jax.ShapeDtypeStruct((kernel_len, LANES), jnp.float32),
            jax.ShapeDtypeStruct((2, LANES), jnp.float32),
        ),
        [],
        LANES * width,
        final,
    )
    return encoded, grad_frames, grad_in, grad_out, grad_kernel.T, grad_gains.T


def solution(mesh):
    n_dp, n_seq = mesh.devices.shape
    side = math.isqrt(n_seq)
    split = Mesh(mesh.devices.reshape(n_dp // 2, 2, side, side), ("z", "core", "x", "y"))
    placed = (
        P((*DP, *SEQ), None),
        P(),
        P(DP, None),
        P(DP, None),
        P(DP, None),
        P(DP, None),
        P(DP, None),
        P(DP, SEQ, None),
    )
    return jax.shard_map(
        per_device,
        mesh=split,
        in_specs=placed,
        out_specs=(
            P(DP, SEQ, None),
            P(DP, SEQ, None),
            P(DP, None),
            P(DP, None),
            P(DP, None),
            P(DP, None),
        ),
        check_vma=False,
    )
```

```python
import math

import jax
import jax.numpy as jnp
from jax import lax
from jax.experimental import pallas as pl
from jax.experimental.pallas import tpu as pltpu
from jax.sharding import Mesh, PartitionSpec as P


DP = ("z", "core")
SEQ = ("x", "y")
ZXY = ("z", "x", "y")
EDGE = 16
LANES = 128
ROWS_STEP = 32
EPS = 1e-05


def forward_kernel(
    gated_ref, ids_ref, taps_ref, gain_ref,
    act_ref, normed_ref, scale_ref, pad_ref, mix_ref,
):
    slabs, padded, width = gated_ref.shape
    blocks = width // LANES
    taps_count = taps_ref.shape[1] - 1
    wide = padded - 2 * EDGE
    shift = EDGE - taps_count // 2

    def one_slab(s, carry):
        for b in range(blocks):
            pad_ref[b] = gated_ref[s, :, b * LANES : (b + 1) * LANES].astype(jnp.float32)

        def conv_step(i, carry):
            row = pl.multiple_of((i // (blocks // 2)) * ROWS_STEP, ROWS_STEP)
            b = (i % (blocks // 2)) * 2
            center = ids_ref[s, pl.ds(row + EDGE, ROWS_STEP)]
            sums = [jnp.zeros((ROWS_STEP, LANES), jnp.float32) for _ in range(2)]
            for k in range(taps_count):
                same = ids_ref[s, pl.ds(row + k + shift, ROWS_STEP)] == center
                for j in range(2):
                    term = pad_ref[b + j, pl.ds(row + k + shift, ROWS_STEP)]
                    sums[j] = sums[j] + jnp.where(same, term, 0.0) * taps_ref[b + j, k : k + 1, :]
            for j in range(2):
                mix_ref[b + j, pl.ds(row, ROWS_STEP)] = sums[j]
            return carry

        lax.fori_loop(0, (wide // ROWS_STEP) * (blocks // 2), conv_step, 0)

        def row_step(i, carry):
            row = pl.multiple_of(i * 16, 16)
            out_row = pl.multiple_of(s * wide + i * 16, 16)
            mixing = jnp.concatenate([mix_ref[b, pl.ds(row, 16)] for b in range(blocks)], axis=1)
            centered = mixing - jnp.mean(mixing, axis=-1, keepdims=True)
            scale = lax.rsqrt(jnp.mean(centered * centered, axis=-1, keepdims=True) + EPS)
            normed = centered * scale
            value = normed * gain_ref[0:1, :]
            act_ref[pl.ds(out_row, 16), :] = (value * jax.nn.sigmoid(value)).astype(act_ref.dtype)
            normed_ref[pl.ds(out_row, 16), :] = normed
            scale_ref[pl.ds(out_row, 16), :] = jnp.broadcast_to(scale, (16, LANES))
            return carry

        return lax.fori_loop(0, wide // 16, row_step, carry)

    lax.fori_loop(0, slabs, one_slab, 0)


def middle_kernel(normed_ref, scale_ref, grad_act_ref, gain_ref, grad_mix_ref, grad_gain_ref):
    slabs, frames, _ = grad_mix_ref.shape
    steps = frames // 16

    def row_step(i, total):
        row = pl.multiple_of(i * 16, 16)
        normed = normed_ref[pl.ds(row, 16), :]
        scale = scale_ref[pl.ds(row, 16), 0:1]
        gain = gain_ref[0:1, :]
        value = normed * gain
        sig = jax.nn.sigmoid(value)
        grad_value = grad_act_ref[pl.ds(row, 16), :] * (sig * (1.0 + value * (1.0 - sig)))
        part = grad_value * normed
        at = i % steps
        own = jnp.logical_and(at > 0, at < steps - 1)
        total = total + jnp.where(own, part[0:8] + part[8:16], 0.0)
        grad_normed = grad_value * gain
        first = jnp.mean(grad_normed, axis=-1, keepdims=True)
        second = jnp.mean(grad_normed * normed, axis=-1, keepdims=True)
        grad_mix_ref[i // steps, pl.ds(pl.multiple_of((i % steps) * 16, 16), 16), :] = scale * (
            grad_normed - first - normed * second
        )
        return total

    grad_gain_ref[...] = lax.fori_loop(
        0, slabs * steps, row_step, jnp.zeros(grad_gain_ref.shape, jnp.float32)
    )


def backward_kernel(
    grad_mix_ref, gated_ref, ids_ref, taps_ref, lin_ref, sig_ref,
    grad_hidden_ref, grad_taps_ref, pad_ref, sum_ref,
):
    slabs, padded, width = gated_ref.shape
    frames = padded - 4 * EDGE
    blocks = width // LANES
    taps_count = taps_ref.shape[1] - 1
    half = taps_count // 2
    sum_ref[...] = jnp.zeros(sum_ref.shape, jnp.float32)

    def one_slab(s, carry):
        for b in range(blocks):
            pad_ref[b] = grad_mix_ref[s, :, b * LANES : (b + 1) * LANES]

        def conv_step(i, carry):
            row = pl.multiple_of((i // (blocks // 2)) * ROWS_STEP, ROWS_STEP)
            out_row = pl.multiple_of(s * frames + row, ROWS_STEP)
            b = (i % (blocks // 2)) * 2
            hid_row = pl.multiple_of(s * padded + 2 * EDGE + row, ROWS_STEP)
            center = ids_ref[s, pl.ds(row + 2 * EDGE, ROWS_STEP)]
            sums = [jnp.zeros((ROWS_STEP, LANES), jnp.float32) for _ in range(2)]
            cols = [pl.ds(pl.multiple_of((b + j) * LANES, LANES), LANES) for j in range(2)]
            here = [gated_ref[s, pl.ds(row + 2 * EDGE, ROWS_STEP), cols[j]].astype(jnp.float32) for j in range(2)]
            for k in range(taps_count):
                at = row + EDGE + half - k
                same = ids_ref[s, pl.ds(at + EDGE, ROWS_STEP)] == center
                for j in range(2):
                    term = jnp.where(same, pad_ref[b + j, pl.ds(at, ROWS_STEP)], 0.0)
                    sums[j] = sums[j] + term * taps_ref[b + j, k : k + 1, :]
                    part = term * here[j]
                    sum_ref[b + j, k] = sum_ref[b + j, k] + (
                        (part[0:8] + part[8:16]) + (part[16:24] + part[24:32])
                    )
            for j in range(2):
                lin = lin_ref[pl.ds(hid_row, ROWS_STEP), cols[j]]
                sig = sig_ref[pl.ds(hid_row, ROWS_STEP), cols[j]]
                grad_lin = sums[j] * sig
                grad_hidden_ref[pl.ds(out_row, ROWS_STEP), cols[j]] = grad_lin.astype(jnp.bfloat16)
                grad_hidden_ref[
                    pl.ds(out_row, ROWS_STEP),
                    pl.ds(pl.multiple_of(width + (b + j) * LANES, LANES), LANES),
                ] = (grad_lin * lin * (1.0 - sig)).astype(jnp.bfloat16)
            return carry

        return lax.fori_loop(0, (frames // ROWS_STEP) * (blocks // 2), conv_step, carry)

    lax.fori_loop(0, slabs, one_slab, 0)
    for b in range(blocks):
        for k in range(taps_count):
            grad_taps_ref[k : k + 1, b * LANES : (b + 1) * LANES] = jnp.sum(
                sum_ref[b, k], axis=0, keepdims=True
            )
        grad_taps_ref[taps_count:, b * LANES : (b + 1) * LANES] = jnp.zeros(
            (grad_taps_ref.shape[0] - taps_count, LANES), jnp.float32
        )


def send_kernel(index_ref, rows_ref, out_ref):
    rows, width = rows_ref.shape
    pick = (lax.broadcasted_iota(jnp.int32, (index_ref.shape[0], rows), 1) == index_ref[...])
    pick = pick.astype(jnp.float32).astype(jnp.bfloat16)
    for h in range(2):
        part = jnp.dot(
            pick,
            rows_ref[:, h * (width // 2) : (h + 1) * (width // 2)],
            preferred_element_type=jnp.float32,
        )
        slots = part.shape[0] // out_ref.shape[0]
        out_ref[:, h * slots : (h + 1) * slots, :] = part.astype(jnp.bfloat16).reshape(
            out_ref.shape[0], slots, width // 2
        )


def receive_kernel(index_ref, arrived_ref, out_ref):
    slots, half = arrived_ref.shape
    columns = lax.broadcasted_iota(jnp.int32, (index_ref.shape[0], slots), 1)
    for h in range(2):
        pick = (columns == index_ref[:, h : h + 1]).astype(jnp.float32).astype(jnp.bfloat16)
        out_ref[:, h * half : (h + 1) * half] = jnp.dot(
            pick, arrived_ref[...], preferred_element_type=jnp.float32
        ).astype(jnp.bfloat16)


def finish_kernel(final_ref, grad_in_ref, grad_out_ref, grad_taps_ref, grad_gains_ref):
    in_width, taps_count = grad_in_ref.shape[1], grad_taps_ref.shape[0]
    grad_in_ref[...] = final_ref[:, :in_width].astype(jnp.float32)
    grad_out_ref[...] = final_ref[:, in_width + LANES :].astype(jnp.float32)
    small = final_ref[:, in_width : in_width + LANES].astype(jnp.float32).T
    grad_taps_ref[...] = small[:taps_count]
    grad_gains_ref[...] = small[taps_count : taps_count + 2]


def product_kernel(core_ref, left_ref, left_other_ref, right_ref, right_other_ref, *rest):
    small_refs, out_ref, turned_ref = rest[:-2], rest[-2], rest[-1]
    rows, channels = left_ref.shape
    width = right_ref.shape[1]
    step = 512
    picks = [
        pl.ds(pl.multiple_of((2 * z + core_ref[0]) * LANES, LANES), LANES)
        for z in range(channels // LANES // 2)
    ]
    for z, pick in enumerate(picks):
        for h, ref in enumerate((left_ref, left_other_ref)):
            turned_ref[z * LANES : (z + 1) * LANES, h * rows : (h + 1) * rows] = ref[:, pick].T
    for at in range(0, width, step):
        right = jnp.concatenate(
            [right_ref[:, at : at + step], right_other_ref[:, at : at + step]], axis=0
        )
        out_ref[:, at : at + step] = jnp.dot(
            turned_ref[...], right, preferred_element_type=jnp.float32
        ).astype(out_ref.dtype)
    if small_refs:
        for z, pick in enumerate(picks):
            small = small_refs[0][:, pick] + small_refs[1][:, pick]
            filled = jnp.concatenate(
                [small, jnp.zeros((LANES - small.shape[0], LANES), jnp.float32)], axis=0
            )
            block = slice(z * LANES, (z + 1) * LANES)
            out_ref[block, width : width + LANES] = filled.T.astype(out_ref.dtype)


def weight_part(core, left, left_other, right, right_other, *small):
    rows, channels = left.shape
    mine = channels // LANES // 2
    width = right.shape[1]
    out_width = width + (LANES if small else 0)
    vmem = pl.BlockSpec(memory_space=pltpu.VMEM)
    return pl.pallas_call(
        product_kernel,
        out_shape=jax.ShapeDtypeStruct((mine * LANES, out_width), jnp.bfloat16),
        in_specs=[pl.BlockSpec(memory_space=pltpu.SMEM)] + [vmem] * (4 + len(small)),
        out_specs=vmem,
        scratch_shapes=[pltpu.VMEM((mine * LANES, 2 * rows), jnp.bfloat16)],
        name="weight_part",
        compiler_params=pltpu.CompilerParams(vmem_limit_bytes=48 * 1024 * 1024),
        cost_estimate=pl.CostEstimate(
            flops=4 * rows * mine * LANES * width,
            bytes_accessed=4 * rows * (channels + width),
            transcendentals=0,
        ),
    )(core, left, left_other, right, right_other, *small)


def norm_kernel(frames_ref, low_ref, high_ref, gain_ref, wide_ref, own_ref):
    slabs, padded, _ = wide_ref.shape
    reach = low_ref.shape[1]
    own = padded - 2 * reach

    def normed_rows(rows):
        values = rows.astype(jnp.float32)
        centered = values - jnp.mean(values, axis=-1, keepdims=True)
        spread_ = jnp.mean(centered * centered, axis=-1, keepdims=True)
        return (centered * lax.rsqrt(spread_ + EPS) * gain_ref[0:1, :]).astype(jnp.bfloat16)

    for s in range(slabs):
        for at in range(0, reach, 16):
            wide_ref[s, at : at + 16, :] = normed_rows(low_ref[s, at : at + 16, :])
            high_at = reach + own + at
            wide_ref[s, high_at : high_at + 16, :] = normed_rows(high_ref[s, at : at + 16, :])

    def step(i, carry):
        row = pl.multiple_of(i * 16, 16)
        rows = normed_rows(frames_ref[pl.ds(row, 16), :])
        own_ref[pl.ds(row, 16), :] = rows
        steps = own // 16
        wide_ref[i // steps, pl.ds(pl.multiple_of(reach + (i % steps) * 16, 16), 16), :] = rows
        return carry

    lax.fori_loop(0, slabs * own // 16, step, 0, unroll=2)


def project_kernel(normed_ref, lin_w_ref, gate_w_ref, lin_ref, sig_ref, gated_ref):
    lin = jnp.dot(normed_ref[...], lin_w_ref[...], preferred_element_type=jnp.float32)
    gate = jnp.dot(normed_ref[...], gate_w_ref[...], preferred_element_type=jnp.float32)
    sig = jax.nn.sigmoid(gate)
    lin_ref[...] = lin
    sig_ref[...] = sig
    gated_ref[...] = (lin * sig).astype(jnp.bfloat16)


def project(normed, weight):
    rows, width = normed.shape
    cols = 256
    steps = width // cols
    out = pl.BlockSpec((rows, cols), lambda j: (0, j))
    return pl.pallas_call(
        project_kernel,
        out_shape=(
            jax.ShapeDtypeStruct((rows, width), jnp.float32),
            jax.ShapeDtypeStruct((rows, width), jnp.float32),
            jax.ShapeDtypeStruct((rows, width), jnp.bfloat16),
        ),
        grid=(steps,),
        in_specs=[
            pl.BlockSpec((rows, width), lambda j: (0, 0)),
            pl.BlockSpec((width, cols), lambda j: (0, j)),
            pl.BlockSpec((width, cols), lambda j: (0, j + steps)),
        ],
        out_specs=(out, out, out),
        name="project",
        compiler_params=pltpu.CompilerParams(vmem_limit_bytes=48 * 1024 * 1024),
        cost_estimate=pl.CostEstimate(
            flops=4 * rows * width * width,
            bytes_accessed=4 * width * width,
            transcendentals=rows * width,
        ),
    )(normed, weight, weight)


def kernel_call(body, outs, scratch, flops, *args):
    moved = sum(a.size * a.dtype.itemsize for a in args)
    return pl.pallas_call(
        body,
        out_shape=outs,
        scratch_shapes=scratch,
        compiler_params=pltpu.CompilerParams(vmem_limit_bytes=48 * 1024 * 1024),
        cost_estimate=pl.CostEstimate(flops=flops, bytes_accessed=moved, transcendentals=0),
    )(*args)


def spread(shard, axes, count):
    return lax.all_to_all(
        jnp.broadcast_to(shard[None], (count, *shard.shape)), axes, 0, 0, tiled=True
    )


def edges(block, count, reach):
    forward = [(i, i + 1) for i in range(count - 1)]
    backward = [(i + 1, i) for i in range(count - 1)]
    low = lax.ppermute(block[:, -reach:], SEQ, forward)
    high = lax.ppermute(block[:, :reach], SEQ, backward)
    return low, high


def norm_rows(values, gain):
    average = jnp.mean(values, axis=-1, keepdims=True)
    centered = values - average
    spread_ = jnp.mean(centered * centered, axis=-1, keepdims=True)
    return centered * lax.rsqrt(spread_ + EPS) * gain


def per_device(
    loaded, plan, segment_ids, in_weight, out_weight, depth_kernel, norm_gains, upstream
):
    rows_dev, width = loaded.shape
    devices = plan.shape[0]
    capacity = 2 * rows_dev // devices
    slabs, slab_len = segment_ids.shape
    n_seq = lax.axis_size(SEQ)
    n_z = lax.axis_size("z")
    frames_dev = slab_len // n_seq
    kernel_len = depth_kernel.shape[1]
    core = lax.axis_index("core")
    sender = lax.axis_index((*DP, *SEQ))
    swap = [(0, 1), (1, 0)]

    in_full = lax.all_gather(in_weight, DP, axis=0, tiled=True)
    out_full = lax.all_gather(out_weight, DP, axis=0, tiled=True)

    send_plan = lax.dynamic_index_in_dim(plan, sender, 0, keepdims=False)
    send_start = jnp.cumsum(send_plan) - send_plan
    slot_index = jnp.arange(capacity, dtype=jnp.int32)
    source_rows = jnp.minimum(send_start[:, None] + slot_index[None, :], rows_dev - 1)
    outgoing = kernel_call(
        send_kernel,
        jax.ShapeDtypeStruct((devices, 2 * capacity, width // 2), jnp.bfloat16),
        [],
        4 * devices * capacity * rows_dev * width,
        source_rows.reshape(-1, 1), loaded,
    )
    arrived = lax.all_to_all(
        outgoing, (*DP, *SEQ), split_axis=0, concat_axis=0, tiled=True
    ).reshape(devices * 2 * capacity, width // 2)
    extras = jnp.pad(
        jnp.concatenate([depth_kernel, norm_gains], axis=1), ((0, 0), (0, LANES - kernel_len - 2))
    )
    upstream_rows = upstream.reshape(rows_dev, width)
    up_low, up_high = edges(upstream, n_seq, EDGE)
    extras_other = lax.ppermute(extras, "core", swap)
    pair = jnp.where(
        core == 0, jnp.stack([extras, extras_other]), jnp.stack([extras_other, extras])
    )
    from_z = [
        lax.ppermute(pair, "z", [(i, (i + d) % n_z) for i in range(n_z)]) for d in range(1, n_z)
    ]
    upstream_other = lax.ppermute(upstream_rows, "core", swap)
    arrived, up_low, up_high, upstream_other, pair, *from_z = lax.optimization_barrier(
        (arrived, up_low, up_high, upstream_other, pair, *from_z)
    )
    by_z = jnp.stack([*from_z[::-1], pair])
    side_all = lax.dynamic_slice_in_dim(
        jnp.concatenate([by_z, by_z]), n_z - 1 - lax.axis_index("z"), n_z, 0
    )
    recv_plan = lax.dynamic_index_in_dim(plan, sender, 1, keepdims=False)
    recv_end = jnp.cumsum(recv_plan)
    frame_index = jnp.arange(rows_dev, dtype=jnp.int32)
    before = recv_end[None, :] <= frame_index[:, None]
    source_dev = jnp.sum(before.astype(jnp.int32), axis=1)
    start_of = jnp.sum(jnp.where(before, recv_plan[None, :], 0), axis=1)
    place = source_dev * 2 * capacity + frame_index - start_of
    frames = kernel_call(
        receive_kernel,
        jax.ShapeDtypeStruct((rows_dev, width), jnp.bfloat16),
        [],
        4 * devices * capacity * rows_dev * width,
        jnp.stack([place, place + capacity], axis=1), arrived,
    )
    low, high = edges(frames.reshape(slabs, frames_dev, width), n_seq, 2 * EDGE)
    side = side_all.reshape(width, LANES)[:, : kernel_len + 2].astype(jnp.float32).T
    gain_pre, gain_mid = side[kernel_len], side[kernel_len + 1]
    taps = jnp.pad(side[:kernel_len], ((0, 1), (0, 0)))
    taps = taps.reshape(kernel_len + 1, width // LANES, LANES).transpose(1, 0, 2)

    upstream_wide = jnp.concatenate([up_low, upstream, up_high], axis=1).reshape(-1, width)

    id_pad = jnp.pad(segment_ids, ((0, 0), (2 * EDGE, 2 * EDGE)), constant_values=-1)
    window = lax.dynamic_slice_in_dim(
        id_pad, lax.axis_index(SEQ) * frames_dev, frames_dev + 4 * EDGE, 1
    )
    ids = jnp.broadcast_to(window[:, :, None], (*window.shape, LANES))

    frame_rows = frames.astype(jnp.float32)
    _, pull_pre = jax.vjp(norm_rows, frame_rows, gain_pre)
    padded = frames_dev + 4 * EDGE
    normed_wide, normed = kernel_call(
        norm_kernel,
        (
            jax.ShapeDtypeStruct((slabs, padded, width), jnp.bfloat16),
            jax.ShapeDtypeStruct((rows_dev, width), jnp.bfloat16),
        ),
        [],
        rows_dev * width * 10,
        frames, low, high, gain_pre[None],
    )
    normed_other = lax.ppermute(normed, "core", swap)
    in_full, normed_other = lax.optimization_barrier((in_full, normed_other))
    lin, sig, gated = project(normed_wide.reshape(-1, width), in_full)
    gated = gated.reshape(slabs, padded, width)
    elements = rows_dev * width
    wide = frames_dev + 2 * EDGE
    blocks = width // LANES
    act_wide, normed_mid, scale_mid = kernel_call(
        forward_kernel,
        (
            jax.ShapeDtypeStruct((slabs * wide, width), jnp.bfloat16),
            jax.ShapeDtypeStruct((slabs * wide, width), jnp.float32),
            jax.ShapeDtypeStruct((slabs * wide, LANES), jnp.float32),
        ),
        [
            pltpu.VMEM((blocks, padded, LANES), jnp.float32),
            pltpu.VMEM((blocks, wide, LANES), jnp.float32),
        ],
        elements * 3 * kernel_len,
        gated, ids, taps, gain_mid[None],
    )
    activated = act_wide.reshape(slabs, wide, width)[:, EDGE : EDGE + frames_dev]
    activated = activated.reshape(rows_dev, width)
    act_other = lax.ppermute(activated, "core", swap)
    grad_act = jnp.dot(upstream_wide, out_full.T, preferred_element_type=jnp.float32)
    grad_mixing, grad_gain_mid = kernel_call(
        middle_kernel,
        (
            jax.ShapeDtypeStruct((slabs, wide, width), jnp.float32),
            jax.ShapeDtypeStruct((8, width), jnp.float32),
        ),
        [],
        elements * 30,
        normed_mid, scale_mid, grad_act, gain_mid[None],
    )

    def summed(part):
        arrived_parts = lax.all_to_all(
            part.reshape(n_z * n_seq, LANES // n_seq, part.shape[1]), ZXY, 0, 0, tiled=True
        )
        return jnp.sum(arrived_parts.astype(jnp.float32), axis=0)

    core_ref = core[None].astype(jnp.int32)
    out_part = weight_part(core_ref, activated, act_other, upstream_rows, upstream_other)
    out_sum = summed(out_part)
    projected = jnp.dot(activated, out_full, preferred_element_type=jnp.float32)
    encoded = (frame_rows + projected).astype(jnp.bfloat16).reshape(slabs, frames_dev, width)

    grad_hidden, grad_taps = kernel_call(
        backward_kernel,
        (
            jax.ShapeDtypeStruct((rows_dev, 2 * width), jnp.bfloat16),
            jax.ShapeDtypeStruct((kernel_len + 1, width), jnp.float32),
        ),
        [
            pltpu.VMEM((blocks, wide, LANES), jnp.float32),
            pltpu.VMEM((blocks, kernel_len, 8, LANES), jnp.float32),
        ],
        elements * 5 * kernel_len,
        grad_mixing, gated, ids, taps, lin, sig,
    )
    hidden_other = lax.ppermute(grad_hidden, "core", swap)
    small = jnp.concatenate(
        [
            grad_taps,
            jnp.sum(grad_gain_mid, axis=0)[None],
            jnp.zeros((7, width), jnp.float32),
        ],
        axis=0,
    )
    small_other = lax.ppermute(small, "core", swap)
    in_part = weight_part(
        core_ref, normed, normed_other, grad_hidden, hidden_other, small, small_other
    )
    in_sum = summed(in_part)
    grad_normed = lax.dot_general(
        grad_hidden, in_full, (((1,), (1,)), ((), ())), preferred_element_type=jnp.float32
    )
    grad_rows, _ = pull_pre(grad_normed)
    grad_frames = (
        (upstream_rows.astype(jnp.float32) + grad_rows)
        .astype(jnp.bfloat16)
        .reshape(slabs, frames_dev, width)
    )
    share = LANES // n_seq
    first = lax.axis_index(SEQ) * share
    own_weight = lax.dynamic_slice_in_dim(in_weight, first, share, 0).astype(jnp.float32)
    own_gain = lax.dynamic_slice_in_dim(norm_gains, first, share, 0)[:, :1].astype(jnp.float32)
    grad_gain_pre = (
        jnp.sum(own_weight * in_sum[:, : 2 * width], axis=1, keepdims=True) / own_gain
    )
    place = jnp.arange(LANES) == kernel_len
    small_sum = jnp.where(place[None], grad_gain_pre, in_sum[:, 2 * width :])
    scale = 1.0 / math.sqrt(devices * rows_dev)
    total = (
        jnp.concatenate([in_sum[:, : 2 * width], small_sum, out_sum], axis=1) * scale
    ).astype(jnp.bfloat16)
    final = spread(total, SEQ, n_seq).reshape(LANES, total.shape[1])
    grad_in, grad_out, grad_kernel, grad_gains = kernel_call(
        finish_kernel,
        (
            jax.ShapeDtypeStruct((LANES, 2 * width), jnp.float32),
            jax.ShapeDtypeStruct((LANES, width), jnp.float32),
            jax.ShapeDtypeStruct((kernel_len, LANES), jnp.float32),
            jax.ShapeDtypeStruct((2, LANES), jnp.float32),
        ),
        [],
        LANES * width,
        final,
    )
    return encoded, grad_frames, grad_in, grad_out, grad_kernel.T, grad_gains.T


def solution(mesh):
    n_dp, n_seq = mesh.devices.shape
    side = math.isqrt(n_seq)
    split = Mesh(mesh.devices.reshape(n_dp // 2, 2, side, side), ("z", "core", "x", "y"))
    placed = (
        P((*DP, *SEQ), None),
        P(),
        P(DP, None),
        P(DP, None),
        P(DP, None),
        P(DP, None),
        P(DP, None),
        P(DP, SEQ, None),
    )
    return jax.shard_map(
        per_device,
        mesh=split,
        in_specs=placed,
        out_specs=(
            P(DP, SEQ, None),
            P(DP, SEQ, None),
            P(DP, None),
            P(DP, None),
            P(DP, None),
            P(DP, None),
        ),
        check_vma=False,
    )
```

```python
import functools
import math

import jax
import jax.numpy as jnp
from jax import lax
from jax.experimental import pallas as pl
from jax.experimental.pallas import tpu as pltpu
from jax.sharding import Mesh, PartitionSpec as P


DP = ("z", "core")
SEQ = ("x", "y")
ZXY = ("z", "x", "y")
EDGE = 16
LANES = 128
ROWS_STEP = 32
EPS = 1e-05
SMALL = 2 * LANES
VMEM_GRANT = 16 * 1024 * 1024


def forward_kernel(
    gated_ref, ids_ref, taps_ref, gain_ref,
    act_ref, normed_ref, scale_ref, pad_ref, mix_ref,
):
    slabs, padded, width = gated_ref.shape
    blocks = width // LANES
    taps_count = taps_ref.shape[1] - 1
    wide = padded - 2 * EDGE
    shift = EDGE - taps_count // 2

    def one_slab(s, carry):
        for b in range(blocks):
            pad_ref[b] = gated_ref[s, :, b * LANES : (b + 1) * LANES].astype(jnp.float32)

        def conv_step(i, carry):
            row = pl.multiple_of((i // (blocks // 2)) * ROWS_STEP, ROWS_STEP)
            b = (i % (blocks // 2)) * 2
            center = ids_ref[s, pl.ds(row + EDGE, ROWS_STEP)]
            sums = [jnp.zeros((ROWS_STEP, LANES), jnp.float32) for _ in range(2)]
            for k in range(taps_count):
                same = ids_ref[s, pl.ds(row + k + shift, ROWS_STEP)] == center
                for j in range(2):
                    term = pad_ref[b + j, pl.ds(row + k + shift, ROWS_STEP)]
                    sums[j] = sums[j] + jnp.where(same, term, 0.0) * taps_ref[b + j, k : k + 1, :]
            for j in range(2):
                mix_ref[b + j, pl.ds(row, ROWS_STEP)] = sums[j]
            return carry

        lax.fori_loop(0, (wide // ROWS_STEP) * (blocks // 2), conv_step, 0)

        def row_step(i, carry):
            row = pl.multiple_of(i * 16, 16)
            out_row = pl.multiple_of(s * wide + i * 16, 16)
            mixing = jnp.concatenate([mix_ref[b, pl.ds(row, 16)] for b in range(blocks)], axis=1)
            centered = mixing - jnp.mean(mixing, axis=-1, keepdims=True)
            scale = lax.rsqrt(jnp.mean(centered * centered, axis=-1, keepdims=True) + EPS)
            normed = centered * scale
            value = normed * gain_ref[0:1, :]
            act_ref[pl.ds(out_row, 16), :] = (value * jax.nn.sigmoid(value)).astype(act_ref.dtype)
            normed_ref[pl.ds(out_row, 16), :] = normed
            scale_ref[pl.ds(out_row, 16), :] = jnp.broadcast_to(scale, (16, LANES))
            return carry

        return lax.fori_loop(0, wide // 16, row_step, carry)

    lax.fori_loop(0, slabs, one_slab, 0)


def middle_kernel(normed_ref, scale_ref, grad_act_ref, gain_ref, grad_mix_ref, grad_gain_ref):
    slabs, frames, _ = grad_mix_ref.shape
    steps = frames // 16

    def row_step(i, total):
        row = pl.multiple_of(i * 16, 16)
        normed = normed_ref[pl.ds(row, 16), :]
        scale = scale_ref[pl.ds(row, 16), 0:1]
        gain = gain_ref[0:1, :]
        value = normed * gain
        sig = jax.nn.sigmoid(value)
        grad_value = grad_act_ref[pl.ds(row, 16), :] * (sig * (1.0 + value * (1.0 - sig)))
        part = grad_value * normed
        at = i % steps
        own = jnp.logical_and(at > 0, at < steps - 1)
        total = total + jnp.where(own, part[0:8] + part[8:16], 0.0)
        grad_normed = grad_value * gain
        first = jnp.mean(grad_normed, axis=-1, keepdims=True)
        second = jnp.mean(grad_normed * normed, axis=-1, keepdims=True)
        grad_mix_ref[i // steps, pl.ds(pl.multiple_of((i % steps) * 16, 16), 16), :] = scale * (
            grad_normed - first - normed * second
        )
        return total

    grad_gain_ref[...] = lax.fori_loop(
        0, slabs * steps, row_step, jnp.zeros(grad_gain_ref.shape, jnp.float32)
    )


def backward_kernel(
    grad_mix_ref, gated_ref, ids_ref, taps_ref, lin_ref, sig_ref, grad_gain_ref,
    grad_hidden_ref, grad_taps_ref, pad_ref, sum_ref,
):
    slabs, padded, width = gated_ref.shape
    frames = padded - 4 * EDGE
    blocks = width // LANES
    taps_count = taps_ref.shape[1] - 1
    half = taps_count // 2
    sum_ref[...] = jnp.zeros(sum_ref.shape, jnp.float32)

    def one_slab(s, carry):
        for b in range(blocks):
            pad_ref[b] = grad_mix_ref[s, :, b * LANES : (b + 1) * LANES]

        def conv_step(i, carry):
            row = pl.multiple_of((i // (blocks // 2)) * ROWS_STEP, ROWS_STEP)
            out_row = pl.multiple_of(s * frames + row, ROWS_STEP)
            b = (i % (blocks // 2)) * 2
            hid_row = pl.multiple_of(s * padded + 2 * EDGE + row, ROWS_STEP)
            center = ids_ref[s, pl.ds(row + 2 * EDGE, ROWS_STEP)]
            sums = [jnp.zeros((ROWS_STEP, LANES), jnp.float32) for _ in range(2)]
            cols = [pl.ds(pl.multiple_of((b + j) * LANES, LANES), LANES) for j in range(2)]
            here = [gated_ref[s, pl.ds(row + 2 * EDGE, ROWS_STEP), cols[j]].astype(jnp.float32) for j in range(2)]
            for k in range(taps_count):
                at = row + EDGE + half - k
                same = ids_ref[s, pl.ds(at + EDGE, ROWS_STEP)] == center
                for j in range(2):
                    term = jnp.where(same, pad_ref[b + j, pl.ds(at, ROWS_STEP)], 0.0)
                    sums[j] = sums[j] + term * taps_ref[b + j, k : k + 1, :]
                    part = term * here[j]
                    sum_ref[b + j, k] = sum_ref[b + j, k] + (
                        (part[0:8] + part[8:16]) + (part[16:24] + part[24:32])
                    )
            for j in range(2):
                lin = lin_ref[pl.ds(hid_row, ROWS_STEP), cols[j]]
                sig = sig_ref[pl.ds(hid_row, ROWS_STEP), cols[j]]
                grad_lin = sums[j] * sig
                grad_hidden_ref[pl.ds(out_row, ROWS_STEP), cols[j]] = grad_lin.astype(jnp.bfloat16)
                grad_hidden_ref[
                    pl.ds(out_row, ROWS_STEP),
                    pl.ds(pl.multiple_of(width + (b + j) * LANES, LANES), LANES),
                ] = (grad_lin * lin * (1.0 - sig)).astype(jnp.bfloat16)
            return carry

        return lax.fori_loop(0, (frames // ROWS_STEP) * (blocks // 2), conv_step, carry)

    lax.fori_loop(0, slabs, one_slab, 0)
    for b in range(blocks):
        for k in range(taps_count):
            grad_taps_ref[k : k + 1, b * LANES : (b + 1) * LANES] = jnp.sum(
                sum_ref[b, k], axis=0, keepdims=True
            )
    grad_taps_ref[taps_count:, :] = jnp.zeros(
        (grad_taps_ref.shape[0] - taps_count, width), jnp.float32
    )
    grad_taps_ref[taps_count + 1 : taps_count + 2, :] = jnp.sum(
        grad_gain_ref[...], axis=0, keepdims=True
    )


def send_kernel(index_ref, rows_ref, out_ref):
    rows, width = rows_ref.shape
    pick = (lax.broadcasted_iota(jnp.int32, (index_ref.shape[0], rows), 1) == index_ref[...])
    pick = pick.astype(jnp.float32).astype(jnp.bfloat16)
    for h in range(2):
        part = jnp.dot(
            pick,
            rows_ref[:, h * (width // 2) : (h + 1) * (width // 2)],
            preferred_element_type=jnp.float32,
        )
        slots = part.shape[0] // out_ref.shape[0]
        out_ref[:, h * slots : (h + 1) * slots, :] = part.astype(jnp.bfloat16).reshape(
            out_ref.shape[0], slots, width // 2
        )


def receive_kernel(index_ref, arrived_ref, upstream_ref, out_ref, last_ref, first_ref):
    slots, half = arrived_ref.shape
    slabs, frames, _ = upstream_ref.shape
    reach = 2 * EDGE
    columns = lax.broadcasted_iota(jnp.int32, (index_ref.shape[0], slots), 1)
    for h in range(2):
        pick = (columns == index_ref[:, h : h + 1]).astype(jnp.float32).astype(jnp.bfloat16)
        rows = jnp.dot(pick, arrived_ref[...], preferred_element_type=jnp.float32)
        rows = rows.astype(jnp.bfloat16)
        cols = slice(h * half, (h + 1) * half)
        out_ref[:, cols] = rows
        for s in range(slabs):
            last_ref[s, :reach, cols] = rows[(s + 1) * frames - reach : (s + 1) * frames]
            first_ref[s, :reach, cols] = rows[s * frames : s * frames + reach]
    for s in range(slabs):
        last_ref[s, reach:, :] = upstream_ref[s, frames - EDGE :, :]
        first_ref[s, reach:, :] = upstream_ref[s, :EDGE, :]


def total_kernel(parts_ref, out_sum_ref, weight_ref, gain_ref, total_ref, sum_ref, *, tap, scale):
    count, share, width = parts_ref.shape
    in_width = weight_ref.shape[1]
    grad_gain = jnp.zeros((share, 1), jnp.float32)
    for at in range(0, width, SMALL):
        cols = slice(at, at + SMALL)
        part = jnp.zeros((share, SMALL), jnp.float32)
        for j in range(0, count, 16):
            part = part + jnp.sum(parts_ref[j : j + 16, :, cols].astype(jnp.float32), axis=0)
        sum_ref[:, cols] = part
        if at < in_width:
            grad_gain = grad_gain + jnp.sum(part * weight_ref[:, cols], axis=1, keepdims=True)
    small = sum_ref[:, in_width:]
    column = lax.broadcasted_iota(jnp.int32, small.shape, 1)
    sum_ref[:, in_width:] = jnp.where(column == tap, grad_gain / gain_ref[...], small)
    for i in range(total_ref.shape[0]):
        total_ref[i, :, :width] = (sum_ref[...] * scale).astype(jnp.bfloat16)
        total_ref[i, :, width:] = (out_sum_ref[...] * scale).astype(jnp.bfloat16)


def finish_kernel(final_ref, grad_in_ref, grad_out_ref, grad_taps_ref, grad_gains_ref):
    in_width, taps_count = grad_in_ref.shape[1], grad_taps_ref.shape[0]
    grad_in_ref[...] = final_ref[:, :in_width].astype(jnp.float32)
    grad_out_ref[...] = final_ref[:, in_width + SMALL :].astype(jnp.float32)
    small = final_ref[:, in_width : in_width + LANES].astype(jnp.float32).T
    grad_taps_ref[...] = small[:taps_count]
    grad_gains_ref[...] = small[taps_count : taps_count + 2]


def product_kernel(core_ref, left_ref, left_other_ref, right_ref, right_other_ref, *rest):
    small_refs, out_ref, turned_ref = rest[:-2], rest[-2], rest[-1]
    rows, channels = left_ref.shape
    width = right_ref.shape[1]
    step = 512
    picks = [
        pl.ds(pl.multiple_of((2 * z + core_ref[0]) * LANES, LANES), LANES)
        for z in range(channels // LANES // 2)
    ]
    for z, pick in enumerate(picks):
        for h, ref in enumerate((left_ref, left_other_ref)):
            turned_ref[z * LANES : (z + 1) * LANES, h * rows : (h + 1) * rows] = ref[:, pick].T
    for at in range(0, width, step):
        right = jnp.concatenate(
            [right_ref[:, at : at + step], right_other_ref[:, at : at + step]], axis=0
        )
        out_ref[:, at : at + step] = jnp.dot(
            turned_ref[...], right, preferred_element_type=jnp.float32
        ).astype(out_ref.dtype)
    if small_refs:
        for z, pick in enumerate(picks):
            small = small_refs[0][:, pick] + small_refs[1][:, pick]
            filled = jnp.concatenate(
                [small, jnp.zeros((LANES - small.shape[0], LANES), jnp.float32)], axis=0
            )
            block = slice(z * LANES, (z + 1) * LANES)
            out_ref[block, width : width + LANES] = filled.T.astype(out_ref.dtype)
            out_ref[block, width + LANES :] = jnp.zeros((LANES, SMALL - LANES), out_ref.dtype)


def weight_part(core, left, left_other, right, right_other, *small):
    rows, channels = left.shape
    mine = channels // LANES // 2
    width = right.shape[1]
    out_width = width + (SMALL if small else 0)
    vmem = pl.BlockSpec(memory_space=pltpu.VMEM)
    return pl.pallas_call(
        product_kernel,
        out_shape=jax.ShapeDtypeStruct((mine * LANES, out_width), jnp.bfloat16),
        in_specs=[pl.BlockSpec(memory_space=pltpu.SMEM)] + [vmem] * (4 + len(small)),
        out_specs=vmem,
        scratch_shapes=[pltpu.VMEM((mine * LANES, 2 * rows), jnp.bfloat16)],
        name="weight_part",
        compiler_params=pltpu.CompilerParams(vmem_limit_bytes=VMEM_GRANT),
        cost_estimate=pl.CostEstimate(
            flops=4 * rows * mine * LANES * width,
            bytes_accessed=4 * rows * (channels + width),
            transcendentals=0,
        ),
    )(core, left, left_other, right, right_other, *small)


def norm_kernel(frames_ref, low_ref, high_ref, gain_ref, wide_ref, own_ref):
    slabs, padded, _ = wide_ref.shape
    reach = 2 * EDGE
    own = padded - 2 * reach

    def normed_rows(rows):
        values = rows.astype(jnp.float32)
        centered = values - jnp.mean(values, axis=-1, keepdims=True)
        spread_ = jnp.mean(centered * centered, axis=-1, keepdims=True)
        return (centered * lax.rsqrt(spread_ + EPS) * gain_ref[0:1, :]).astype(jnp.bfloat16)

    for s in range(slabs):
        for at in range(0, reach, 16):
            wide_ref[s, at : at + 16, :] = normed_rows(low_ref[s, at : at + 16, :])
            high_at = reach + own + at
            wide_ref[s, high_at : high_at + 16, :] = normed_rows(high_ref[s, at : at + 16, :])

    def step(i, carry):
        row = pl.multiple_of(i * 16, 16)
        rows = normed_rows(frames_ref[pl.ds(row, 16), :])
        own_ref[pl.ds(row, 16), :] = rows
        steps = own // 16
        wide_ref[i // steps, pl.ds(pl.multiple_of(reach + (i % steps) * 16, 16), 16), :] = rows
        return carry

    lax.fori_loop(0, slabs * own // 16, step, 0, unroll=2)


def project_kernel(normed_ref, lin_w_ref, gate_w_ref, lin_ref, sig_ref, gated_ref):
    lin = jnp.dot(normed_ref[...], lin_w_ref[...], preferred_element_type=jnp.float32)
    gate = jnp.dot(normed_ref[...], gate_w_ref[...], preferred_element_type=jnp.float32)
    sig = jax.nn.sigmoid(gate)
    lin_ref[...] = lin
    sig_ref[...] = sig
    gated_ref[...] = (lin * sig).astype(jnp.bfloat16)


def project(normed, weight):
    rows, width = normed.shape
    cols = 256
    steps = width // cols
    out = pl.BlockSpec((rows, cols), lambda j: (0, j))
    return pl.pallas_call(
        project_kernel,
        out_shape=(
            jax.ShapeDtypeStruct((rows, width), jnp.float32),
            jax.ShapeDtypeStruct((rows, width), jnp.float32),
            jax.ShapeDtypeStruct((rows, width), jnp.bfloat16),
        ),
        grid=(steps,),
        in_specs=[
            pl.BlockSpec((rows, width), lambda j: (0, 0)),
            pl.BlockSpec((width, cols), lambda j: (0, j)),
            pl.BlockSpec((width, cols), lambda j: (0, j + steps)),
        ],
        out_specs=(out, out, out),
        name="project",
        compiler_params=pltpu.CompilerParams(vmem_limit_bytes=VMEM_GRANT),
        cost_estimate=pl.CostEstimate(
            flops=4 * rows * width * width,
            bytes_accessed=4 * width * width,
            transcendentals=rows * width,
        ),
    )(normed, weight, weight)


def kernel_call(body, outs, scratch, flops, *args):
    moved = sum(a.size * a.dtype.itemsize for a in args)
    return pl.pallas_call(
        body,
        out_shape=outs,
        scratch_shapes=scratch,
        compiler_params=pltpu.CompilerParams(vmem_limit_bytes=VMEM_GRANT),
        cost_estimate=pl.CostEstimate(flops=flops, bytes_accessed=moved, transcendentals=0),
    )(*args)


def to_neighbours(last, first, count):
    forward = [(i, i + 1) for i in range(count - 1)]
    backward = [(i + 1, i) for i in range(count - 1)]
    return lax.ppermute(last, SEQ, forward), lax.ppermute(first, SEQ, backward)


def norm_rows(values, gain):
    average = jnp.mean(values, axis=-1, keepdims=True)
    centered = values - average
    spread_ = jnp.mean(centered * centered, axis=-1, keepdims=True)
    return centered * lax.rsqrt(spread_ + EPS) * gain


def per_device(
    loaded, plan, segment_ids, in_weight, out_weight, depth_kernel, norm_gains, upstream
):
    rows_dev, width = loaded.shape
    devices = plan.shape[0]
    capacity = 2 * rows_dev // devices
    slabs, slab_len = segment_ids.shape
    n_seq = lax.axis_size(SEQ)
    n_z = lax.axis_size("z")
    frames_dev = slab_len // n_seq
    kernel_len = depth_kernel.shape[1]
    core = lax.axis_index("core")
    sender = lax.axis_index((*DP, *SEQ))
    swap = [(0, 1), (1, 0)]

    in_full = lax.all_gather(in_weight, DP, axis=0, tiled=True)
    out_full = lax.all_gather(out_weight, DP, axis=0, tiled=True)

    send_plan = lax.dynamic_index_in_dim(plan, sender, 0, keepdims=False)
    send_start = jnp.cumsum(send_plan) - send_plan
    slot_index = jnp.arange(capacity, dtype=jnp.int32)
    source_rows = jnp.minimum(send_start[:, None] + slot_index[None, :], rows_dev - 1)
    outgoing = kernel_call(
        send_kernel,
        jax.ShapeDtypeStruct((devices, 2 * capacity, width // 2), jnp.bfloat16),
        [],
        4 * devices * capacity * rows_dev * width,
        source_rows.reshape(-1, 1), loaded,
    )
    arrived = lax.all_to_all(
        outgoing, (*DP, *SEQ), split_axis=0, concat_axis=0, tiled=True
    ).reshape(devices * 2 * capacity, width // 2)
    extras = jnp.pad(
        jnp.concatenate([depth_kernel, norm_gains], axis=1), ((0, 0), (0, LANES - kernel_len - 2))
    )
    upstream_rows = upstream.reshape(rows_dev, width)
    extras_other = lax.ppermute(extras, "core", swap)
    pair = jnp.where(
        core == 0, jnp.stack([extras, extras_other]), jnp.stack([extras_other, extras])
    )
    from_z = [
        lax.ppermute(pair, "z", [(i, (i + d) % n_z) for i in range(n_z)]) for d in range(1, n_z)
    ]
    upstream_other = lax.ppermute(upstream_rows, "core", swap)
    arrived, upstream_other, pair, *from_z = lax.optimization_barrier(
        (arrived, upstream_other, pair, *from_z)
    )
    by_z = jnp.stack([*from_z[::-1], pair])
    side_all = lax.dynamic_slice_in_dim(
        jnp.concatenate([by_z, by_z]), n_z - 1 - lax.axis_index("z"), n_z, 0
    )
    recv_plan = lax.dynamic_index_in_dim(plan, sender, 1, keepdims=False)
    recv_end = jnp.cumsum(recv_plan)
    frame_index = jnp.arange(rows_dev, dtype=jnp.int32)
    before = recv_end[None, :] <= frame_index[:, None]
    source_dev = jnp.sum(before.astype(jnp.int32), axis=1)
    start_of = jnp.sum(jnp.where(before, recv_plan[None, :], 0), axis=1)
    place = source_dev * 2 * capacity + frame_index - start_of
    frames, last, first = kernel_call(
        receive_kernel,
        (
            jax.ShapeDtypeStruct((rows_dev, width), jnp.bfloat16),
            jax.ShapeDtypeStruct((slabs, 3 * EDGE, width), jnp.bfloat16),
            jax.ShapeDtypeStruct((slabs, 3 * EDGE, width), jnp.bfloat16),
        ),
        [],
        4 * devices * capacity * rows_dev * width,
        jnp.stack([place, place + capacity], axis=1), arrived, upstream,
    )
    low, high = to_neighbours(last, first, n_seq)
    side = side_all.reshape(width, LANES)[:, : kernel_len + 2].astype(jnp.float32).T
    gain_pre, gain_mid = side[kernel_len], side[kernel_len + 1]
    taps = jnp.pad(side[:kernel_len], ((0, 1), (0, 0)))
    taps = taps.reshape(kernel_len + 1, width // LANES, LANES).transpose(1, 0, 2)

    upstream_wide = jnp.concatenate(
        [low[:, 2 * EDGE :], upstream, high[:, 2 * EDGE :]], axis=1
    ).reshape(-1, width)

    id_pad = jnp.pad(segment_ids, ((0, 0), (2 * EDGE, 2 * EDGE)), constant_values=-1)
    window = lax.dynamic_slice_in_dim(
        id_pad, lax.axis_index(SEQ) * frames_dev, frames_dev + 4 * EDGE, 1
    )
    ids = jnp.broadcast_to(window[:, :, None], (*window.shape, LANES))

    frame_rows = frames.astype(jnp.float32)
    _, pull_pre = jax.vjp(norm_rows, frame_rows, gain_pre)
    padded = frames_dev + 4 * EDGE
    normed_wide, normed = kernel_call(
        norm_kernel,
        (
            jax.ShapeDtypeStruct((slabs, padded, width), jnp.bfloat16),
            jax.ShapeDtypeStruct((rows_dev, width), jnp.bfloat16),
        ),
        [],
        rows_dev * width * 10,
        frames, low, high, gain_pre[None],
    )
    normed_other = lax.ppermute(normed, "core", swap)
    in_full, normed_other = lax.optimization_barrier((in_full, normed_other))
    lin, sig, gated = project(normed_wide.reshape(-1, width), in_full)
    gated = gated.reshape(slabs, padded, width)
    elements = rows_dev * width
    wide = frames_dev + 2 * EDGE
    blocks = width // LANES
    act_wide, normed_mid, scale_mid = kernel_call(
        forward_kernel,
        (
            jax.ShapeDtypeStruct((slabs * wide, width), jnp.bfloat16),
            jax.ShapeDtypeStruct((slabs * wide, width), jnp.float32),
            jax.ShapeDtypeStruct((slabs * wide, LANES), jnp.float32),
        ),
        [
            pltpu.VMEM((blocks, padded, LANES), jnp.float32),
            pltpu.VMEM((blocks, wide, LANES), jnp.float32),
        ],
        elements * 3 * kernel_len,
        gated, ids, taps, gain_mid[None],
    )
    activated = act_wide.reshape(slabs, wide, width)[:, EDGE : EDGE + frames_dev]
    activated = activated.reshape(rows_dev, width)
    act_other = lax.ppermute(activated, "core", swap)
    grad_act = jnp.dot(upstream_wide, out_full.T, preferred_element_type=jnp.float32)
    grad_mixing, grad_gain_mid = kernel_call(
        middle_kernel,
        (
            jax.ShapeDtypeStruct((slabs, wide, width), jnp.float32),
            jax.ShapeDtypeStruct((8, width), jnp.float32),
        ),
        [],
        elements * 30,
        normed_mid, scale_mid, grad_act, gain_mid[None],
    )

    def exchanged(part):
        return lax.all_to_all(
            part.reshape(n_z * n_seq, LANES // n_seq, part.shape[1]), ZXY, 0, 0, tiled=True
        )

    core_ref = core[None].astype(jnp.int32)
    out_part = weight_part(core_ref, activated, act_other, upstream_rows, upstream_other)
    out_parts = exchanged(out_part)
    out_sum = jnp.sum(out_parts.astype(jnp.float32), axis=0)
    projected = jnp.dot(activated, out_full, preferred_element_type=jnp.float32)
    encoded = (frame_rows + projected).astype(jnp.bfloat16).reshape(slabs, frames_dev, width)

    grad_hidden, grad_taps = kernel_call(
        backward_kernel,
        (
            jax.ShapeDtypeStruct((rows_dev, 2 * width), jnp.bfloat16),
            jax.ShapeDtypeStruct((kernel_len + 9, width), jnp.float32),
        ),
        [
            pltpu.VMEM((blocks, wide, LANES), jnp.float32),
            pltpu.VMEM((blocks, kernel_len, 8, LANES), jnp.float32),
        ],
        elements * 5 * kernel_len,
        grad_mixing, gated, ids, taps, lin, sig, grad_gain_mid,
    )
    hidden_other = lax.ppermute(grad_hidden, "core", swap)
    small_other = lax.ppermute(grad_taps, "core", swap)
    in_part = weight_part(
        core_ref, normed, normed_other, grad_hidden, hidden_other, grad_taps, small_other
    )
    in_parts = exchanged(in_part)
    grad_normed = lax.dot_general(
        grad_hidden, in_full, (((1,), (1,)), ((), ())), preferred_element_type=jnp.float32
    )
    grad_rows, _ = pull_pre(grad_normed)
    grad_frames = (
        (upstream_rows.astype(jnp.float32) + grad_rows)
        .astype(jnp.bfloat16)
        .reshape(slabs, frames_dev, width)
    )
    share = LANES // n_seq
    start = lax.axis_index(SEQ) * share
    own_weight = lax.dynamic_slice_in_dim(in_weight, start, share, 0).astype(jnp.float32)
    own_gain = lax.dynamic_slice_in_dim(norm_gains, start, share, 0)[:, :1].astype(jnp.float32)
    total = kernel_call(
        functools.partial(
            total_kernel, tap=kernel_len, scale=1.0 / math.sqrt(devices * rows_dev)
        ),
        jax.ShapeDtypeStruct((n_seq, share, 3 * width + SMALL), jnp.bfloat16),
        [pltpu.VMEM((share, 2 * width + SMALL), jnp.float32)],
        in_parts.size,
        in_parts, out_sum, own_weight, own_gain,
    )
    final = lax.all_to_all(total, SEQ, 0, 0, tiled=True).reshape(LANES, -1)
    grad_in, grad_out, grad_kernel, grad_gains = kernel_call(
        finish_kernel,
        (
            jax.ShapeDtypeStruct((LANES, 2 * width), jnp.float32),
            jax.ShapeDtypeStruct((LANES, width), jnp.float32),
            jax.ShapeDtypeStruct((kernel_len, LANES), jnp.float32),
            jax.ShapeDtypeStruct((2, LANES), jnp.float32),
        ),
        [],
        LANES * width,
        final,
    )
    return encoded, grad_frames, grad_in, grad_out, grad_kernel.T, grad_gains.T


def solution(mesh):
    n_dp, n_seq = mesh.devices.shape
    side = math.isqrt(n_seq)
    split = Mesh(mesh.devices.reshape(n_dp // 2, 2, side, side), ("z", "core", "x", "y"))
    placed = (
        P((*DP, *SEQ), None),
        P(),
        P(DP, None),
        P(DP, None),
        P(DP, None),
        P(DP, None),
        P(DP, None),
        P(DP, SEQ, None),
    )
    return jax.shard_map(
        per_device,
        mesh=split,
        in_specs=placed,
        out_specs=(
            P(DP, SEQ, None),
            P(DP, SEQ, None),
            P(DP, None),
            P(DP, None),
            P(DP, None),
            P(DP, None),
        ),
        check_vma=False,
    )
```

```python
import functools
import math

import jax
import jax.numpy as jnp
from jax import lax
from jax.experimental import pallas as pl
from jax.experimental.pallas import tpu as pltpu
from jax.sharding import Mesh, PartitionSpec as P


DP = ("z", "core")
SEQ = ("x", "y")
ZXY = ("z", "x", "y")
EDGE = 16
LANES = 128
ROWS_STEP = 32
EPS = 1e-05
SMALL = 2 * LANES
VMEM_GRANT = 16 * 1024 * 1024


def forward_kernel(
    gated_ref, ids_ref, taps_ref, gain_ref,
    act_ref, normed_ref, scale_ref, pad_ref, mix_ref,
):
    slabs, padded, width = gated_ref.shape
    blocks = width // LANES
    taps_count = taps_ref.shape[1] - 1
    wide = padded - 2 * EDGE
    own = wide - 2 * EDGE
    shift = EDGE - taps_count // 2

    def one_slab(s, carry):
        for b in range(blocks):
            pad_ref[b] = gated_ref[s, :, b * LANES : (b + 1) * LANES].astype(jnp.float32)

        def conv_step(i, carry):
            row = pl.multiple_of((i // (blocks // 2)) * ROWS_STEP, ROWS_STEP)
            b = (i % (blocks // 2)) * 2
            center = ids_ref[s, pl.ds(row + EDGE, ROWS_STEP)]
            sums = [jnp.zeros((ROWS_STEP, LANES), jnp.float32) for _ in range(2)]
            for k in range(taps_count):
                same = ids_ref[s, pl.ds(row + k + shift, ROWS_STEP)] == center
                for j in range(2):
                    term = pad_ref[b + j, pl.ds(row + k + shift, ROWS_STEP)]
                    sums[j] = sums[j] + jnp.where(same, term, 0.0) * taps_ref[b + j, k : k + 1, :]
            for j in range(2):
                mix_ref[b + j, pl.ds(row, ROWS_STEP)] = sums[j]
            return carry

        lax.fori_loop(0, (wide // ROWS_STEP) * (blocks // 2), conv_step, 0)

        def row_step(i, own_rows):
            row = pl.multiple_of(i * 16, 16)
            out_row = pl.multiple_of(s * wide + i * 16, 16)
            mixing = jnp.concatenate([mix_ref[b, pl.ds(row, 16)] for b in range(blocks)], axis=1)
            centered = mixing - jnp.mean(mixing, axis=-1, keepdims=True)
            scale = lax.rsqrt(jnp.mean(centered * centered, axis=-1, keepdims=True) + EPS)
            normed = centered * scale
            if own_rows:
                act_row = pl.multiple_of(s * own + i * 16 - EDGE, 16)
                value = normed * gain_ref[0:1, :]
                act_ref[pl.ds(act_row, 16), :] = (value * jax.nn.sigmoid(value)).astype(
                    act_ref.dtype
                )
            normed_ref[pl.ds(out_row, 16), :] = normed
            scale_ref[pl.ds(out_row, 16), :] = jnp.broadcast_to(scale, (16, LANES))

        steps = wide // 16
        row_step(0, False)
        row_step(steps - 1, False)

        def own_step(i, carry):
            row_step(i + 1, True)
            return carry

        return lax.fori_loop(0, steps - 2, own_step, carry, unroll=4)

    lax.fori_loop(0, slabs, one_slab, 0)


def middle_kernel(
    normed_ref, scale_ref, upstream_ref, weight_ref, gain_ref,
    grad_mix_ref, grad_gain_ref, grad_act_ref,
):
    slabs, frames, _ = grad_mix_ref.shape
    steps = frames // 16
    grad_act_ref[...] = lax.dot_general(
        upstream_ref[...],
        weight_ref[...],
        (((1,), (1,)), ((), ())),
        preferred_element_type=jnp.float32,
    )

    def row_step(i, total):
        row = pl.multiple_of(i * 16, 16)
        normed = normed_ref[pl.ds(row, 16), :]
        scale = scale_ref[pl.ds(row, 16), 0:1]
        gain = gain_ref[0:1, :]
        value = normed * gain
        sig = jax.nn.sigmoid(value)
        grad_value = grad_act_ref[pl.ds(row, 16), :] * (sig * (1.0 + value * (1.0 - sig)))
        part = grad_value * normed
        at = i % steps
        own = jnp.logical_and(at > 0, at < steps - 1)
        total = total + jnp.where(own, part[0:8] + part[8:16], 0.0)
        grad_normed = grad_value * gain
        first = jnp.mean(grad_normed, axis=-1, keepdims=True)
        second = jnp.mean(grad_normed * normed, axis=-1, keepdims=True)
        grad_mix_ref[i // steps, pl.ds(pl.multiple_of((i % steps) * 16, 16), 16), :] = scale * (
            grad_normed - first - normed * second
        )
        return total

    grad_gain_ref[...] = lax.fori_loop(
        0, slabs * steps, row_step, jnp.zeros(grad_gain_ref.shape, jnp.float32), unroll=4
    )


def backward_kernel(
    grad_mix_ref, gated_ref, ids_ref, taps_ref, lin_ref, sig_ref, grad_gain_ref,
    grad_hidden_ref, grad_taps_ref, pad_ref, sum_ref,
):
    slabs, padded, width = gated_ref.shape
    frames = padded - 4 * EDGE
    blocks = width // LANES
    taps_count = taps_ref.shape[1] - 1
    half = taps_count // 2
    sum_ref[...] = jnp.zeros(sum_ref.shape, jnp.float32)

    def one_slab(s, carry):
        for b in range(blocks):
            pad_ref[b] = grad_mix_ref[s, :, b * LANES : (b + 1) * LANES]

        def conv_step(i, carry):
            row = pl.multiple_of((i // (blocks // 2)) * ROWS_STEP, ROWS_STEP)
            out_row = pl.multiple_of(s * frames + row, ROWS_STEP)
            b = (i % (blocks // 2)) * 2
            hid_row = pl.multiple_of(s * padded + 2 * EDGE + row, ROWS_STEP)
            center = ids_ref[s, pl.ds(row + 2 * EDGE, ROWS_STEP)]
            sums = [jnp.zeros((ROWS_STEP, LANES), jnp.float32) for _ in range(2)]
            cols = [pl.ds(pl.multiple_of((b + j) * LANES, LANES), LANES) for j in range(2)]
            here = [gated_ref[s, pl.ds(row + 2 * EDGE, ROWS_STEP), cols[j]].astype(jnp.float32) for j in range(2)]
            for k in range(taps_count):
                at = row + EDGE + half - k
                same = ids_ref[s, pl.ds(at + EDGE, ROWS_STEP)] == center
                for j in range(2):
                    term = jnp.where(same, pad_ref[b + j, pl.ds(at, ROWS_STEP)], 0.0)
                    sums[j] = sums[j] + term * taps_ref[b + j, k : k + 1, :]
                    part = term * here[j]
                    sum_ref[b + j, k] = sum_ref[b + j, k] + (
                        (part[0:8] + part[8:16]) + (part[16:24] + part[24:32])
                    )
            for j in range(2):
                lin = lin_ref[pl.ds(hid_row, ROWS_STEP), cols[j]]
                sig = sig_ref[pl.ds(hid_row, ROWS_STEP), cols[j]]
                grad_lin = sums[j] * sig
                grad_hidden_ref[pl.ds(out_row, ROWS_STEP), cols[j]] = grad_lin.astype(jnp.bfloat16)
                grad_hidden_ref[
                    pl.ds(out_row, ROWS_STEP),
                    pl.ds(pl.multiple_of(width + (b + j) * LANES, LANES), LANES),
                ] = (grad_lin * lin * (1.0 - sig)).astype(jnp.bfloat16)
            return carry

        return lax.fori_loop(0, (frames // ROWS_STEP) * (blocks // 2), conv_step, carry)

    lax.fori_loop(0, slabs, one_slab, 0)
    for b in range(blocks):
        for k in range(taps_count):
            grad_taps_ref[k : k + 1, b * LANES : (b + 1) * LANES] = jnp.sum(
                sum_ref[b, k], axis=0, keepdims=True
            )
    grad_taps_ref[taps_count:, :] = jnp.zeros(
        (grad_taps_ref.shape[0] - taps_count, width), jnp.float32
    )
    grad_taps_ref[taps_count + 1 : taps_count + 2, :] = jnp.sum(
        grad_gain_ref[...], axis=0, keepdims=True
    )


def send_kernel(index_ref, rows_ref, out_ref):
    rows, width = rows_ref.shape
    pick = (lax.broadcasted_iota(jnp.int32, (index_ref.shape[0], rows), 1) == index_ref[...])
    pick = pick.astype(jnp.float32).astype(jnp.bfloat16)
    for h in range(2):
        part = jnp.dot(
            pick,
            rows_ref[:, h * (width // 2) : (h + 1) * (width // 2)],
            preferred_element_type=jnp.float32,
        )
        slots = part.shape[0] // out_ref.shape[0]
        out_ref[:, h * slots : (h + 1) * slots, :] = part.astype(jnp.bfloat16).reshape(
            out_ref.shape[0], slots, width // 2
        )


def receive_kernel(index_ref, arrived_ref, upstream_ref, out_ref, last_ref, first_ref):
    slots, half = arrived_ref.shape
    slabs, frames, _ = upstream_ref.shape
    reach = 2 * EDGE
    columns = lax.broadcasted_iota(jnp.int32, (index_ref.shape[0], slots), 1)
    for h in range(2):
        pick = (columns == index_ref[:, h : h + 1]).astype(jnp.float32).astype(jnp.bfloat16)
        rows = jnp.dot(pick, arrived_ref[...], preferred_element_type=jnp.float32)
        rows = rows.astype(jnp.bfloat16)
        cols = slice(h * half, (h + 1) * half)
        out_ref[:, cols] = rows
        for s in range(slabs):
            last_ref[s, :reach, cols] = rows[(s + 1) * frames - reach : (s + 1) * frames]
            first_ref[s, :reach, cols] = rows[s * frames : s * frames + reach]
    for s in range(slabs):
        last_ref[s, reach:, :] = upstream_ref[s, frames - EDGE :, :]
        first_ref[s, reach:, :] = upstream_ref[s, :EDGE, :]


def total_kernel(parts_ref, out_sum_ref, weight_ref, gain_ref, total_ref, sum_ref, *, tap, scale):
    count, share, width = parts_ref.shape
    in_width = weight_ref.shape[1]
    grad_gain = jnp.zeros((share, 1), jnp.float32)
    for at in range(0, width, SMALL):
        cols = slice(at, at + SMALL)
        part = jnp.zeros((share, SMALL), jnp.float32)
        for j in range(0, count, 16):
            part = part + jnp.sum(parts_ref[j : j + 16, :, cols].astype(jnp.float32), axis=0)
        sum_ref[:, cols] = part
        if at < in_width:
            grad_gain = grad_gain + jnp.sum(part * weight_ref[:, cols], axis=1, keepdims=True)
    small = sum_ref[:, in_width:]
    column = lax.broadcasted_iota(jnp.int32, small.shape, 1)
    sum_ref[:, in_width:] = jnp.where(column == tap, grad_gain / gain_ref[...], small)
    for i in range(total_ref.shape[0]):
        total_ref[i, :, :width] = (sum_ref[...] * scale).astype(jnp.bfloat16)
        total_ref[i, :, width:] = (out_sum_ref[...] * scale).astype(jnp.bfloat16)


def finish_kernel(final_ref, grad_in_ref, grad_out_ref, grad_taps_ref, grad_gains_ref):
    in_width, taps_count = grad_in_ref.shape[1], grad_taps_ref.shape[0]
    grad_in_ref[...] = final_ref[:, :in_width].astype(jnp.float32)
    grad_out_ref[...] = final_ref[:, in_width + SMALL :].astype(jnp.float32)
    small = final_ref[:, in_width : in_width + LANES].astype(jnp.float32).T
    grad_taps_ref[...] = small[:taps_count]
    grad_gains_ref[...] = small[taps_count : taps_count + 2]


def product_kernel(core_ref, left_ref, left_other_ref, right_ref, right_other_ref, *rest):
    small_refs, out_ref, turned_ref = rest[:-2], rest[-2], rest[-1]
    rows, channels = left_ref.shape
    width = right_ref.shape[1]
    step = 512
    picks = [
        pl.ds(pl.multiple_of((2 * z + core_ref[0]) * LANES, LANES), LANES)
        for z in range(channels // LANES // 2)
    ]
    for z, pick in enumerate(picks):
        for h, ref in enumerate((left_ref, left_other_ref)):
            turned_ref[z * LANES : (z + 1) * LANES, h * rows : (h + 1) * rows] = ref[:, pick].T
    for at in range(0, width, step):
        right = jnp.concatenate(
            [right_ref[:, at : at + step], right_other_ref[:, at : at + step]], axis=0
        )
        out_ref[:, at : at + step] = jnp.dot(
            turned_ref[...], right, preferred_element_type=jnp.float32
        ).astype(out_ref.dtype)
    if small_refs:
        for z, pick in enumerate(picks):
            small = small_refs[0][:, pick] + small_refs[1][:, pick]
            filled = jnp.concatenate(
                [small, jnp.zeros((LANES - small.shape[0], LANES), jnp.float32)], axis=0
            )
            block = slice(z * LANES, (z + 1) * LANES)
            out_ref[block, width : width + LANES] = filled.T.astype(out_ref.dtype)
            out_ref[block, width + LANES :] = jnp.zeros((LANES, SMALL - LANES), out_ref.dtype)


def weight_part(core, left, left_other, right, right_other, *small):
    rows, channels = left.shape
    mine = channels // LANES // 2
    width = right.shape[1]
    out_width = width + (SMALL if small else 0)
    vmem = pl.BlockSpec(memory_space=pltpu.VMEM)
    return pl.pallas_call(
        product_kernel,
        out_shape=jax.ShapeDtypeStruct((mine * LANES, out_width), jnp.bfloat16),
        in_specs=[pl.BlockSpec(memory_space=pltpu.SMEM)] + [vmem] * (4 + len(small)),
        out_specs=vmem,
        scratch_shapes=[pltpu.VMEM((mine * LANES, 2 * rows), jnp.bfloat16)],
        name="weight_part",
        compiler_params=pltpu.CompilerParams(vmem_limit_bytes=VMEM_GRANT),
        cost_estimate=pl.CostEstimate(
            flops=4 * rows * mine * LANES * width,
            bytes_accessed=4 * rows * (channels + width),
            transcendentals=0,
        ),
    )(core, left, left_other, right, right_other, *small)


def norm_kernel(
    frames_ref, low_ref, high_ref, upstream_ref, gain_ref, wide_ref, own_ref, up_wide_ref
):
    slabs, padded, _ = wide_ref.shape
    reach = 2 * EDGE
    own = padded - 2 * reach

    def normed_rows(rows):
        values = rows.astype(jnp.float32)
        centered = values - jnp.mean(values, axis=-1, keepdims=True)
        spread_ = jnp.mean(centered * centered, axis=-1, keepdims=True)
        return (centered * lax.rsqrt(spread_ + EPS) * gain_ref[0:1, :]).astype(jnp.bfloat16)

    for s in range(slabs):
        for at in range(0, reach, 16):
            wide_ref[s, at : at + 16, :] = normed_rows(low_ref[s, at : at + 16, :])
            high_at = reach + own + at
            wide_ref[s, high_at : high_at + 16, :] = normed_rows(high_ref[s, at : at + 16, :])

    def step(i, carry):
        row = pl.multiple_of(i * 16, 16)
        rows = normed_rows(frames_ref[pl.ds(row, 16), :])
        own_ref[pl.ds(row, 16), :] = rows
        steps = own // 16
        wide_ref[i // steps, pl.ds(pl.multiple_of(reach + (i % steps) * 16, 16), 16), :] = rows
        return carry

    lax.fori_loop(0, slabs * own // 16, step, 0, unroll=4)
    for s in range(slabs):
        base = s * (own + 2 * EDGE)
        up_wide_ref[base : base + EDGE, :] = low_ref[s, reach:, :]
        up_wide_ref[base + EDGE : base + EDGE + own, :] = upstream_ref[s]
        up_wide_ref[base + EDGE + own : base + 2 * EDGE + own, :] = high_ref[s, reach:, :]


def project_kernel(normed_ref, lin_w_ref, gate_w_ref, lin_ref, sig_ref, gated_ref):
    lin = jnp.dot(normed_ref[...], lin_w_ref[...], preferred_element_type=jnp.float32)
    gate = jnp.dot(normed_ref[...], gate_w_ref[...], preferred_element_type=jnp.float32)
    sig = jax.nn.sigmoid(gate)
    lin_ref[...] = lin
    sig_ref[...] = sig
    gated_ref[...] = (lin * sig).astype(jnp.bfloat16)


def project(normed, weight):
    rows, width = normed.shape
    cols = 256
    steps = width // cols
    out = pl.BlockSpec((rows, cols), lambda j: (0, j))
    return pl.pallas_call(
        project_kernel,
        out_shape=(
            jax.ShapeDtypeStruct((rows, width), jnp.float32),
            jax.ShapeDtypeStruct((rows, width), jnp.float32),
            jax.ShapeDtypeStruct((rows, width), jnp.bfloat16),
        ),
        grid=(steps,),
        in_specs=[
            pl.BlockSpec((rows, width), lambda j: (0, 0)),
            pl.BlockSpec((width, cols), lambda j: (0, j)),
            pl.BlockSpec((width, cols), lambda j: (0, j + steps)),
        ],
        out_specs=(out, out, out),
        name="project",
        compiler_params=pltpu.CompilerParams(vmem_limit_bytes=50 * 1024 * 1024),
        cost_estimate=pl.CostEstimate(
            flops=4 * rows * width * width,
            bytes_accessed=4 * width * width,
            transcendentals=rows * width,
        ),
    )(normed, weight, weight)


def kernel_call(body, outs, scratch, flops, *args):
    moved = sum(a.size * a.dtype.itemsize for a in args)
    return pl.pallas_call(
        body,
        out_shape=outs,
        scratch_shapes=scratch,
        compiler_params=pltpu.CompilerParams(vmem_limit_bytes=VMEM_GRANT),
        cost_estimate=pl.CostEstimate(flops=flops, bytes_accessed=moved, transcendentals=0),
    )(*args)


def to_neighbours(last, first, count):
    forward = [(i, i + 1) for i in range(count - 1)]
    backward = [(i + 1, i) for i in range(count - 1)]
    return lax.ppermute(last, SEQ, forward), lax.ppermute(first, SEQ, backward)


def norm_rows(values, gain):
    average = jnp.mean(values, axis=-1, keepdims=True)
    centered = values - average
    spread_ = jnp.mean(centered * centered, axis=-1, keepdims=True)
    return centered * lax.rsqrt(spread_ + EPS) * gain


def per_device(
    loaded, plan, segment_ids, in_weight, out_weight, depth_kernel, norm_gains, upstream
):
    rows_dev, width = loaded.shape
    devices = plan.shape[0]
    capacity = 2 * rows_dev // devices
    slabs, slab_len = segment_ids.shape
    n_seq = lax.axis_size(SEQ)
    n_z = lax.axis_size("z")
    frames_dev = slab_len // n_seq
    kernel_len = depth_kernel.shape[1]
    core = lax.axis_index("core")
    sender = lax.axis_index((*DP, *SEQ))
    swap = [(0, 1), (1, 0)]

    in_full = lax.all_gather(in_weight, DP, axis=0, tiled=True)
    out_full = lax.all_gather(out_weight, DP, axis=0, tiled=True)

    send_plan = lax.dynamic_index_in_dim(plan, sender, 0, keepdims=False)
    send_start = jnp.cumsum(send_plan) - send_plan
    slot_index = jnp.arange(capacity, dtype=jnp.int32)
    source_rows = jnp.minimum(send_start[:, None] + slot_index[None, :], rows_dev - 1)
    outgoing = kernel_call(
        send_kernel,
        jax.ShapeDtypeStruct((devices, 2 * capacity, width // 2), jnp.bfloat16),
        [],
        4 * devices * capacity * rows_dev * width,
        source_rows.reshape(-1, 1), loaded,
    )
    arrived = lax.all_to_all(
        outgoing, (*DP, *SEQ), split_axis=0, concat_axis=0, tiled=True
    ).reshape(devices * 2 * capacity, width // 2)
    extras = jnp.pad(
        jnp.concatenate([depth_kernel, norm_gains], axis=1), ((0, 0), (0, LANES - kernel_len - 2))
    )
    upstream_rows = upstream.reshape(rows_dev, width)
    extras_other = lax.ppermute(extras, "core", swap)
    pair = jnp.where(
        core == 0, jnp.stack([extras, extras_other]), jnp.stack([extras_other, extras])
    )
    from_z = [
        lax.ppermute(pair, "z", [(i, (i + d) % n_z) for i in range(n_z)]) for d in range(1, n_z)
    ]
    upstream_other = lax.ppermute(upstream_rows, "core", swap)
    arrived, upstream_other, pair, *from_z = lax.optimization_barrier(
        (arrived, upstream_other, pair, *from_z)
    )
    by_z = jnp.stack([*from_z[::-1], pair])
    side_all = lax.dynamic_slice_in_dim(
        jnp.concatenate([by_z, by_z]), n_z - 1 - lax.axis_index("z"), n_z, 0
    )
    recv_plan = lax.dynamic_index_in_dim(plan, sender, 1, keepdims=False)
    recv_end = jnp.cumsum(recv_plan)
    frame_index = jnp.arange(rows_dev, dtype=jnp.int32)
    before = recv_end[None, :] <= frame_index[:, None]
    source_dev = jnp.sum(before.astype(jnp.int32), axis=1)
    start_of = jnp.sum(jnp.where(before, recv_plan[None, :], 0), axis=1)
    place = source_dev * 2 * capacity + frame_index - start_of
    frames, last, first = kernel_call(
        receive_kernel,
        (
            jax.ShapeDtypeStruct((rows_dev, width), jnp.bfloat16),
            jax.ShapeDtypeStruct((slabs, 3 * EDGE, width), jnp.bfloat16),
            jax.ShapeDtypeStruct((slabs, 3 * EDGE, width), jnp.bfloat16),
        ),
        [],
        4 * devices * capacity * rows_dev * width,
        jnp.stack([place, place + capacity], axis=1), arrived, upstream,
    )
    low, high = to_neighbours(last, first, n_seq)
    side = side_all.reshape(width, LANES)[:, : kernel_len + 2].astype(jnp.float32).T
    gain_pre, gain_mid = side[kernel_len], side[kernel_len + 1]
    taps = jnp.pad(side[:kernel_len], ((0, 1), (0, 0)))
    taps = taps.reshape(kernel_len + 1, width // LANES, LANES).transpose(1, 0, 2)

    id_pad = jnp.pad(segment_ids, ((0, 0), (2 * EDGE, 2 * EDGE)), constant_values=-1)
    window = lax.dynamic_slice_in_dim(
        id_pad, lax.axis_index(SEQ) * frames_dev, frames_dev + 4 * EDGE, 1
    )
    ids = jnp.broadcast_to(window[:, :, None], (*window.shape, LANES))

    frame_rows = frames.astype(jnp.float32)
    _, pull_pre = jax.vjp(norm_rows, frame_rows, gain_pre)
    padded = frames_dev + 4 * EDGE
    normed_wide, normed, upstream_wide = kernel_call(
        norm_kernel,
        (
            jax.ShapeDtypeStruct((slabs, padded, width), jnp.bfloat16),
            jax.ShapeDtypeStruct((rows_dev, width), jnp.bfloat16),
            jax.ShapeDtypeStruct((slabs * (frames_dev + 2 * EDGE), width), jnp.bfloat16),
        ),
        [],
        rows_dev * width * 10,
        frames, low, high, upstream, gain_pre[None],
    )
    normed_other = lax.ppermute(normed, "core", swap)
    lin, sig, gated = project(normed_wide.reshape(-1, width), in_full)
    gated, normed_other = lax.optimization_barrier((gated, normed_other))
    gated = gated.reshape(slabs, padded, width)
    elements = rows_dev * width
    wide = frames_dev + 2 * EDGE
    blocks = width // LANES
    activated, normed_mid, scale_mid = kernel_call(
        forward_kernel,
        (
            jax.ShapeDtypeStruct((rows_dev, width), jnp.bfloat16),
            jax.ShapeDtypeStruct((slabs * wide, width), jnp.float32),
            jax.ShapeDtypeStruct((slabs * wide, LANES), jnp.float32),
        ),
        [
            pltpu.VMEM((blocks, padded, LANES), jnp.float32),
            pltpu.VMEM((blocks, wide, LANES), jnp.float32),
        ],
        elements * 3 * kernel_len,
        gated, ids, taps, gain_mid[None],
    )
    act_other = lax.ppermute(activated, "core", swap)
    grad_mixing, grad_gain_mid = kernel_call(
        middle_kernel,
        (
            jax.ShapeDtypeStruct((slabs, wide, width), jnp.float32),
            jax.ShapeDtypeStruct((8, width), jnp.float32),
        ),
        [pltpu.VMEM((slabs * wide, width), jnp.float32)],
        2 * slabs * wide * width * width,
        normed_mid, scale_mid, upstream_wide, out_full, gain_mid[None],
    )

    def exchanged(part):
        return lax.all_to_all(
            part.reshape(n_z * n_seq, LANES // n_seq, part.shape[1]), ZXY, 0, 0, tiled=True
        )

    core_ref = core[None].astype(jnp.int32)
    out_part = weight_part(core_ref, activated, act_other, upstream_rows, upstream_other)
    out_parts = exchanged(out_part)
    out_sum = jnp.sum(out_parts.astype(jnp.float32), axis=0)
    projected = jnp.dot(activated, out_full, preferred_element_type=jnp.float32)
    encoded = (frame_rows + projected).astype(jnp.bfloat16).reshape(slabs, frames_dev, width)

    grad_hidden, grad_taps = kernel_call(
        backward_kernel,
        (
            jax.ShapeDtypeStruct((rows_dev, 2 * width), jnp.bfloat16),
            jax.ShapeDtypeStruct((kernel_len + 9, width), jnp.float32),
        ),
        [
            pltpu.VMEM((blocks, wide, LANES), jnp.float32),
            pltpu.VMEM((blocks, kernel_len, 8, LANES), jnp.float32),
        ],
        elements * 5 * kernel_len,
        grad_mixing, gated, ids, taps, lin, sig, grad_gain_mid,
    )
    hidden_other = lax.ppermute(grad_hidden, "core", swap)
    small_other = lax.ppermute(grad_taps, "core", swap)
    in_part = weight_part(
        core_ref, normed, normed_other, grad_hidden, hidden_other, grad_taps, small_other
    )
    in_parts = exchanged(in_part)
    grad_normed = lax.dot_general(
        grad_hidden, in_full, (((1,), (1,)), ((), ())), preferred_element_type=jnp.float32
    )
    grad_rows, _ = pull_pre(grad_normed)
    grad_frames = (
        (upstream_rows.astype(jnp.float32) + grad_rows)
        .astype(jnp.bfloat16)
        .reshape(slabs, frames_dev, width)
    )
    share = LANES // n_seq
    start = lax.axis_index(SEQ) * share
    own_weight = lax.dynamic_slice_in_dim(in_weight, start, share, 0).astype(jnp.float32)
    own_gain = lax.dynamic_slice_in_dim(norm_gains, start, share, 0)[:, :1].astype(jnp.float32)
    total = kernel_call(
        functools.partial(
            total_kernel, tap=kernel_len, scale=1.0 / math.sqrt(devices * rows_dev)
        ),
        jax.ShapeDtypeStruct((n_seq, share, 3 * width + SMALL), jnp.bfloat16),
        [pltpu.VMEM((share, 2 * width + SMALL), jnp.float32)],
        in_parts.size,
        in_parts, out_sum, own_weight, own_gain,
    )
    final = lax.all_to_all(total, SEQ, 0, 0, tiled=True).reshape(LANES, -1)
    grad_in, grad_out, grad_kernel, grad_gains = kernel_call(
        finish_kernel,
        (
            jax.ShapeDtypeStruct((LANES, 2 * width), jnp.float32),
            jax.ShapeDtypeStruct((LANES, width), jnp.float32),
            jax.ShapeDtypeStruct((kernel_len, LANES), jnp.float32),
            jax.ShapeDtypeStruct((2, LANES), jnp.float32),
        ),
        [],
        LANES * width,
        final,
    )
    return encoded, grad_frames, grad_in, grad_out, grad_kernel.T, grad_gains.T


def solution(mesh):
    n_dp, n_seq = mesh.devices.shape
    side = math.isqrt(n_seq)
    split = Mesh(mesh.devices.reshape(n_dp // 2, 2, side, side), ("z", "core", "x", "y"))
    placed = (
        P((*DP, *SEQ), None),
        P(),
        P(DP, None),
        P(DP, None),
        P(DP, None),
        P(DP, None),
        P(DP, None),
        P(DP, SEQ, None),
    )
    return jax.shard_map(
        per_device,
        mesh=split,
        in_specs=placed,
        out_specs=(
            P(DP, SEQ, None),
            P(DP, SEQ, None),
            P(DP, None),
            P(DP, None),
            P(DP, None),
            P(DP, None),
        ),
        check_vma=False,
    )
```

```python
import functools
import math

import jax
import jax.numpy as jnp
from jax import lax
from jax.experimental import pallas as pl
from jax.experimental.pallas import tpu as pltpu
from jax.sharding import Mesh, PartitionSpec as P


DP = ("z", "core")
SEQ = ("x", "y")
ZXY = ("z", "x", "y")
EDGE = 16
LANES = 128
ROWS_STEP = 32
EPS = 1e-05
SMALL = LANES
VMEM_GRANT = 16 * 1024 * 1024


def forward_kernel(
    gated_ref, ids_ref, taps_ref, gain_ref,
    act_ref, normed_ref, pad_ref, mix_ref,
):
    slabs, padded, width = gated_ref.shape
    blocks = width // LANES
    taps_count = taps_ref.shape[1] - 1
    wide = padded - 2 * EDGE
    own = wide - 2 * EDGE
    shift = EDGE - taps_count // 2

    def one_slab(s, carry):
        for b in range(blocks):
            pad_ref[b] = gated_ref[s, :, b * LANES : (b + 1) * LANES].astype(jnp.float32)

        def conv_step(i, carry):
            row = pl.multiple_of((i // (blocks // 2)) * ROWS_STEP, ROWS_STEP)
            b = (i % (blocks // 2)) * 2
            center = ids_ref[s, pl.ds(row + EDGE, ROWS_STEP)]
            sums = [jnp.zeros((ROWS_STEP, LANES), jnp.float32) for _ in range(2)]
            for k in range(taps_count):
                same = ids_ref[s, pl.ds(row + k + shift, ROWS_STEP)] == center
                for j in range(2):
                    term = pad_ref[b + j, pl.ds(row + k + shift, ROWS_STEP)]
                    sums[j] = sums[j] + jnp.where(same, term, 0.0) * taps_ref[b + j, k : k + 1, :]
            for j in range(2):
                mix_ref[b + j, pl.ds(row, ROWS_STEP)] = sums[j]
            return carry

        lax.fori_loop(0, (wide // ROWS_STEP) * (blocks // 2), conv_step, 0)

        def row_step(i, own_rows):
            row = pl.multiple_of(i * 16, 16)
            out_row = pl.multiple_of(s * wide + i * 16, 16)
            mixing = jnp.concatenate([mix_ref[b, pl.ds(row, 16)] for b in range(blocks)], axis=1)
            centered = mixing - jnp.mean(mixing, axis=-1, keepdims=True)
            scale = lax.rsqrt(jnp.mean(centered * centered, axis=-1, keepdims=True) + EPS)
            normed = centered * scale
            if own_rows:
                act_row = pl.multiple_of(s * own + i * 16 - EDGE, 16)
                value = normed * gain_ref[0:1, :]
                act_ref[pl.ds(act_row, 16), :] = (value * jax.nn.sigmoid(value)).astype(
                    act_ref.dtype
                )
            normed_ref[pl.ds(out_row, 16), :width] = normed
            normed_ref[pl.ds(out_row, 16), width:] = jnp.broadcast_to(scale, (16, LANES))

        steps = wide // 16
        row_step(0, False)
        row_step(steps - 1, False)

        def own_step(i, carry):
            row_step(i + 1, True)
            return carry

        return lax.fori_loop(0, steps - 2, own_step, carry, unroll=4)

    lax.fori_loop(0, slabs, one_slab, 0)


def middle_kernel(
    normed_ref, upstream_ref, weight_ref, gain_ref,
    grad_mix_ref, grad_gain_ref, grad_act_ref, up_ref, loaded_ref, arrivals,
):
    slabs, frames, width = grad_mix_ref.shape
    steps = frames // 16
    parts, depth, _ = loaded_ref.shape
    up_copy = pltpu.make_async_copy(upstream_ref, up_ref, arrivals.at[parts])
    up_copy.start()
    copies = [
        pltpu.make_async_copy(
            weight_ref.at[pl.ds(h * depth, depth)], loaded_ref.at[h], arrivals.at[h]
        )
        for h in range(parts)
    ]
    for copy in copies:
        copy.start()
    up_copy.wait()
    for h, copy in enumerate(copies):
        copy.wait()
        grad_act_ref[:, h * depth : (h + 1) * depth] = lax.dot_general(
            up_ref[...],
            loaded_ref[h],
            (((1,), (1,)), ((), ())),
            preferred_element_type=jnp.float32,
        )

    def row_step(i, total):
        row = pl.multiple_of(i * 16, 16)
        normed = normed_ref[pl.ds(row, 16), :width]
        scale = normed_ref[pl.ds(row, 16), width : width + 1]
        gain = gain_ref[0:1, :]
        value = normed * gain
        sig = jax.nn.sigmoid(value)
        grad_value = grad_act_ref[pl.ds(row, 16), :] * (sig * (1.0 + value * (1.0 - sig)))
        part = grad_value * normed
        at = i % steps
        own = jnp.logical_and(at > 0, at < steps - 1)
        total = total + jnp.where(own, part[0:8] + part[8:16], 0.0)
        grad_normed = grad_value * gain
        first = jnp.mean(grad_normed, axis=-1, keepdims=True)
        second = jnp.mean(grad_normed * normed, axis=-1, keepdims=True)
        grad_mix_ref[i // steps, pl.ds(pl.multiple_of((i % steps) * 16, 16), 16), :] = scale * (
            grad_normed - first - normed * second
        )
        return total

    grad_gain_ref[...] = lax.fori_loop(
        0, slabs * steps, row_step, jnp.zeros(grad_gain_ref.shape, jnp.float32), unroll=4
    )


def backward_kernel(
    grad_mix_ref, gated_ref, ids_ref, taps_ref, lin_ref, sig_ref, grad_gain_ref,
    grad_hidden_ref, grad_taps_ref, pad_ref, sum_ref,
):
    slabs, padded, width = gated_ref.shape
    frames = padded - 4 * EDGE
    blocks = width // LANES
    taps_count = taps_ref.shape[1] - 1
    half = taps_count // 2
    sum_ref[...] = jnp.zeros(sum_ref.shape, jnp.float32)

    def one_slab(s, carry):
        for b in range(blocks):
            pad_ref[b] = grad_mix_ref[s, :, b * LANES : (b + 1) * LANES]

        def conv_step(i, carry):
            row = pl.multiple_of((i // (blocks // 2)) * ROWS_STEP, ROWS_STEP)
            out_row = pl.multiple_of(s * frames + row, ROWS_STEP)
            b = (i % (blocks // 2)) * 2
            hid_row = pl.multiple_of(s * padded + 2 * EDGE + row, ROWS_STEP)
            center = ids_ref[s, pl.ds(row + 2 * EDGE, ROWS_STEP)]
            sums = [jnp.zeros((ROWS_STEP, LANES), jnp.float32) for _ in range(2)]
            cols = [pl.ds(pl.multiple_of((b + j) * LANES, LANES), LANES) for j in range(2)]
            here = [gated_ref[s, pl.ds(row + 2 * EDGE, ROWS_STEP), cols[j]].astype(jnp.float32) for j in range(2)]
            for k in range(taps_count):
                at = row + EDGE + half - k
                same = ids_ref[s, pl.ds(at + EDGE, ROWS_STEP)] == center
                for j in range(2):
                    term = jnp.where(same, pad_ref[b + j, pl.ds(at, ROWS_STEP)], 0.0)
                    sums[j] = sums[j] + term * taps_ref[b + j, k : k + 1, :]
                    part = term * here[j]
                    sum_ref[b + j, k] = sum_ref[b + j, k] + (
                        (part[0:8] + part[8:16]) + (part[16:24] + part[24:32])
                    )
            for j in range(2):
                lin = lin_ref[pl.ds(hid_row, ROWS_STEP), cols[j]]
                sig = sig_ref[pl.ds(hid_row, ROWS_STEP), cols[j]]
                grad_lin = sums[j] * sig
                grad_hidden_ref[pl.ds(out_row, ROWS_STEP), cols[j]] = grad_lin.astype(jnp.bfloat16)
                grad_hidden_ref[
                    pl.ds(out_row, ROWS_STEP),
                    pl.ds(pl.multiple_of(width + (b + j) * LANES, LANES), LANES),
                ] = (grad_lin * lin * (1.0 - sig)).astype(jnp.bfloat16)
            return carry

        return lax.fori_loop(0, (frames // ROWS_STEP) * (blocks // 2), conv_step, carry)

    lax.fori_loop(0, slabs, one_slab, 0)
    for b in range(blocks):
        for k in range(taps_count):
            grad_taps_ref[k : k + 1, b * LANES : (b + 1) * LANES] = jnp.sum(
                sum_ref[b, k], axis=0, keepdims=True
            )
    grad_taps_ref[taps_count:, :] = jnp.zeros(
        (grad_taps_ref.shape[0] - taps_count, width), jnp.float32
    )
    grad_taps_ref[taps_count + 1 : taps_count + 2, :] = jnp.sum(
        grad_gain_ref[...], axis=0, keepdims=True
    )


def send_kernel(index_ref, rows_ref, out_ref):
    rows, width = rows_ref.shape
    pick = (lax.broadcasted_iota(jnp.int32, (index_ref.shape[0], rows), 1) == index_ref[...])
    pick = pick.astype(jnp.float32).astype(jnp.bfloat16)
    for h in range(2):
        part = jnp.dot(
            pick,
            rows_ref[:, h * (width // 2) : (h + 1) * (width // 2)],
            preferred_element_type=jnp.float32,
        )
        slots = part.shape[0] // out_ref.shape[0]
        out_ref[:, h * slots : (h + 1) * slots, :] = part.astype(jnp.bfloat16).reshape(
            out_ref.shape[0], slots, width // 2
        )


def receive_kernel(index_ref, arrived_ref, upstream_ref, out_ref, last_ref, first_ref):
    slots, half = arrived_ref.shape
    slabs, frames, _ = upstream_ref.shape
    reach = 2 * EDGE
    columns = lax.broadcasted_iota(jnp.int32, (index_ref.shape[0], slots), 1)
    for h in range(2):
        pick = (columns == index_ref[:, h : h + 1]).astype(jnp.float32).astype(jnp.bfloat16)
        rows = jnp.dot(pick, arrived_ref[...], preferred_element_type=jnp.float32)
        rows = rows.astype(jnp.bfloat16)
        cols = slice(h * half, (h + 1) * half)
        out_ref[:, cols] = rows
        for s in range(slabs):
            last_ref[s, :reach, cols] = rows[(s + 1) * frames - reach : (s + 1) * frames]
            first_ref[s, :reach, cols] = rows[s * frames : s * frames + reach]
    for s in range(slabs):
        last_ref[s, reach:, :] = upstream_ref[s, frames - EDGE :, :]
        first_ref[s, reach:, :] = upstream_ref[s, :EDGE, :]


def total_kernel(
    parts_ref, out_sum_ref, weight_ref, gain_ref, total_ref, sum_ref, tile_ref, leaving, *, tap, scale
):
    count, share, width = parts_ref.shape
    in_width = weight_ref.shape[1]
    grad_gain = jnp.zeros((share, 1), jnp.float32)
    for at in range(0, width, SMALL):
        cols = slice(at, at + SMALL)
        part = jnp.zeros((share, SMALL), jnp.float32)
        for j in range(0, count, 16):
            part = part + jnp.sum(parts_ref[j : j + 16, :, cols].astype(jnp.float32), axis=0)
        sum_ref[:, cols] = part
        if at < in_width:
            grad_gain = grad_gain + jnp.sum(part * weight_ref[:, cols], axis=1, keepdims=True)
    small = sum_ref[:, in_width:]
    column = lax.broadcasted_iota(jnp.int32, small.shape, 1)
    sum_ref[:, in_width:] = jnp.where(column == tap, grad_gain / gain_ref[...], small)
    tile_ref[0, :, :width] = (sum_ref[...] * scale).astype(jnp.bfloat16)
    tile_ref[0, :, width:] = (out_sum_ref[...] * scale).astype(jnp.bfloat16)
    copies = [
        pltpu.make_async_copy(tile_ref, total_ref.at[pl.ds(i, 1)], leaving.at[i])
        for i in range(total_ref.shape[0])
    ]
    for copy in copies:
        copy.start()
    for copy in copies:
        copy.wait()


def finish_kernel(final_ref, grad_in_ref, grad_out_ref, grad_taps_ref, grad_gains_ref):
    in_width, taps_count = grad_in_ref.shape[1], grad_taps_ref.shape[0]
    grad_in_ref[...] = final_ref[:, :in_width].astype(jnp.float32)
    grad_out_ref[...] = final_ref[:, in_width + SMALL :].astype(jnp.float32)
    small = final_ref[:, in_width : in_width + LANES].astype(jnp.float32).T
    grad_taps_ref[...] = small[:taps_count]
    grad_gains_ref[...] = small[taps_count : taps_count + 2]


def product_kernel(core_ref, left_ref, left_other_ref, right_ref, right_other_ref, *rest):
    small_refs, out_ref, turned_ref = rest[:-2], rest[-2], rest[-1]
    rows, channels = left_ref.shape
    width = right_ref.shape[1]
    step = 512
    picks = [
        pl.ds(pl.multiple_of((2 * z + core_ref[0]) * LANES, LANES), LANES)
        for z in range(channels // LANES // 2)
    ]
    for z, pick in enumerate(picks):
        for h, ref in enumerate((left_ref, left_other_ref)):
            turned_ref[z * LANES : (z + 1) * LANES, h * rows : (h + 1) * rows] = ref[:, pick].T
    for at in range(0, width, step):
        right = jnp.concatenate(
            [right_ref[:, at : at + step], right_other_ref[:, at : at + step]], axis=0
        )
        out_ref[:, at : at + step] = jnp.dot(
            turned_ref[...], right, preferred_element_type=jnp.float32
        ).astype(out_ref.dtype)
    if small_refs:
        for z, pick in enumerate(picks):
            small = small_refs[0][:, pick] + small_refs[1][:, pick]
            filled = jnp.concatenate(
                [small, jnp.zeros((LANES - small.shape[0], LANES), jnp.float32)], axis=0
            )
            block = slice(z * LANES, (z + 1) * LANES)
            out_ref[block, width : width + LANES] = filled.T.astype(out_ref.dtype)


def weight_part(core, left, left_other, right, right_other, *small):
    rows, channels = left.shape
    mine = channels // LANES // 2
    width = right.shape[1]
    out_width = width + (SMALL if small else 0)
    vmem = pl.BlockSpec(memory_space=pltpu.VMEM)
    return pl.pallas_call(
        product_kernel,
        out_shape=jax.ShapeDtypeStruct((mine * LANES, out_width), jnp.bfloat16),
        in_specs=[pl.BlockSpec(memory_space=pltpu.SMEM)] + [vmem] * (4 + len(small)),
        out_specs=vmem,
        scratch_shapes=[pltpu.VMEM((mine * LANES, 2 * rows), jnp.bfloat16)],
        name="weight_part",
        compiler_params=pltpu.CompilerParams(vmem_limit_bytes=VMEM_GRANT),
        cost_estimate=pl.CostEstimate(
            flops=4 * rows * mine * LANES * width,
            bytes_accessed=4 * rows * (channels + width),
            transcendentals=0,
        ),
    )(core, left, left_other, right, right_other, *small)


def norm_kernel(
    frames_ref, low_ref, high_ref, upstream_ref, gain_ref, wide_ref, own_ref, up_wide_ref
):
    slabs, padded, _ = wide_ref.shape
    reach = 2 * EDGE
    own = padded - 2 * reach

    def normed_rows(rows):
        values = rows.astype(jnp.float32)
        centered = values - jnp.mean(values, axis=-1, keepdims=True)
        spread_ = jnp.mean(centered * centered, axis=-1, keepdims=True)
        return (centered * lax.rsqrt(spread_ + EPS) * gain_ref[0:1, :]).astype(jnp.bfloat16)

    for s in range(slabs):
        for at in range(0, reach, 16):
            wide_ref[s, at : at + 16, :] = normed_rows(low_ref[s, at : at + 16, :])
            high_at = reach + own + at
            wide_ref[s, high_at : high_at + 16, :] = normed_rows(high_ref[s, at : at + 16, :])

    def step(i, carry):
        row = pl.multiple_of(i * 16, 16)
        rows = normed_rows(frames_ref[pl.ds(row, 16), :])
        own_ref[pl.ds(row, 16), :] = rows
        steps = own // 16
        wide_ref[i // steps, pl.ds(pl.multiple_of(reach + (i % steps) * 16, 16), 16), :] = rows
        return carry

    lax.fori_loop(0, slabs * own // 16, step, 0, unroll=4)
    for s in range(slabs):
        base = s * (own + 2 * EDGE)
        up_wide_ref[base : base + EDGE, :] = low_ref[s, reach:, :]
        up_wide_ref[base + EDGE : base + EDGE + own, :] = upstream_ref[s]
        up_wide_ref[base + EDGE + own : base + 2 * EDGE + own, :] = high_ref[s, reach:, :]


def project_kernel(normed_ref, weight_ref, lin_ref, sig_ref, gated_ref, loaded_ref, arrivals):
    parts, depth, both = loaded_ref.shape
    width = both // 2
    step = 256
    copies = [
        pltpu.make_async_copy(
            weight_ref.at[pl.ds(h * depth, depth)], loaded_ref.at[h], arrivals.at[h]
        )
        for h in range(parts)
    ]
    for copy in copies:
        copy.start()
    for h, copy in enumerate(copies):
        copy.wait()
        rows = normed_ref[:, h * depth : (h + 1) * depth]
        for at in range(0, width, step):
            cols = slice(at, at + step)
            lin = jnp.dot(rows, loaded_ref[h, :, cols], preferred_element_type=jnp.float32)
            gate = jnp.dot(
                rows,
                loaded_ref[h, :, width + at : width + at + step],
                preferred_element_type=jnp.float32,
            )
            if h > 0:
                lin = lin + lin_ref[:, cols]
                gate = gate + sig_ref[:, cols]
            if h == parts - 1:
                gate = jax.nn.sigmoid(gate)
                gated_ref[:, cols] = (lin * gate).astype(jnp.bfloat16)
            lin_ref[:, cols] = lin
            sig_ref[:, cols] = gate


def project(normed, weight):
    rows, width = normed.shape
    parts = 2
    vmem = pl.BlockSpec(memory_space=pltpu.VMEM)
    return pl.pallas_call(
        project_kernel,
        out_shape=(
            jax.ShapeDtypeStruct((rows, width), jnp.float32),
            jax.ShapeDtypeStruct((rows, width), jnp.float32),
            jax.ShapeDtypeStruct((rows, width), jnp.bfloat16),
        ),
        in_specs=[vmem, pl.BlockSpec(memory_space=pltpu.HBM)],
        out_specs=(vmem, vmem, vmem),
        scratch_shapes=[
            pltpu.VMEM((parts, width // parts, 2 * width), jnp.bfloat16),
            pltpu.SemaphoreType.DMA((parts,)),
        ],
        name="project",
        compiler_params=pltpu.CompilerParams(vmem_limit_bytes=VMEM_GRANT),
        cost_estimate=pl.CostEstimate(
            flops=4 * rows * width * width,
            bytes_accessed=4 * width * width,
            transcendentals=rows * width,
        ),
    )(normed, pltpu.with_memory_space_constraint(weight, pltpu.HBM))


def kernel_call(body, outs, scratch, flops, *args, in_hbm=(), out_hbm=False):
    moved = sum(a.size * a.dtype.itemsize for a in args)
    specs = {}
    if in_hbm:
        specs["in_specs"] = [
            pl.BlockSpec(memory_space=pltpu.HBM if i in in_hbm else pltpu.VMEM)
            for i in range(len(args))
        ]
    if out_hbm:
        specs["out_specs"] = pl.BlockSpec(memory_space=pltpu.HBM)
        outs = pltpu.HBM(outs.shape, outs.dtype)
    args = [
        pltpu.with_memory_space_constraint(a, pltpu.HBM) if i in in_hbm else a
        for i, a in enumerate(args)
    ]
    return pl.pallas_call(
        body,
        out_shape=outs,
        scratch_shapes=scratch,
        compiler_params=pltpu.CompilerParams(vmem_limit_bytes=VMEM_GRANT),
        cost_estimate=pl.CostEstimate(flops=flops, bytes_accessed=moved, transcendentals=0),
        **specs,
    )(*args)


def to_neighbours(last, first, count):
    forward = [(i, i + 1) for i in range(count - 1)]
    backward = [(i + 1, i) for i in range(count - 1)]
    return lax.ppermute(last, SEQ, forward), lax.ppermute(first, SEQ, backward)


def norm_rows(values, gain):
    average = jnp.mean(values, axis=-1, keepdims=True)
    centered = values - average
    spread_ = jnp.mean(centered * centered, axis=-1, keepdims=True)
    return centered * lax.rsqrt(spread_ + EPS) * gain


def per_device(
    loaded, plan, segment_ids, in_weight, out_weight, depth_kernel, norm_gains, upstream
):
    rows_dev, width = loaded.shape
    devices = plan.shape[0]
    capacity = 2 * rows_dev // devices
    slabs, slab_len = segment_ids.shape
    n_seq = lax.axis_size(SEQ)
    n_z = lax.axis_size("z")
    frames_dev = slab_len // n_seq
    kernel_len = depth_kernel.shape[1]
    core = lax.axis_index("core")
    sender = lax.axis_index((*DP, *SEQ))
    swap = [(0, 1), (1, 0)]

    in_full = lax.all_gather(in_weight, DP, axis=0, tiled=True)
    out_full = lax.all_gather(out_weight, DP, axis=0, tiled=True)

    send_plan = lax.dynamic_index_in_dim(plan, sender, 0, keepdims=False)
    send_start = jnp.cumsum(send_plan) - send_plan
    slot_index = jnp.arange(capacity, dtype=jnp.int32)
    source_rows = jnp.minimum(send_start[:, None] + slot_index[None, :], rows_dev - 1)
    outgoing = kernel_call(
        send_kernel,
        jax.ShapeDtypeStruct((devices, 2 * capacity, width // 2), jnp.bfloat16),
        [],
        4 * devices * capacity * rows_dev * width,
        source_rows.reshape(-1, 1), loaded,
    )
    arrived = lax.all_to_all(
        outgoing, (*DP, *SEQ), split_axis=0, concat_axis=0, tiled=True
    ).reshape(devices * 2 * capacity, width // 2)
    extras = jnp.pad(
        jnp.concatenate([depth_kernel, norm_gains], axis=1), ((0, 0), (0, LANES - kernel_len - 2))
    )
    upstream_rows = upstream.reshape(rows_dev, width)
    extras_other = lax.ppermute(extras, "core", swap)
    pair = jnp.where(
        core == 0, jnp.stack([extras, extras_other]), jnp.stack([extras_other, extras])
    )
    from_z = [
        lax.ppermute(pair, "z", [(i, (i + d) % n_z) for i in range(n_z)])
        for d in range(1, n_z)
    ]
    upstream_other = lax.ppermute(upstream_rows, "core", swap)
    arrived, upstream_other, pair = lax.optimization_barrier((arrived, upstream_other, pair))
    by_z = jnp.stack([*from_z[::-1], pair])
    side_all = lax.dynamic_slice_in_dim(
        jnp.concatenate([by_z, by_z]), n_z - 1 - lax.axis_index("z"), n_z, 0
    )
    recv_plan = lax.dynamic_index_in_dim(plan, sender, 1, keepdims=False)
    recv_end = jnp.cumsum(recv_plan)
    frame_index = jnp.arange(rows_dev, dtype=jnp.int32)
    before = recv_end[None, :] <= frame_index[:, None]
    source_dev = jnp.sum(before.astype(jnp.int32), axis=1)
    start_of = jnp.sum(jnp.where(before, recv_plan[None, :], 0), axis=1)
    place = source_dev * 2 * capacity + frame_index - start_of
    frames, last, first = kernel_call(
        receive_kernel,
        (
            jax.ShapeDtypeStruct((rows_dev, width), jnp.bfloat16),
            jax.ShapeDtypeStruct((slabs, 3 * EDGE, width), jnp.bfloat16),
            jax.ShapeDtypeStruct((slabs, 3 * EDGE, width), jnp.bfloat16),
        ),
        [],
        4 * devices * capacity * rows_dev * width,
        jnp.stack([place, place + capacity], axis=1), arrived, upstream,
    )
    low, high = to_neighbours(last, first, n_seq)
    side = side_all.reshape(width, LANES)[:, : kernel_len + 2].astype(jnp.float32).T
    gain_pre, gain_mid = side[kernel_len], side[kernel_len + 1]
    taps = jnp.pad(side[:kernel_len], ((0, 1), (0, 0)))
    taps = taps.reshape(kernel_len + 1, width // LANES, LANES).transpose(1, 0, 2)

    id_pad = jnp.pad(segment_ids, ((0, 0), (2 * EDGE, 2 * EDGE)), constant_values=-1)
    window = lax.dynamic_slice_in_dim(
        id_pad, lax.axis_index(SEQ) * frames_dev, frames_dev + 4 * EDGE, 1
    )
    ids = jnp.broadcast_to(window[:, :, None], (*window.shape, LANES))

    frame_rows = frames.astype(jnp.float32)
    _, pull_pre = jax.vjp(norm_rows, frame_rows, gain_pre)
    padded = frames_dev + 4 * EDGE
    normed_wide, normed, upstream_wide = kernel_call(
        norm_kernel,
        (
            jax.ShapeDtypeStruct((slabs, padded, width), jnp.bfloat16),
            jax.ShapeDtypeStruct((rows_dev, width), jnp.bfloat16),
            jax.ShapeDtypeStruct((slabs * (frames_dev + 2 * EDGE), width), jnp.bfloat16),
        ),
        [],
        rows_dev * width * 10,
        frames, low, high, upstream, gain_pre[None],
    )
    normed_other = lax.ppermute(normed, "core", swap)
    lin, sig, gated = project(normed_wide.reshape(-1, width), in_full)
    gated, normed_other = lax.optimization_barrier((gated, normed_other))
    gated = gated.reshape(slabs, padded, width)
    elements = rows_dev * width
    wide = frames_dev + 2 * EDGE
    blocks = width // LANES
    activated, normed_mid = kernel_call(
        forward_kernel,
        (
            jax.ShapeDtypeStruct((rows_dev, width), jnp.bfloat16),
            jax.ShapeDtypeStruct((slabs * wide, width + LANES), jnp.float32),
        ),
        [
            pltpu.VMEM((blocks, padded, LANES), jnp.float32),
            pltpu.VMEM((blocks, wide, LANES), jnp.float32),
        ],
        elements * 3 * kernel_len,
        gated, ids, taps, gain_mid[None],
    )
    act_other = lax.ppermute(activated, "core", swap)
    grad_mixing, grad_gain_mid = kernel_call(
        middle_kernel,
        (
            jax.ShapeDtypeStruct((slabs, wide, width), jnp.float32),
            jax.ShapeDtypeStruct((8, width), jnp.float32),
        ),
        [
            pltpu.VMEM((slabs * wide, width), jnp.float32),
            pltpu.VMEM((slabs * wide, width), jnp.bfloat16),
            pltpu.VMEM((4, width // 4, width), jnp.bfloat16),
            pltpu.SemaphoreType.DMA((5,)),
        ],
        2 * slabs * wide * width * width,
        normed_mid, upstream_wide, out_full, gain_mid[None],
        in_hbm=(1, 2),
    )

    def exchanged(part):
        return lax.all_to_all(
            part.reshape(n_z * n_seq, LANES // n_seq, part.shape[1]), ZXY, 0, 0, tiled=True
        )

    core_ref = core[None].astype(jnp.int32)
    out_part = weight_part(core_ref, activated, act_other, upstream_rows, upstream_other)
    out_parts = exchanged(out_part)
    out_sum = jnp.sum(out_parts.astype(jnp.float32), axis=0)
    projected = jnp.dot(activated, out_full, preferred_element_type=jnp.float32)
    encoded = (frame_rows + projected).astype(jnp.bfloat16).reshape(slabs, frames_dev, width)

    grad_hidden, grad_taps = kernel_call(
        backward_kernel,
        (
            jax.ShapeDtypeStruct((rows_dev, 2 * width), jnp.bfloat16),
            jax.ShapeDtypeStruct((kernel_len + 9, width), jnp.float32),
        ),
        [
            pltpu.VMEM((blocks, wide, LANES), jnp.float32),
            pltpu.VMEM((blocks, kernel_len, 8, LANES), jnp.float32),
        ],
        elements * 5 * kernel_len,
        grad_mixing, gated, ids, taps, lin, sig, grad_gain_mid,
    )
    hidden_other = lax.ppermute(grad_hidden, "core", swap)
    small_other = lax.ppermute(grad_taps, "core", swap)
    in_part = weight_part(
        core_ref, normed, normed_other, grad_hidden, hidden_other, grad_taps, small_other
    )
    in_parts = exchanged(in_part)
    grad_normed = lax.dot_general(
        grad_hidden, in_full, (((1,), (1,)), ((), ())), preferred_element_type=jnp.float32
    )
    grad_rows, _ = pull_pre(grad_normed)
    grad_frames = (
        (upstream_rows.astype(jnp.float32) + grad_rows)
        .astype(jnp.bfloat16)
        .reshape(slabs, frames_dev, width)
    )
    share = LANES // n_seq
    start = lax.axis_index(SEQ) * share
    own_weight = lax.dynamic_slice_in_dim(in_weight, start, share, 0).astype(jnp.float32)
    own_gain = lax.dynamic_slice_in_dim(norm_gains, start, share, 0)[:, :1].astype(jnp.float32)
    total = kernel_call(
        functools.partial(
            total_kernel, tap=kernel_len, scale=1.0 / math.sqrt(devices * rows_dev)
        ),
        jax.ShapeDtypeStruct((n_seq, share, 3 * width + SMALL), jnp.bfloat16),
        [
            pltpu.VMEM((share, 2 * width + SMALL), jnp.float32),
            pltpu.VMEM((1, share, 3 * width + SMALL), jnp.bfloat16),
            pltpu.SemaphoreType.DMA((n_seq,)),
        ],
        in_parts.size,
        in_parts, out_sum, own_weight, own_gain,
        out_hbm=True,
    )
    final = lax.all_to_all(total, SEQ, 0, 0, tiled=True).reshape(LANES, -1)
    grad_in, grad_out, grad_kernel, grad_gains = kernel_call(
        finish_kernel,
        (
            jax.ShapeDtypeStruct((LANES, 2 * width), jnp.float32),
            jax.ShapeDtypeStruct((LANES, width), jnp.float32),
            jax.ShapeDtypeStruct((kernel_len, LANES), jnp.float32),
            jax.ShapeDtypeStruct((2, LANES), jnp.float32),
        ),
        [],
        LANES * width,
        final,
    )
    return encoded, grad_frames, grad_in, grad_out, grad_kernel.T, grad_gains.T


def solution(mesh):
    n_dp, n_seq = mesh.devices.shape
    side = math.isqrt(n_seq)
    split = Mesh(mesh.devices.reshape(n_dp // 2, 2, side, side), ("z", "core", "x", "y"))
    placed = (
        P((*DP, *SEQ), None),
        P(),
        P(DP, None),
        P(DP, None),
        P(DP, None),
        P(DP, None),
        P(DP, None),
        P(DP, SEQ, None),
    )
    return jax.shard_map(
        per_device,
        mesh=split,
        in_specs=placed,
        out_specs=(
            P(DP, SEQ, None),
            P(DP, SEQ, None),
            P(DP, None),
            P(DP, None),
            P(DP, None),
            P(DP, None),
        ),
        check_vma=False,
    )
```

```python
import functools
import math

import jax
import jax.numpy as jnp
from jax import lax
from jax.experimental import pallas as pl
from jax.experimental.pallas import tpu as pltpu
from jax.sharding import Mesh, PartitionSpec as P


DP = ("z", "core")
SEQ = ("x", "y")
ZXY = ("z", "x", "y")
EDGE = 16
LANES = 128
ROWS_STEP = 32
EPS = 1e-05
SMALL = LANES
VMEM_GRANT = 16 * 1024 * 1024


def forward_kernel(
    gated_ref, ids_ref, taps_ref, gain_ref,
    act_ref, normed_ref, pad_ref, mix_ref,
):
    slabs, padded, width = gated_ref.shape
    blocks = width // LANES
    taps_count = taps_ref.shape[1] - 1
    wide = padded - 2 * EDGE
    own = wide - 2 * EDGE
    shift = EDGE - taps_count // 2

    def one_slab(s, carry):
        for b in range(blocks):
            pad_ref[b] = gated_ref[s, :, b * LANES : (b + 1) * LANES].astype(jnp.float32)

        def conv_step(i, carry):
            row = pl.multiple_of((i // (blocks // 2)) * ROWS_STEP, ROWS_STEP)
            b = (i % (blocks // 2)) * 2
            center = ids_ref[s, pl.ds(row + EDGE, ROWS_STEP)]
            sums = [jnp.zeros((ROWS_STEP, LANES), jnp.float32) for _ in range(2)]
            for k in range(taps_count):
                same = ids_ref[s, pl.ds(row + k + shift, ROWS_STEP)] == center
                for j in range(2):
                    term = pad_ref[b + j, pl.ds(row + k + shift, ROWS_STEP)]
                    sums[j] = sums[j] + jnp.where(same, term, 0.0) * taps_ref[b + j, k : k + 1, :]
            for j in range(2):
                mix_ref[b + j, pl.ds(row, ROWS_STEP)] = sums[j]
            return carry

        lax.fori_loop(0, (wide // ROWS_STEP) * (blocks // 2), conv_step, 0)

        def row_step(i, own_rows):
            row = pl.multiple_of(i * 16, 16)
            out_row = pl.multiple_of(s * wide + i * 16, 16)
            mixing = jnp.concatenate([mix_ref[b, pl.ds(row, 16)] for b in range(blocks)], axis=1)
            centered = mixing - jnp.mean(mixing, axis=-1, keepdims=True)
            scale = lax.rsqrt(jnp.mean(centered * centered, axis=-1, keepdims=True) + EPS)
            normed = centered * scale
            if own_rows:
                act_row = pl.multiple_of(s * own + i * 16 - EDGE, 16)
                value = normed * gain_ref[0:1, :]
                act_ref[pl.ds(act_row, 16), :] = (value * jax.nn.sigmoid(value)).astype(
                    act_ref.dtype
                )
            normed_ref[pl.ds(out_row, 16), :width] = normed
            normed_ref[pl.ds(out_row, 16), width:] = jnp.broadcast_to(scale, (16, LANES))

        steps = wide // 16
        row_step(0, False)
        row_step(steps - 1, False)

        def own_step(i, carry):
            row_step(i + 1, True)
            return carry

        return lax.fori_loop(0, steps - 2, own_step, carry, unroll=4)

    lax.fori_loop(0, slabs, one_slab, 0)


def middle_kernel(
    normed_ref, upstream_ref, weight_ref, gain_ref,
    grad_mix_ref, grad_gain_ref, grad_act_ref, up_ref, loaded_ref, arrivals,
):
    slabs, frames, width = grad_mix_ref.shape
    steps = frames // 16
    parts, depth, _ = loaded_ref.shape
    up_copy = pltpu.make_async_copy(upstream_ref, up_ref, arrivals.at[parts])
    up_copy.start()
    copies = [
        pltpu.make_async_copy(
            weight_ref.at[pl.ds(h * depth, depth)], loaded_ref.at[h], arrivals.at[h]
        )
        for h in range(parts)
    ]
    for copy in copies:
        copy.start()
    up_copy.wait()
    for h, copy in enumerate(copies):
        copy.wait()
        grad_act_ref[:, h * depth : (h + 1) * depth] = lax.dot_general(
            up_ref[...],
            loaded_ref[h],
            (((1,), (1,)), ((), ())),
            preferred_element_type=jnp.float32,
        )

    def row_step(i, total):
        row = pl.multiple_of(i * 16, 16)
        normed = normed_ref[pl.ds(row, 16), :width]
        scale = normed_ref[pl.ds(row, 16), width : width + 1]
        gain = gain_ref[0:1, :]
        value = normed * gain
        sig = jax.nn.sigmoid(value)
        grad_value = grad_act_ref[pl.ds(row, 16), :] * (sig * (1.0 + value * (1.0 - sig)))
        part = grad_value * normed
        at = i % steps
        own = jnp.logical_and(at > 0, at < steps - 1)
        total = total + jnp.where(own, part[0:8] + part[8:16], 0.0)
        grad_normed = grad_value * gain
        first = jnp.mean(grad_normed, axis=-1, keepdims=True)
        second = jnp.mean(grad_normed * normed, axis=-1, keepdims=True)
        grad_mix_ref[i // steps, pl.ds(pl.multiple_of((i % steps) * 16, 16), 16), :] = scale * (
            grad_normed - first - normed * second
        )
        return total

    grad_gain_ref[...] = lax.fori_loop(
        0, slabs * steps, row_step, jnp.zeros(grad_gain_ref.shape, jnp.float32), unroll=4
    )


def backward_kernel(
    grad_mix_ref, gated_ref, ids_ref, taps_ref, lin_ref, sig_ref, grad_gain_ref,
    grad_hidden_ref, grad_taps_ref, pad_ref, sum_ref,
):
    slabs, padded, width = gated_ref.shape
    frames = padded - 4 * EDGE
    blocks = width // LANES
    taps_count = taps_ref.shape[1] - 1
    half = taps_count // 2
    sum_ref[...] = jnp.zeros(sum_ref.shape, jnp.float32)

    def one_slab(s, carry):
        for b in range(blocks):
            pad_ref[b] = grad_mix_ref[s, :, b * LANES : (b + 1) * LANES]

        def conv_step(i, carry):
            row = pl.multiple_of((i // (blocks // 2)) * ROWS_STEP, ROWS_STEP)
            out_row = pl.multiple_of(s * frames + row, ROWS_STEP)
            b = (i % (blocks // 2)) * 2
            center = ids_ref[s, pl.ds(row + 2 * EDGE, ROWS_STEP)]
            sums = [jnp.zeros((ROWS_STEP, LANES), jnp.float32) for _ in range(2)]
            cols = [pl.ds(pl.multiple_of((b + j) * LANES, LANES), LANES) for j in range(2)]
            here = [gated_ref[s, pl.ds(row + 2 * EDGE, ROWS_STEP), cols[j]].astype(jnp.float32) for j in range(2)]
            for k in range(taps_count):
                at = row + EDGE + half - k
                same = ids_ref[s, pl.ds(at + EDGE, ROWS_STEP)] == center
                for j in range(2):
                    term = jnp.where(same, pad_ref[b + j, pl.ds(at, ROWS_STEP)], 0.0)
                    sums[j] = sums[j] + term * taps_ref[b + j, k : k + 1, :]
                    part = term * here[j]
                    sum_ref[b + j, k] = sum_ref[b + j, k] + (
                        (part[0:8] + part[8:16]) + (part[16:24] + part[24:32])
                    )
            for j in range(2):
                lin = lin_ref[s, pl.ds(row, ROWS_STEP), cols[j]]
                sig = sig_ref[s, pl.ds(row, ROWS_STEP), cols[j]]
                grad_lin = sums[j] * sig
                grad_hidden_ref[pl.ds(out_row, ROWS_STEP), cols[j]] = grad_lin.astype(jnp.bfloat16)
                grad_hidden_ref[
                    pl.ds(out_row, ROWS_STEP),
                    pl.ds(pl.multiple_of(width + (b + j) * LANES, LANES), LANES),
                ] = (grad_lin * lin * (1.0 - sig)).astype(jnp.bfloat16)
            return carry

        return lax.fori_loop(0, (frames // ROWS_STEP) * (blocks // 2), conv_step, carry)

    lax.fori_loop(0, slabs, one_slab, 0)
    for b in range(blocks):
        for k in range(taps_count):
            grad_taps_ref[k : k + 1, b * LANES : (b + 1) * LANES] = jnp.sum(
                sum_ref[b, k], axis=0, keepdims=True
            )
    grad_taps_ref[taps_count:, :] = jnp.zeros(
        (grad_taps_ref.shape[0] - taps_count, width), jnp.float32
    )
    grad_taps_ref[taps_count + 1 : taps_count + 2, :] = jnp.sum(
        grad_gain_ref[...], axis=0, keepdims=True
    )


def send_kernel(index_ref, rows_ref, out_ref):
    rows, width = rows_ref.shape
    pick = (lax.broadcasted_iota(jnp.int32, (index_ref.shape[0], rows), 1) == index_ref[...])
    pick = pick.astype(jnp.float32).astype(jnp.bfloat16)
    for h in range(2):
        part = jnp.dot(
            pick,
            rows_ref[:, h * (width // 2) : (h + 1) * (width // 2)],
            preferred_element_type=jnp.float32,
        )
        slots = part.shape[0] // out_ref.shape[0]
        out_ref[:, h * slots : (h + 1) * slots, :] = part.astype(jnp.bfloat16).reshape(
            out_ref.shape[0], slots, width // 2
        )


def receive_kernel(index_ref, arrived_ref, upstream_ref, out_ref, last_ref, first_ref):
    slots, half = arrived_ref.shape
    slabs, frames, _ = upstream_ref.shape
    reach = 2 * EDGE
    columns = lax.broadcasted_iota(jnp.int32, (index_ref.shape[0], slots), 1)
    for h in range(2):
        pick = (columns == index_ref[:, h : h + 1]).astype(jnp.float32).astype(jnp.bfloat16)
        rows = jnp.dot(pick, arrived_ref[...], preferred_element_type=jnp.float32)
        rows = rows.astype(jnp.bfloat16)
        cols = slice(h * half, (h + 1) * half)
        out_ref[:, cols] = rows
        for s in range(slabs):
            last_ref[s, :reach, cols] = rows[(s + 1) * frames - reach : (s + 1) * frames]
            first_ref[s, :reach, cols] = rows[s * frames : s * frames + reach]
    for s in range(slabs):
        last_ref[s, reach:, :] = upstream_ref[s, frames - EDGE :, :]
        first_ref[s, reach:, :] = upstream_ref[s, :EDGE, :]


def total_kernel(
    parts_ref, out_sum_ref, weight_ref, gain_ref, total_ref, sum_ref, tile_ref, leaving, *, tap, scale
):
    count, share, width = parts_ref.shape
    in_width = weight_ref.shape[1]
    grad_gain = jnp.zeros((share, 1), jnp.float32)
    for at in range(0, width, SMALL):
        cols = slice(at, at + SMALL)
        part = jnp.zeros((share, SMALL), jnp.float32)
        for j in range(0, count, 16):
            part = part + jnp.sum(parts_ref[j : j + 16, :, cols].astype(jnp.float32), axis=0)
        sum_ref[:, cols] = part
        if at < in_width:
            grad_gain = grad_gain + jnp.sum(part * weight_ref[:, cols], axis=1, keepdims=True)
    small = sum_ref[:, in_width:]
    column = lax.broadcasted_iota(jnp.int32, small.shape, 1)
    sum_ref[:, in_width:] = jnp.where(column == tap, grad_gain / gain_ref[...], small)
    tile_ref[0, :, :width] = (sum_ref[...] * scale).astype(jnp.bfloat16)
    tile_ref[0, :, width:] = (out_sum_ref[...] * scale).astype(jnp.bfloat16)
    copies = [
        pltpu.make_async_copy(tile_ref, total_ref.at[pl.ds(i, 1)], leaving.at[i])
        for i in range(total_ref.shape[0])
    ]
    for copy in copies:
        copy.start()
    for copy in copies:
        copy.wait()


def finish_kernel(final_ref, grad_in_ref, grad_out_ref, grad_taps_ref, grad_gains_ref):
    in_width, taps_count = grad_in_ref.shape[1], grad_taps_ref.shape[0]
    grad_in_ref[...] = final_ref[:, :in_width].astype(jnp.float32)
    grad_out_ref[...] = final_ref[:, in_width + SMALL :].astype(jnp.float32)
    small = final_ref[:, in_width : in_width + LANES].astype(jnp.float32).T
    grad_taps_ref[...] = small[:taps_count]
    grad_gains_ref[...] = small[taps_count : taps_count + 2]


def product_kernel(core_ref, left_ref, left_other_ref, right_ref, right_other_ref, *rest):
    small_refs, out_ref, turned_ref = rest[:-2], rest[-2], rest[-1]
    rows, channels = left_ref.shape
    width = right_ref.shape[1]
    step = 512
    picks = [
        pl.ds(pl.multiple_of((2 * z + core_ref[0]) * LANES, LANES), LANES)
        for z in range(channels // LANES // 2)
    ]
    for z, pick in enumerate(picks):
        for h, ref in enumerate((left_ref, left_other_ref)):
            turned_ref[z * LANES : (z + 1) * LANES, h * rows : (h + 1) * rows] = ref[:, pick].T
    for at in range(0, width, step):
        right = jnp.concatenate(
            [right_ref[:, at : at + step], right_other_ref[:, at : at + step]], axis=0
        )
        out_ref[:, at : at + step] = jnp.dot(
            turned_ref[...], right, preferred_element_type=jnp.float32
        ).astype(out_ref.dtype)
    if small_refs:
        for z, pick in enumerate(picks):
            small = small_refs[0][:, pick] + small_refs[1][:, pick]
            filled = jnp.concatenate(
                [small, jnp.zeros((LANES - small.shape[0], LANES), jnp.float32)], axis=0
            )
            block = slice(z * LANES, (z + 1) * LANES)
            out_ref[block, width : width + LANES] = filled.T.astype(out_ref.dtype)


def weight_part(core, left, left_other, right, right_other, *small):
    rows, channels = left.shape
    mine = channels // LANES // 2
    width = right.shape[1]
    out_width = width + (SMALL if small else 0)
    vmem = pl.BlockSpec(memory_space=pltpu.VMEM)
    return pl.pallas_call(
        product_kernel,
        out_shape=jax.ShapeDtypeStruct((mine * LANES, out_width), jnp.bfloat16),
        in_specs=[pl.BlockSpec(memory_space=pltpu.SMEM)] + [vmem] * (4 + len(small)),
        out_specs=vmem,
        scratch_shapes=[pltpu.VMEM((mine * LANES, 2 * rows), jnp.bfloat16)],
        name="weight_part",
        compiler_params=pltpu.CompilerParams(vmem_limit_bytes=VMEM_GRANT),
        cost_estimate=pl.CostEstimate(
            flops=4 * rows * mine * LANES * width,
            bytes_accessed=4 * rows * (channels + width),
            transcendentals=0,
        ),
    )(core, left, left_other, right, right_other, *small)


def norm_kernel(
    frames_ref, low_ref, high_ref, upstream_ref, gain_ref, wide_ref, own_ref, up_wide_ref
):
    slabs, padded, _ = wide_ref.shape
    reach = 2 * EDGE
    own = padded - 2 * reach

    def normed_rows(rows):
        values = rows.astype(jnp.float32)
        centered = values - jnp.mean(values, axis=-1, keepdims=True)
        spread_ = jnp.mean(centered * centered, axis=-1, keepdims=True)
        return (centered * lax.rsqrt(spread_ + EPS) * gain_ref[0:1, :]).astype(jnp.bfloat16)

    for s in range(slabs):
        for at in range(0, reach, 16):
            wide_ref[s, at : at + 16, :] = normed_rows(low_ref[s, at : at + 16, :])
            high_at = reach + own + at
            wide_ref[s, high_at : high_at + 16, :] = normed_rows(high_ref[s, at : at + 16, :])

    def step(i, carry):
        row = pl.multiple_of(i * 16, 16)
        rows = normed_rows(frames_ref[pl.ds(row, 16), :])
        own_ref[pl.ds(row, 16), :] = rows
        steps = own // 16
        wide_ref[i // steps, pl.ds(pl.multiple_of(reach + (i % steps) * 16, 16), 16), :] = rows
        return carry

    lax.fori_loop(0, slabs * own // 16, step, 0, unroll=4)
    for s in range(slabs):
        base = s * (own + 2 * EDGE)
        up_wide_ref[base : base + EDGE, :] = low_ref[s, reach:, :]
        up_wide_ref[base + EDGE : base + EDGE + own, :] = upstream_ref[s]
        up_wide_ref[base + EDGE + own : base + 2 * EDGE + own, :] = high_ref[s, reach:, :]


def project_kernel(
    normed_ref, weight_ref, lin_ref, sig_ref, gated_ref,
    loaded_ref, lin_sum_ref, gate_sum_ref, rows_ref, arrivals,
):
    slabs, padded = lin_ref.shape[0], normed_ref.shape[0] // lin_ref.shape[0]
    parts, depth, both = loaded_ref.shape
    width = both // 2
    step = 256
    copies = [
        pltpu.make_async_copy(
            weight_ref.at[pl.ds(h * depth, depth)], loaded_ref.at[h], arrivals.at[h]
        )
        for h in range(parts)
    ]
    rows_copy = pltpu.make_async_copy(normed_ref, rows_ref, arrivals.at[parts])
    rows_copy.start()
    for copy in copies:
        copy.start()
    rows_copy.wait()
    for h, copy in enumerate(copies):
        copy.wait()
        rows = rows_ref[:, h * depth : (h + 1) * depth]
        for at in range(0, width, step):
            cols = slice(at, at + step)
            lin = jnp.dot(rows, loaded_ref[h, :, cols], preferred_element_type=jnp.float32)
            gate = jnp.dot(
                rows,
                loaded_ref[h, :, width + at : width + at + step],
                preferred_element_type=jnp.float32,
            )
            if h < parts - 1:
                lin_sum_ref[:, cols] = lin
                gate_sum_ref[:, cols] = gate
                continue
            lin = lin + lin_sum_ref[:, cols]
            sig = jax.nn.sigmoid(gate + gate_sum_ref[:, cols])
            gated_ref[:, cols] = (lin * sig).astype(jnp.bfloat16)
            for s in range(slabs):
                inner = slice(s * padded + 2 * EDGE, (s + 1) * padded - 2 * EDGE)
                lin_ref[s, :, cols] = lin[inner]
                sig_ref[s, :, cols] = sig[inner]


def project(normed, weight, slabs):
    rows, width = normed.shape
    own = pltpu.VMEM((rows, width), jnp.float32)
    kept = jax.ShapeDtypeStruct((slabs, rows // slabs - 4 * EDGE, width), jnp.float32)
    parts = 2
    vmem = pl.BlockSpec(memory_space=pltpu.VMEM)
    return pl.pallas_call(
        project_kernel,
        out_shape=(
            kept,
            kept,
            jax.ShapeDtypeStruct((rows, width), jnp.bfloat16),
        ),
        in_specs=[pl.BlockSpec(memory_space=pltpu.HBM)] * 2,
        out_specs=(vmem, vmem, vmem),
        scratch_shapes=[
            pltpu.VMEM((parts, width // parts, 2 * width), jnp.bfloat16),
            own,
            own,
            pltpu.VMEM((rows, width), jnp.bfloat16),
            pltpu.SemaphoreType.DMA((parts + 1,)),
        ],
        name="project",
        compiler_params=pltpu.CompilerParams(vmem_limit_bytes=VMEM_GRANT),
        cost_estimate=pl.CostEstimate(
            flops=4 * rows * width * width,
            bytes_accessed=4 * width * width,
            transcendentals=rows * width,
        ),
    )(*(pltpu.with_memory_space_constraint(a, pltpu.HBM) for a in (normed, weight)))


def kernel_call(body, outs, scratch, flops, *args, in_hbm=(), out_hbm=False):
    moved = sum(a.size * a.dtype.itemsize for a in args)
    specs = {}
    if in_hbm:
        specs["in_specs"] = [
            pl.BlockSpec(memory_space=pltpu.HBM if i in in_hbm else pltpu.VMEM)
            for i in range(len(args))
        ]
    if out_hbm:
        specs["out_specs"] = pl.BlockSpec(memory_space=pltpu.HBM)
        outs = pltpu.HBM(outs.shape, outs.dtype)
    args = [
        pltpu.with_memory_space_constraint(a, pltpu.HBM) if i in in_hbm else a
        for i, a in enumerate(args)
    ]
    return pl.pallas_call(
        body,
        out_shape=outs,
        scratch_shapes=scratch,
        compiler_params=pltpu.CompilerParams(vmem_limit_bytes=VMEM_GRANT),
        cost_estimate=pl.CostEstimate(flops=flops, bytes_accessed=moved, transcendentals=0),
        **specs,
    )(*args)


def to_neighbours(last, first, count):
    forward = [(i, i + 1) for i in range(count - 1)]
    backward = [(i + 1, i) for i in range(count - 1)]
    return lax.ppermute(last, SEQ, forward), lax.ppermute(first, SEQ, backward)


def norm_rows(values, gain):
    average = jnp.mean(values, axis=-1, keepdims=True)
    centered = values - average
    spread_ = jnp.mean(centered * centered, axis=-1, keepdims=True)
    return centered * lax.rsqrt(spread_ + EPS) * gain


def per_device(
    loaded, plan, segment_ids, in_weight, out_weight, depth_kernel, norm_gains, upstream
):
    rows_dev, width = loaded.shape
    devices = plan.shape[0]
    capacity = 2 * rows_dev // devices
    slabs, slab_len = segment_ids.shape
    n_seq = lax.axis_size(SEQ)
    n_z = lax.axis_size("z")
    frames_dev = slab_len // n_seq
    kernel_len = depth_kernel.shape[1]
    core = lax.axis_index("core")
    sender = lax.axis_index((*DP, *SEQ))
    swap = [(0, 1), (1, 0)]

    in_full = lax.all_gather(in_weight, DP, axis=0, tiled=True)
    out_full = lax.all_gather(out_weight, DP, axis=0, tiled=True)

    send_plan = lax.dynamic_index_in_dim(plan, sender, 0, keepdims=False)
    send_start = jnp.cumsum(send_plan) - send_plan
    slot_index = jnp.arange(capacity, dtype=jnp.int32)
    source_rows = jnp.minimum(send_start[:, None] + slot_index[None, :], rows_dev - 1)
    outgoing = kernel_call(
        send_kernel,
        jax.ShapeDtypeStruct((devices, 2 * capacity, width // 2), jnp.bfloat16),
        [],
        4 * devices * capacity * rows_dev * width,
        source_rows.reshape(-1, 1), loaded,
    )
    arrived = lax.all_to_all(
        outgoing, (*DP, *SEQ), split_axis=0, concat_axis=0, tiled=True
    ).reshape(devices * 2 * capacity, width // 2)
    extras = jnp.pad(
        jnp.concatenate([depth_kernel, norm_gains], axis=1), ((0, 0), (0, LANES - kernel_len - 2))
    )
    upstream_rows = upstream.reshape(rows_dev, width)
    extras_other = lax.ppermute(extras, "core", swap)
    pair = jnp.where(
        core == 0, jnp.stack([extras, extras_other]), jnp.stack([extras_other, extras])
    )
    from_z = [
        lax.ppermute(pair, "z", [(i, (i + d) % n_z) for i in range(n_z)])
        for d in range(1, n_z)
    ]
    upstream_other = lax.ppermute(upstream_rows, "core", swap)
    arrived, upstream_other, pair = lax.optimization_barrier((arrived, upstream_other, pair))
    by_z = jnp.stack([*from_z[::-1], pair])
    side_all = lax.dynamic_slice_in_dim(
        jnp.concatenate([by_z, by_z]), n_z - 1 - lax.axis_index("z"), n_z, 0
    )
    recv_plan = lax.dynamic_index_in_dim(plan, sender, 1, keepdims=False)
    recv_end = jnp.cumsum(recv_plan)
    frame_index = jnp.arange(rows_dev, dtype=jnp.int32)
    before = recv_end[None, :] <= frame_index[:, None]
    source_dev = jnp.sum(before.astype(jnp.int32), axis=1)
    start_of = jnp.sum(jnp.where(before, recv_plan[None, :], 0), axis=1)
    place = source_dev * 2 * capacity + frame_index - start_of
    frames, last, first = kernel_call(
        receive_kernel,
        (
            jax.ShapeDtypeStruct((rows_dev, width), jnp.bfloat16),
            jax.ShapeDtypeStruct((slabs, 3 * EDGE, width), jnp.bfloat16),
            jax.ShapeDtypeStruct((slabs, 3 * EDGE, width), jnp.bfloat16),
        ),
        [],
        4 * devices * capacity * rows_dev * width,
        jnp.stack([place, place + capacity], axis=1), arrived, upstream,
    )
    low, high = to_neighbours(last, first, n_seq)
    side = side_all.reshape(width, LANES)[:, : kernel_len + 2].astype(jnp.float32).T
    gain_pre, gain_mid = side[kernel_len], side[kernel_len + 1]
    taps = jnp.pad(side[:kernel_len], ((0, 1), (0, 0)))
    taps = taps.reshape(kernel_len + 1, width // LANES, LANES).transpose(1, 0, 2)

    id_pad = jnp.pad(segment_ids, ((0, 0), (2 * EDGE, 2 * EDGE)), constant_values=-1)
    window = lax.dynamic_slice_in_dim(
        id_pad, lax.axis_index(SEQ) * frames_dev, frames_dev + 4 * EDGE, 1
    )
    ids = jnp.broadcast_to(window[:, :, None], (*window.shape, LANES))

    frame_rows = frames.astype(jnp.float32)
    _, pull_pre = jax.vjp(norm_rows, frame_rows, gain_pre)
    padded = frames_dev + 4 * EDGE
    normed_wide, normed, upstream_wide = kernel_call(
        norm_kernel,
        (
            jax.ShapeDtypeStruct((slabs, padded, width), jnp.bfloat16),
            jax.ShapeDtypeStruct((rows_dev, width), jnp.bfloat16),
            jax.ShapeDtypeStruct((slabs * (frames_dev + 2 * EDGE), width), jnp.bfloat16),
        ),
        [],
        rows_dev * width * 10,
        frames, low, high, upstream, gain_pre[None],
    )
    normed_other = lax.ppermute(normed, "core", swap)
    lin, sig, gated = project(normed_wide.reshape(-1, width), in_full, slabs)
    gated, normed_other = lax.optimization_barrier((gated, normed_other))
    gated = gated.reshape(slabs, padded, width)
    elements = rows_dev * width
    wide = frames_dev + 2 * EDGE
    blocks = width // LANES
    activated, normed_mid = kernel_call(
        forward_kernel,
        (
            jax.ShapeDtypeStruct((rows_dev, width), jnp.bfloat16),
            jax.ShapeDtypeStruct((slabs * wide, width + LANES), jnp.float32),
        ),
        [
            pltpu.VMEM((blocks, padded, LANES), jnp.float32),
            pltpu.VMEM((blocks, wide, LANES), jnp.float32),
        ],
        elements * 3 * kernel_len,
        gated, ids, taps, gain_mid[None],
    )
    act_other = lax.ppermute(activated, "core", swap)
    grad_mixing, grad_gain_mid = kernel_call(
        middle_kernel,
        (
            jax.ShapeDtypeStruct((slabs, wide, width), jnp.float32),
            jax.ShapeDtypeStruct((8, width), jnp.float32),
        ),
        [
            pltpu.VMEM((slabs * wide, width), jnp.float32),
            pltpu.VMEM((slabs * wide, width), jnp.bfloat16),
            pltpu.VMEM((4, width // 4, width), jnp.bfloat16),
            pltpu.SemaphoreType.DMA((5,)),
        ],
        2 * slabs * wide * width * width,
        normed_mid, upstream_wide, out_full, gain_mid[None],
        in_hbm=(1, 2),
    )

    def exchanged(part):
        return lax.all_to_all(
            part.reshape(n_z * n_seq, LANES // n_seq, part.shape[1]), ZXY, 0, 0, tiled=True
        )

    core_ref = core[None].astype(jnp.int32)
    out_part = weight_part(core_ref, activated, act_other, upstream_rows, upstream_other)
    out_parts = exchanged(out_part)
    out_sum = jnp.sum(out_parts.astype(jnp.float32), axis=0)
    projected = jnp.dot(activated, out_full, preferred_element_type=jnp.float32)
    encoded = (frame_rows + projected).astype(jnp.bfloat16).reshape(slabs, frames_dev, width)

    grad_hidden, grad_taps = kernel_call(
        backward_kernel,
        (
            jax.ShapeDtypeStruct((rows_dev, 2 * width), jnp.bfloat16),
            jax.ShapeDtypeStruct((kernel_len + 9, width), jnp.float32),
        ),
        [
            pltpu.VMEM((blocks, wide, LANES), jnp.float32),
            pltpu.VMEM((blocks, kernel_len, 8, LANES), jnp.float32),
        ],
        elements * 5 * kernel_len,
        grad_mixing, gated, ids, taps, lin, sig, grad_gain_mid,
    )
    hidden_other = lax.ppermute(grad_hidden, "core", swap)
    small_other = lax.ppermute(grad_taps, "core", swap)
    in_part = weight_part(
        core_ref, normed, normed_other, grad_hidden, hidden_other, grad_taps, small_other
    )
    in_parts = exchanged(in_part)
    grad_normed = lax.dot_general(
        grad_hidden, in_full, (((1,), (1,)), ((), ())), preferred_element_type=jnp.float32
    )
    grad_rows, _ = pull_pre(grad_normed)
    grad_frames = (
        (upstream_rows.astype(jnp.float32) + grad_rows)
        .astype(jnp.bfloat16)
        .reshape(slabs, frames_dev, width)
    )
    share = LANES // n_seq
    start = lax.axis_index(SEQ) * share
    own_weight = lax.dynamic_slice_in_dim(in_weight, start, share, 0).astype(jnp.float32)
    own_gain = lax.dynamic_slice_in_dim(norm_gains, start, share, 0)[:, :1].astype(jnp.float32)
    total = kernel_call(
        functools.partial(
            total_kernel, tap=kernel_len, scale=1.0 / math.sqrt(devices * rows_dev)
        ),
        jax.ShapeDtypeStruct((n_seq, share, 3 * width + SMALL), jnp.bfloat16),
        [
            pltpu.VMEM((share, 2 * width + SMALL), jnp.float32),
            pltpu.VMEM((1, share, 3 * width + SMALL), jnp.bfloat16),
            pltpu.SemaphoreType.DMA((n_seq,)),
        ],
        in_parts.size,
        in_parts, out_sum, own_weight, own_gain,
        out_hbm=True,
    )
    final = lax.all_to_all(total, SEQ, 0, 0, tiled=True).reshape(LANES, -1)
    grad_in, grad_out, grad_kernel, grad_gains = kernel_call(
        finish_kernel,
        (
            jax.ShapeDtypeStruct((LANES, 2 * width), jnp.float32),
            jax.ShapeDtypeStruct((LANES, width), jnp.float32),
            jax.ShapeDtypeStruct((kernel_len, LANES), jnp.float32),
            jax.ShapeDtypeStruct((2, LANES), jnp.float32),
        ),
        [],
        LANES * width,
        final,
    )
    return encoded, grad_frames, grad_in, grad_out, grad_kernel.T, grad_gains.T


def solution(mesh):
    n_dp, n_seq = mesh.devices.shape
    side = math.isqrt(n_seq)
    split = Mesh(mesh.devices.reshape(n_dp // 2, 2, side, side), ("z", "core", "x", "y"))
    placed = (
        P((*DP, *SEQ), None),
        P(),
        P(DP, None),
        P(DP, None),
        P(DP, None),
        P(DP, None),
        P(DP, None),
        P(DP, SEQ, None),
    )
    return jax.shard_map(
        per_device,
        mesh=split,
        in_specs=placed,
        out_specs=(
            P(DP, SEQ, None),
            P(DP, SEQ, None),
            P(DP, None),
            P(DP, None),
            P(DP, None),
            P(DP, None),
        ),
        check_vma=False,
    )
```

```python
import functools
import math

import jax
import jax.numpy as jnp
from jax import lax
from jax.experimental import pallas as pl
from jax.experimental.pallas import tpu as pltpu
from jax.sharding import Mesh, PartitionSpec as P


DP = ("z", "core")
SEQ = ("x", "y")
ZXY = ("z", "x", "y")
EDGE = 16
LANES = 128
ROWS_STEP = 32
EPS = 1e-05
SMALL = LANES
VMEM_GRANT = 16 * 1024 * 1024


def forward_kernel(
    gated_ref, ids_ref, taps_ref, gain_ref,
    act_ref, normed_ref, pad_ref, mix_ref,
):
    slabs, padded, width = gated_ref.shape
    blocks = width // LANES
    taps_count = taps_ref.shape[1] - 1
    wide = padded - 2 * EDGE
    own = wide - 2 * EDGE
    shift = EDGE - taps_count // 2

    def one_slab(s, carry):
        for b in range(blocks):
            pad_ref[b] = gated_ref[s, :, b * LANES : (b + 1) * LANES].astype(jnp.float32)

        def conv_step(i, carry):
            row = pl.multiple_of((i // (blocks // 2)) * ROWS_STEP, ROWS_STEP)
            b = (i % (blocks // 2)) * 2
            center = ids_ref[s, pl.ds(row + EDGE, ROWS_STEP)]
            sums = [jnp.zeros((ROWS_STEP, LANES), jnp.float32) for _ in range(2)]
            for k in range(taps_count):
                same = ids_ref[s, pl.ds(row + k + shift, ROWS_STEP)] == center
                for j in range(2):
                    term = pad_ref[b + j, pl.ds(row + k + shift, ROWS_STEP)]
                    sums[j] = sums[j] + jnp.where(same, term, 0.0) * taps_ref[b + j, k : k + 1, :]
            for j in range(2):
                mix_ref[b + j, pl.ds(row, ROWS_STEP)] = sums[j]
            return carry

        lax.fori_loop(0, (wide // ROWS_STEP) * (blocks // 2), conv_step, 0)

        def row_step(i, own_rows):
            row = pl.multiple_of(i * 16, 16)
            out_row = pl.multiple_of(s * wide + i * 16, 16)
            mixing = jnp.concatenate([mix_ref[b, pl.ds(row, 16)] for b in range(blocks)], axis=1)
            centered = mixing - jnp.mean(mixing, axis=-1, keepdims=True)
            scale = lax.rsqrt(jnp.mean(centered * centered, axis=-1, keepdims=True) + EPS)
            normed = centered * scale
            if own_rows:
                act_row = pl.multiple_of(s * own + i * 16 - EDGE, 16)
                value = normed * gain_ref[0:1, :]
                act_ref[pl.ds(act_row, 16), :] = (value * jax.nn.sigmoid(value)).astype(
                    act_ref.dtype
                )
            normed_ref[pl.ds(out_row, 16), :width] = normed
            normed_ref[pl.ds(out_row, 16), width:] = jnp.broadcast_to(scale, (16, LANES))

        steps = wide // 16
        row_step(0, False)
        row_step(steps - 1, False)

        def own_step(i, carry):
            row_step(i + 1, True)
            return carry

        return lax.fori_loop(0, steps - 2, own_step, carry, unroll=4)

    lax.fori_loop(0, slabs, one_slab, 0)


def middle_kernel(
    normed_ref, upstream_ref, weight_ref, gain_ref,
    grad_mix_ref, grad_gain_ref, grad_act_ref,
):
    slabs, frames, width = grad_mix_ref.shape
    steps = frames // 16
    grad_act_ref[...] = lax.dot_general(
        upstream_ref[...],
        weight_ref[...],
        (((1,), (1,)), ((), ())),
        preferred_element_type=jnp.float32,
    )

    def row_step(i, total):
        row = pl.multiple_of(i * 16, 16)
        normed = normed_ref[pl.ds(row, 16), :width]
        scale = normed_ref[pl.ds(row, 16), width : width + 1]
        gain = gain_ref[0:1, :]
        value = normed * gain
        sig = jax.nn.sigmoid(value)
        grad_value = grad_act_ref[pl.ds(row, 16), :] * (sig * (1.0 + value * (1.0 - sig)))
        part = grad_value * normed
        at = i % steps
        own = jnp.logical_and(at > 0, at < steps - 1)
        total = total + jnp.where(own, part[0:8] + part[8:16], 0.0)
        grad_normed = grad_value * gain
        first = jnp.mean(grad_normed, axis=-1, keepdims=True)
        second = jnp.mean(grad_normed * normed, axis=-1, keepdims=True)
        grad_mix_ref[i // steps, pl.ds(pl.multiple_of((i % steps) * 16, 16), 16), :] = scale * (
            grad_normed - first - normed * second
        )
        return total

    grad_gain_ref[...] = lax.fori_loop(
        0, slabs * steps, row_step, jnp.zeros(grad_gain_ref.shape, jnp.float32), unroll=4
    )


def backward_kernel(
    grad_mix_ref, gated_ref, ids_ref, taps_ref, lin_ref, sig_ref, grad_gain_ref,
    grad_hidden_ref, grad_taps_ref, kept_ref, pad_ref, sum_ref, leaving,
):
    slabs, padded, width = gated_ref.shape
    frames = padded - 4 * EDGE
    blocks = width // LANES
    taps_count = taps_ref.shape[1] - 1
    half = taps_count // 2
    sum_ref[...] = jnp.zeros(sum_ref.shape, jnp.float32)

    def one_slab(s, carry):
        for b in range(blocks):
            pad_ref[b] = grad_mix_ref[s, :, b * LANES : (b + 1) * LANES]

        def conv_step(i, carry):
            row = pl.multiple_of((i // (blocks // 2)) * ROWS_STEP, ROWS_STEP)
            out_row = pl.multiple_of(s * frames + row, ROWS_STEP)
            b = (i % (blocks // 2)) * 2
            hid_row = pl.multiple_of(s * padded + 2 * EDGE + row, ROWS_STEP)
            center = ids_ref[s, pl.ds(row + 2 * EDGE, ROWS_STEP)]
            sums = [jnp.zeros((ROWS_STEP, LANES), jnp.float32) for _ in range(2)]
            cols = [pl.ds(pl.multiple_of((b + j) * LANES, LANES), LANES) for j in range(2)]
            here = [gated_ref[s, pl.ds(row + 2 * EDGE, ROWS_STEP), cols[j]].astype(jnp.float32) for j in range(2)]
            for k in range(taps_count):
                at = row + EDGE + half - k
                same = ids_ref[s, pl.ds(at + EDGE, ROWS_STEP)] == center
                for j in range(2):
                    term = jnp.where(same, pad_ref[b + j, pl.ds(at, ROWS_STEP)], 0.0)
                    sums[j] = sums[j] + term * taps_ref[b + j, k : k + 1, :]
                    part = term * here[j]
                    sum_ref[b + j, k] = sum_ref[b + j, k] + (
                        (part[0:8] + part[8:16]) + (part[16:24] + part[24:32])
                    )
            for j in range(2):
                lin = lin_ref[pl.ds(hid_row, ROWS_STEP), cols[j]]
                sig = sig_ref[pl.ds(hid_row, ROWS_STEP), cols[j]]
                grad_lin = sums[j] * sig
                grad_hidden_ref[pl.ds(out_row, ROWS_STEP), cols[j]] = grad_lin.astype(jnp.bfloat16)
                grad_hidden_ref[
                    pl.ds(out_row, ROWS_STEP),
                    pl.ds(pl.multiple_of(width + (b + j) * LANES, LANES), LANES),
                ] = (grad_lin * lin * (1.0 - sig)).astype(jnp.bfloat16)
            return carry

        lax.fori_loop(0, (frames // ROWS_STEP) * (blocks // 2), conv_step, 0)
        kept_copy(s).start()
        return carry

    def kept_copy(s):
        rows = pl.ds(pl.multiple_of(s * frames, ROWS_STEP), frames)
        return pltpu.make_async_copy(grad_hidden_ref.at[rows], kept_ref.at[rows], leaving.at[s])

    lax.fori_loop(0, slabs, one_slab, 0)
    for b in range(blocks):
        for k in range(taps_count):
            grad_taps_ref[k : k + 1, b * LANES : (b + 1) * LANES] = jnp.sum(
                sum_ref[b, k], axis=0, keepdims=True
            )
    grad_taps_ref[taps_count:, :] = jnp.zeros(
        (grad_taps_ref.shape[0] - taps_count, width), jnp.float32
    )
    grad_taps_ref[taps_count + 1 : taps_count + 2, :] = jnp.sum(
        grad_gain_ref[...], axis=0, keepdims=True
    )
    for s in range(slabs):
        kept_copy(s).wait()


def send_kernel(index_ref, rows_ref, out_ref):
    rows, width = rows_ref.shape
    pick = (lax.broadcasted_iota(jnp.int32, (index_ref.shape[0], rows), 1) == index_ref[...])
    pick = pick.astype(jnp.float32).astype(jnp.bfloat16)
    for h in range(2):
        part = jnp.dot(
            pick,
            rows_ref[:, h * (width // 2) : (h + 1) * (width // 2)],
            preferred_element_type=jnp.float32,
        )
        slots = part.shape[0] // out_ref.shape[0]
        out_ref[:, h * slots : (h + 1) * slots, :] = part.astype(jnp.bfloat16).reshape(
            out_ref.shape[0], slots, width // 2
        )


def receive_kernel(index_ref, arrived_ref, upstream_ref, out_ref, last_ref, first_ref):
    slots, half = arrived_ref.shape
    slabs, frames, _ = upstream_ref.shape
    reach = 2 * EDGE
    columns = lax.broadcasted_iota(jnp.int32, (index_ref.shape[0], slots), 1)
    for h in range(2):
        pick = (columns == index_ref[:, h : h + 1]).astype(jnp.float32).astype(jnp.bfloat16)
        rows = jnp.dot(pick, arrived_ref[...], preferred_element_type=jnp.float32)
        rows = rows.astype(jnp.bfloat16)
        cols = slice(h * half, (h + 1) * half)
        out_ref[:, cols] = rows
        for s in range(slabs):
            last_ref[s, :reach, cols] = rows[(s + 1) * frames - reach : (s + 1) * frames]
            first_ref[s, :reach, cols] = rows[s * frames : s * frames + reach]
    for s in range(slabs):
        last_ref[s, reach:, :] = upstream_ref[s, frames - EDGE :, :]
        first_ref[s, reach:, :] = upstream_ref[s, :EDGE, :]


def total_kernel(parts_ref, out_sum_ref, weight_ref, gain_ref, total_ref, sum_ref, *, tap, scale):
    count, share, width = parts_ref.shape
    in_width = weight_ref.shape[1]
    grad_gain = jnp.zeros((share, 1), jnp.float32)
    for at in range(0, width, SMALL):
        cols = slice(at, at + SMALL)
        part = jnp.zeros((share, SMALL), jnp.float32)
        for j in range(0, count, 16):
            part = part + jnp.sum(parts_ref[j : j + 16, :, cols].astype(jnp.float32), axis=0)
        sum_ref[:, cols] = part
        if at < in_width:
            grad_gain = grad_gain + jnp.sum(part * weight_ref[:, cols], axis=1, keepdims=True)
    small = sum_ref[:, in_width:]
    column = lax.broadcasted_iota(jnp.int32, small.shape, 1)
    sum_ref[:, in_width:] = jnp.where(column == tap, grad_gain / gain_ref[...], small)
    for i in range(total_ref.shape[0]):
        total_ref[i, :, :width] = (sum_ref[...] * scale).astype(jnp.bfloat16)
        total_ref[i, :, width:] = (out_sum_ref[...] * scale).astype(jnp.bfloat16)


def finish_kernel(final_ref, grad_in_ref, grad_out_ref, grad_taps_ref, grad_gains_ref):
    in_width, taps_count = grad_in_ref.shape[1], grad_taps_ref.shape[0]
    grad_in_ref[...] = final_ref[:, :in_width].astype(jnp.float32)
    grad_out_ref[...] = final_ref[:, in_width + SMALL :].astype(jnp.float32)
    small = final_ref[:, in_width : in_width + LANES].astype(jnp.float32).T
    grad_taps_ref[...] = small[:taps_count]
    grad_gains_ref[...] = small[taps_count : taps_count + 2]


def product_kernel(core_ref, left_ref, left_other_ref, right_ref, right_other_ref, *rest):
    small_refs, out_ref, turned_ref = rest[:-2], rest[-2], rest[-1]
    rows, channels = left_ref.shape
    width = right_ref.shape[1]
    step = 512
    picks = [
        pl.ds(pl.multiple_of((2 * z + core_ref[0]) * LANES, LANES), LANES)
        for z in range(channels // LANES // 2)
    ]
    for z, pick in enumerate(picks):
        for h, ref in enumerate((left_ref, left_other_ref)):
            turned_ref[z * LANES : (z + 1) * LANES, h * rows : (h + 1) * rows] = ref[:, pick].T
    for at in range(0, width, step):
        right = jnp.concatenate(
            [right_ref[:, at : at + step], right_other_ref[:, at : at + step]], axis=0
        )
        out_ref[:, at : at + step] = jnp.dot(
            turned_ref[...], right, preferred_element_type=jnp.float32
        ).astype(out_ref.dtype)
    if small_refs:
        for z, pick in enumerate(picks):
            small = small_refs[0][:, pick] + small_refs[1][:, pick]
            filled = jnp.concatenate(
                [small, jnp.zeros((LANES - small.shape[0], LANES), jnp.float32)], axis=0
            )
            block = slice(z * LANES, (z + 1) * LANES)
            out_ref[block, width : width + LANES] = filled.T.astype(out_ref.dtype)


def weight_part(core, left, left_other, right, right_other, *small):
    rows, channels = left.shape
    mine = channels // LANES // 2
    width = right.shape[1]
    out_width = width + (SMALL if small else 0)
    vmem = pl.BlockSpec(memory_space=pltpu.VMEM)
    return pl.pallas_call(
        product_kernel,
        out_shape=jax.ShapeDtypeStruct((mine * LANES, out_width), jnp.bfloat16),
        in_specs=[pl.BlockSpec(memory_space=pltpu.SMEM)] + [vmem] * (4 + len(small)),
        out_specs=vmem,
        scratch_shapes=[pltpu.VMEM((mine * LANES, 2 * rows), jnp.bfloat16)],
        name="weight_part",
        compiler_params=pltpu.CompilerParams(vmem_limit_bytes=VMEM_GRANT),
        cost_estimate=pl.CostEstimate(
            flops=4 * rows * mine * LANES * width,
            bytes_accessed=4 * rows * (channels + width),
            transcendentals=0,
        ),
    )(core, left, left_other, right, right_other, *small)


def norm_kernel(
    frames_ref, low_ref, high_ref, upstream_ref, gain_ref, wide_ref, own_ref, up_wide_ref
):
    slabs, padded, _ = wide_ref.shape
    reach = 2 * EDGE
    own = padded - 2 * reach

    def normed_rows(rows):
        values = rows.astype(jnp.float32)
        centered = values - jnp.mean(values, axis=-1, keepdims=True)
        spread_ = jnp.mean(centered * centered, axis=-1, keepdims=True)
        return (centered * lax.rsqrt(spread_ + EPS) * gain_ref[0:1, :]).astype(jnp.bfloat16)

    for s in range(slabs):
        for at in range(0, reach, 16):
            wide_ref[s, at : at + 16, :] = normed_rows(low_ref[s, at : at + 16, :])
            high_at = reach + own + at
            wide_ref[s, high_at : high_at + 16, :] = normed_rows(high_ref[s, at : at + 16, :])

    def step(i, carry):
        row = pl.multiple_of(i * 16, 16)
        rows = normed_rows(frames_ref[pl.ds(row, 16), :])
        own_ref[pl.ds(row, 16), :] = rows
        steps = own // 16
        wide_ref[i // steps, pl.ds(pl.multiple_of(reach + (i % steps) * 16, 16), 16), :] = rows
        return carry

    lax.fori_loop(0, slabs * own // 16, step, 0, unroll=4)
    for s in range(slabs):
        base = s * (own + 2 * EDGE)
        up_wide_ref[base : base + EDGE, :] = low_ref[s, reach:, :]
        up_wide_ref[base + EDGE : base + EDGE + own, :] = upstream_ref[s]
        up_wide_ref[base + EDGE + own : base + 2 * EDGE + own, :] = high_ref[s, reach:, :]


def project_kernel(normed_ref, lin_w_ref, gate_w_ref, lin_ref, sig_ref, gated_ref):
    lin = jnp.dot(normed_ref[...], lin_w_ref[...], preferred_element_type=jnp.float32)
    gate = jnp.dot(normed_ref[...], gate_w_ref[...], preferred_element_type=jnp.float32)
    sig = jax.nn.sigmoid(gate)
    lin_ref[...] = lin
    sig_ref[...] = sig
    gated_ref[...] = (lin * sig).astype(jnp.bfloat16)


def project(normed, weight):
    rows, width = normed.shape
    cols = 256
    steps = width // cols
    out = pl.BlockSpec((rows, cols), lambda j: (0, j))
    return pl.pallas_call(
        project_kernel,
        out_shape=(
            jax.ShapeDtypeStruct((rows, width), jnp.float32),
            jax.ShapeDtypeStruct((rows, width), jnp.float32),
            jax.ShapeDtypeStruct((rows, width), jnp.bfloat16),
        ),
        grid=(steps,),
        in_specs=[
            pl.BlockSpec((rows, width), lambda j: (0, 0)),
            pl.BlockSpec((width, cols), lambda j: (0, j)),
            pl.BlockSpec((width, cols), lambda j: (0, j + steps)),
        ],
        out_specs=(out, out, out),
        name="project",
        compiler_params=pltpu.CompilerParams(vmem_limit_bytes=VMEM_GRANT),
        cost_estimate=pl.CostEstimate(
            flops=4 * rows * width * width,
            bytes_accessed=4 * width * width,
            transcendentals=rows * width,
        ),
    )(normed, weight, weight)


def kernel_call(body, outs, scratch, flops, *args, **specs):
    moved = sum(a.size * a.dtype.itemsize for a in args)
    return pl.pallas_call(
        body,
        out_shape=outs,
        scratch_shapes=scratch,
        compiler_params=pltpu.CompilerParams(vmem_limit_bytes=VMEM_GRANT),
        cost_estimate=pl.CostEstimate(flops=flops, bytes_accessed=moved, transcendentals=0),
        **specs,
    )(*args)


def to_neighbours(last, first, count):
    forward = [(i, i + 1) for i in range(count - 1)]
    backward = [(i + 1, i) for i in range(count - 1)]
    return lax.ppermute(last, SEQ, forward), lax.ppermute(first, SEQ, backward)


def norm_rows(values, gain):
    average = jnp.mean(values, axis=-1, keepdims=True)
    centered = values - average
    spread_ = jnp.mean(centered * centered, axis=-1, keepdims=True)
    return centered * lax.rsqrt(spread_ + EPS) * gain


def per_device(
    loaded, plan, segment_ids, in_weight, out_weight, depth_kernel, norm_gains, upstream
):
    rows_dev, width = loaded.shape
    devices = plan.shape[0]
    capacity = 2 * rows_dev // devices
    slabs, slab_len = segment_ids.shape
    n_seq = lax.axis_size(SEQ)
    n_z = lax.axis_size("z")
    frames_dev = slab_len // n_seq
    kernel_len = depth_kernel.shape[1]
    core = lax.axis_index("core")
    sender = lax.axis_index((*DP, *SEQ))
    swap = [(0, 1), (1, 0)]

    in_full = lax.all_gather(in_weight, DP, axis=0, tiled=True)
    out_full = lax.all_gather(out_weight, DP, axis=0, tiled=True)

    send_plan = lax.dynamic_index_in_dim(plan, sender, 0, keepdims=False)
    send_start = jnp.cumsum(send_plan) - send_plan
    slot_index = jnp.arange(capacity, dtype=jnp.int32)
    source_rows = jnp.minimum(send_start[:, None] + slot_index[None, :], rows_dev - 1)
    outgoing = kernel_call(
        send_kernel,
        jax.ShapeDtypeStruct((devices, 2 * capacity, width // 2), jnp.bfloat16),
        [],
        4 * devices * capacity * rows_dev * width,
        source_rows.reshape(-1, 1), loaded,
    )
    arrived = lax.all_to_all(
        outgoing, (*DP, *SEQ), split_axis=0, concat_axis=0, tiled=True
    ).reshape(devices * 2 * capacity, width // 2)
    extras = jnp.pad(
        jnp.concatenate([depth_kernel, norm_gains], axis=1), ((0, 0), (0, LANES - kernel_len - 2))
    )
    upstream_rows = upstream.reshape(rows_dev, width)
    extras_other = lax.ppermute(extras, "core", swap)
    pair = jnp.where(
        core == 0, jnp.stack([extras, extras_other]), jnp.stack([extras_other, extras])
    )
    from_z = [
        lax.ppermute(pair, "z", [(i, (i + d) % n_z) for i in range(n_z)])
        for d in range(1, n_z)
    ]
    upstream_other = lax.ppermute(upstream_rows, "core", swap)
    arrived, upstream_other, pair = lax.optimization_barrier((arrived, upstream_other, pair))
    by_z = jnp.stack([*from_z[::-1], pair])
    side_all = lax.dynamic_slice_in_dim(
        jnp.concatenate([by_z, by_z]), n_z - 1 - lax.axis_index("z"), n_z, 0
    )
    recv_plan = lax.dynamic_index_in_dim(plan, sender, 1, keepdims=False)
    recv_end = jnp.cumsum(recv_plan)
    frame_index = jnp.arange(rows_dev, dtype=jnp.int32)
    before = recv_end[None, :] <= frame_index[:, None]
    source_dev = jnp.sum(before.astype(jnp.int32), axis=1)
    start_of = jnp.sum(jnp.where(before, recv_plan[None, :], 0), axis=1)
    place = source_dev * 2 * capacity + frame_index - start_of
    frames, last, first = kernel_call(
        receive_kernel,
        (
            jax.ShapeDtypeStruct((rows_dev, width), jnp.bfloat16),
            jax.ShapeDtypeStruct((slabs, 3 * EDGE, width), jnp.bfloat16),
            jax.ShapeDtypeStruct((slabs, 3 * EDGE, width), jnp.bfloat16),
        ),
        [],
        4 * devices * capacity * rows_dev * width,
        jnp.stack([place, place + capacity], axis=1), arrived, upstream,
    )
    low, high = to_neighbours(last, first, n_seq)
    side = side_all.reshape(width, LANES)[:, : kernel_len + 2].astype(jnp.float32).T
    gain_pre, gain_mid = side[kernel_len], side[kernel_len + 1]
    taps = jnp.pad(side[:kernel_len], ((0, 1), (0, 0)))
    taps = taps.reshape(kernel_len + 1, width // LANES, LANES).transpose(1, 0, 2)

    id_pad = jnp.pad(segment_ids, ((0, 0), (2 * EDGE, 2 * EDGE)), constant_values=-1)
    window = lax.dynamic_slice_in_dim(
        id_pad, lax.axis_index(SEQ) * frames_dev, frames_dev + 4 * EDGE, 1
    )
    ids = jnp.broadcast_to(window[:, :, None], (*window.shape, LANES))

    frame_rows = frames.astype(jnp.float32)
    _, pull_pre = jax.vjp(norm_rows, frame_rows, gain_pre)
    padded = frames_dev + 4 * EDGE
    normed_wide, normed, upstream_wide = kernel_call(
        norm_kernel,
        (
            jax.ShapeDtypeStruct((slabs, padded, width), jnp.bfloat16),
            jax.ShapeDtypeStruct((rows_dev, width), jnp.bfloat16),
            jax.ShapeDtypeStruct((slabs * (frames_dev + 2 * EDGE), width), jnp.bfloat16),
        ),
        [],
        rows_dev * width * 10,
        frames, low, high, upstream, gain_pre[None],
    )
    normed_other = lax.ppermute(normed, "core", swap)
    lin, sig, gated = project(normed_wide.reshape(-1, width), in_full)
    gated, normed_other = lax.optimization_barrier((gated, normed_other))
    gated = gated.reshape(slabs, padded, width)
    elements = rows_dev * width
    wide = frames_dev + 2 * EDGE
    blocks = width // LANES
    activated, normed_mid = kernel_call(
        forward_kernel,
        (
            jax.ShapeDtypeStruct((rows_dev, width), jnp.bfloat16),
            jax.ShapeDtypeStruct((slabs * wide, width + LANES), jnp.float32),
        ),
        [
            pltpu.VMEM((blocks, padded, LANES), jnp.float32),
            pltpu.VMEM((blocks, wide, LANES), jnp.float32),
        ],
        elements * 3 * kernel_len,
        gated, ids, taps, gain_mid[None],
    )
    act_other = lax.ppermute(activated, "core", swap)
    grad_mixing, grad_gain_mid = kernel_call(
        middle_kernel,
        (
            jax.ShapeDtypeStruct((slabs, wide, width), jnp.float32),
            jax.ShapeDtypeStruct((8, width), jnp.float32),
        ),
        [pltpu.VMEM((slabs * wide, width), jnp.float32)],
        2 * slabs * wide * width * width,
        normed_mid, upstream_wide, out_full, gain_mid[None],
    )

    def exchanged(part):
        return lax.all_to_all(
            part.reshape(n_z * n_seq, LANES // n_seq, part.shape[1]), ZXY, 0, 0, tiled=True
        )

    core_ref = core[None].astype(jnp.int32)
    out_part = weight_part(core_ref, activated, act_other, upstream_rows, upstream_other)
    out_parts = exchanged(out_part)
    out_sum = jnp.sum(out_parts.astype(jnp.float32), axis=0)
    projected = jnp.dot(activated, out_full, preferred_element_type=jnp.float32)
    encoded = (frame_rows + projected).astype(jnp.bfloat16).reshape(slabs, frames_dev, width)

    grad_hidden, grad_taps, grad_hidden_kept = kernel_call(
        backward_kernel,
        (
            jax.ShapeDtypeStruct((rows_dev, 2 * width), jnp.bfloat16),
            jax.ShapeDtypeStruct((kernel_len + 9, width), jnp.float32),
            pltpu.HBM((rows_dev, 2 * width), jnp.bfloat16),
        ),
        [
            pltpu.VMEM((blocks, wide, LANES), jnp.float32),
            pltpu.VMEM((blocks, kernel_len, 8, LANES), jnp.float32),
            pltpu.SemaphoreType.DMA((slabs,)),
        ],
        elements * 5 * kernel_len,
        grad_mixing, gated, ids, taps, lin, sig, grad_gain_mid,
        out_specs=(
            pl.BlockSpec(memory_space=pltpu.VMEM),
            pl.BlockSpec(memory_space=pltpu.VMEM),
            pl.BlockSpec(memory_space=pltpu.HBM),
        ),
    )
    hidden_other = lax.ppermute(grad_hidden, "core", swap)
    small_other = lax.ppermute(grad_taps, "core", swap)
    in_part = weight_part(
        core_ref, normed, normed_other, grad_hidden, hidden_other, grad_taps, small_other
    )
    in_parts = exchanged(in_part)
    grad_normed = lax.dot_general(
        grad_hidden_kept, in_full, (((1,), (1,)), ((), ())), preferred_element_type=jnp.float32
    )
    grad_rows, _ = pull_pre(grad_normed)
    grad_frames = (
        (upstream_rows.astype(jnp.float32) + grad_rows)
        .astype(jnp.bfloat16)
        .reshape(slabs, frames_dev, width)
    )
    share = LANES // n_seq
    start = lax.axis_index(SEQ) * share
    own_weight = lax.dynamic_slice_in_dim(in_weight, start, share, 0).astype(jnp.float32)
    own_gain = lax.dynamic_slice_in_dim(norm_gains, start, share, 0)[:, :1].astype(jnp.float32)
    total = kernel_call(
        functools.partial(
            total_kernel, tap=kernel_len, scale=1.0 / math.sqrt(devices * rows_dev)
        ),
        jax.ShapeDtypeStruct((n_seq, share, 3 * width + SMALL), jnp.bfloat16),
        [pltpu.VMEM((share, 2 * width + SMALL), jnp.float32)],
        in_parts.size,
        in_parts, out_sum, own_weight, own_gain,
    )
    final = lax.all_to_all(total, SEQ, 0, 0, tiled=True).reshape(LANES, -1)
    grad_in, grad_out, grad_kernel, grad_gains = kernel_call(
        finish_kernel,
        (
            jax.ShapeDtypeStruct((LANES, 2 * width), jnp.float32),
            jax.ShapeDtypeStruct((LANES, width), jnp.float32),
            jax.ShapeDtypeStruct((kernel_len, LANES), jnp.float32),
            jax.ShapeDtypeStruct((2, LANES), jnp.float32),
        ),
        [],
        LANES * width,
        final,
    )
    return encoded, grad_frames, grad_in, grad_out, grad_kernel.T, grad_gains.T


def solution(mesh):
    n_dp, n_seq = mesh.devices.shape
    side = math.isqrt(n_seq)
    split = Mesh(mesh.devices.reshape(n_dp // 2, 2, side, side), ("z", "core", "x", "y"))
    placed = (
        P((*DP, *SEQ), None),
        P(),
        P(DP, None),
        P(DP, None),
        P(DP, None),
        P(DP, None),
        P(DP, None),
        P(DP, SEQ, None),
    )
    return jax.shard_map(
        per_device,
        mesh=split,
        in_specs=placed,
        out_specs=(
            P(DP, SEQ, None),
            P(DP, SEQ, None),
            P(DP, None),
            P(DP, None),
            P(DP, None),
            P(DP, None),
        ),
        check_vma=False,
    )
```

```python
import functools
import math

import jax
import jax.numpy as jnp
from jax import lax
from jax.experimental import pallas as pl
from jax.experimental.pallas import tpu as pltpu
from jax.sharding import Mesh, PartitionSpec as P


DP = ("z", "core")
SEQ = ("x", "y")
ZXY = ("z", "x", "y")
EDGE = 16
LANES = 128
ROWS_STEP = 32
EPS = 1e-05
SMALL = LANES
VMEM_GRANT = 16 * 1024 * 1024


def forward_kernel(
    gated_ref, ids_ref, taps_ref, gain_ref,
    act_ref, normed_ref, pad_ref, mix_ref,
):
    slabs, padded, width = gated_ref.shape
    blocks = width // LANES
    taps_count = taps_ref.shape[1] - 1
    wide = padded - 2 * EDGE
    own = wide - 2 * EDGE
    shift = EDGE - taps_count // 2

    def one_slab(s, carry):
        for b in range(blocks):
            pad_ref[b] = gated_ref[s, :, b * LANES : (b + 1) * LANES].astype(jnp.float32)

        def conv_step(i, carry):
            row = pl.multiple_of((i // (blocks // 2)) * ROWS_STEP, ROWS_STEP)
            b = (i % (blocks // 2)) * 2
            center = ids_ref[s, pl.ds(row + EDGE, ROWS_STEP)]
            sums = [jnp.zeros((ROWS_STEP, LANES), jnp.float32) for _ in range(2)]
            for k in range(taps_count):
                same = ids_ref[s, pl.ds(row + k + shift, ROWS_STEP)] == center
                for j in range(2):
                    term = pad_ref[b + j, pl.ds(row + k + shift, ROWS_STEP)]
                    sums[j] = sums[j] + jnp.where(same, term, 0.0) * taps_ref[b + j, k : k + 1, :]
            for j in range(2):
                mix_ref[b + j, pl.ds(row, ROWS_STEP)] = sums[j]
            return carry

        lax.fori_loop(0, (wide // ROWS_STEP) * (blocks // 2), conv_step, 0)

        def row_step(i, own_rows):
            row = pl.multiple_of(i * 16, 16)
            out_row = pl.multiple_of(s * wide + i * 16, 16)
            mixing = jnp.concatenate([mix_ref[b, pl.ds(row, 16)] for b in range(blocks)], axis=1)
            centered = mixing - jnp.mean(mixing, axis=-1, keepdims=True)
            scale = lax.rsqrt(jnp.mean(centered * centered, axis=-1, keepdims=True) + EPS)
            normed = centered * scale
            if own_rows:
                act_row = pl.multiple_of(s * own + i * 16 - EDGE, 16)
                value = normed * gain_ref[0:1, :]
                act_ref[pl.ds(act_row, 16), :] = (value * jax.nn.sigmoid(value)).astype(
                    act_ref.dtype
                )
            normed_ref[pl.ds(out_row, 16), :width] = normed
            normed_ref[pl.ds(out_row, 16), width:] = jnp.broadcast_to(scale, (16, LANES))

        steps = wide // 16
        row_step(0, False)
        row_step(steps - 1, False)

        def own_step(i, carry):
            row_step(i + 1, True)
            return carry

        return lax.fori_loop(0, steps - 2, own_step, carry, unroll=4)

    lax.fori_loop(0, slabs, one_slab, 0)


def middle_kernel(
    normed_ref, upstream_ref, weight_ref, gain_ref,
    grad_mix_ref, grad_gain_ref, grad_act_ref,
):
    slabs, frames, width = grad_mix_ref.shape
    steps = frames // 16
    grad_act_ref[...] = lax.dot_general(
        upstream_ref[...],
        weight_ref[...],
        (((1,), (1,)), ((), ())),
        preferred_element_type=jnp.float32,
    )

    def row_step(i, total):
        row = pl.multiple_of(i * 16, 16)
        normed = normed_ref[pl.ds(row, 16), :width]
        scale = normed_ref[pl.ds(row, 16), width : width + 1]
        gain = gain_ref[0:1, :]
        value = normed * gain
        sig = jax.nn.sigmoid(value)
        grad_value = grad_act_ref[pl.ds(row, 16), :] * (sig * (1.0 + value * (1.0 - sig)))
        part = grad_value * normed
        at = i % steps
        own = jnp.logical_and(at > 0, at < steps - 1)
        total = total + jnp.where(own, part[0:8] + part[8:16], 0.0)
        grad_normed = grad_value * gain
        first = jnp.mean(grad_normed, axis=-1, keepdims=True)
        second = jnp.mean(grad_normed * normed, axis=-1, keepdims=True)
        grad_mix_ref[i // steps, pl.ds(pl.multiple_of((i % steps) * 16, 16), 16), :] = scale * (
            grad_normed - first - normed * second
        )
        return total

    grad_gain_ref[...] = lax.fori_loop(
        0, slabs * steps, row_step, jnp.zeros(grad_gain_ref.shape, jnp.float32), unroll=10
    )


def backward_kernel(
    grad_mix_ref, gated_ref, ids_ref, taps_ref, lin_ref, sig_ref, grad_gain_ref,
    grad_hidden_ref, grad_taps_ref, pad_ref, sum_ref,
):
    slabs, padded, width = gated_ref.shape
    frames = padded - 4 * EDGE
    blocks = width // LANES
    taps_count = taps_ref.shape[1] - 1
    half = taps_count // 2
    sum_ref[...] = jnp.zeros(sum_ref.shape, jnp.float32)

    def one_slab(s, carry):
        for b in range(blocks):
            pad_ref[b] = grad_mix_ref[s, :, b * LANES : (b + 1) * LANES]

        def conv_step(i, carry):
            row = pl.multiple_of((i // (blocks // 2)) * ROWS_STEP, ROWS_STEP)
            out_row = pl.multiple_of(s * frames + row, ROWS_STEP)
            b = (i % (blocks // 2)) * 2
            hid_row = pl.multiple_of(s * padded + 2 * EDGE + row, ROWS_STEP)
            center = ids_ref[s, pl.ds(row + 2 * EDGE, ROWS_STEP)]
            sums = [jnp.zeros((ROWS_STEP, LANES), jnp.float32) for _ in range(2)]
            cols = [pl.ds(pl.multiple_of((b + j) * LANES, LANES), LANES) for j in range(2)]
            here = [gated_ref[s, pl.ds(row + 2 * EDGE, ROWS_STEP), cols[j]].astype(jnp.float32) for j in range(2)]
            for k in range(taps_count):
                at = row + EDGE + half - k
                same = ids_ref[s, pl.ds(at + EDGE, ROWS_STEP)] == center
                for j in range(2):
                    term = jnp.where(same, pad_ref[b + j, pl.ds(at, ROWS_STEP)], 0.0)
                    sums[j] = sums[j] + term * taps_ref[b + j, k : k + 1, :]
                    part = term * here[j]
                    sum_ref[b + j, k] = sum_ref[b + j, k] + (
                        (part[0:8] + part[8:16]) + (part[16:24] + part[24:32])
                    )
            for j in range(2):
                lin = lin_ref[pl.ds(hid_row, ROWS_STEP), cols[j]]
                sig = sig_ref[pl.ds(hid_row, ROWS_STEP), cols[j]]
                grad_lin = sums[j] * sig
                grad_hidden_ref[pl.ds(out_row, ROWS_STEP), cols[j]] = grad_lin.astype(jnp.bfloat16)
                grad_hidden_ref[
                    pl.ds(out_row, ROWS_STEP),
                    pl.ds(pl.multiple_of(width + (b + j) * LANES, LANES), LANES),
                ] = (grad_lin * lin * (1.0 - sig)).astype(jnp.bfloat16)
            return carry

        return lax.fori_loop(0, (frames // ROWS_STEP) * (blocks // 2), conv_step, carry)

    lax.fori_loop(0, slabs, one_slab, 0)
    for b in range(blocks):
        for k in range(taps_count):
            grad_taps_ref[k : k + 1, b * LANES : (b + 1) * LANES] = jnp.sum(
                sum_ref[b, k], axis=0, keepdims=True
            )
    grad_taps_ref[taps_count:, :] = jnp.zeros(
        (grad_taps_ref.shape[0] - taps_count, width), jnp.float32
    )
    grad_taps_ref[taps_count + 1 : taps_count + 2, :] = jnp.sum(
        grad_gain_ref[...], axis=0, keepdims=True
    )


def send_kernel(index_ref, rows_ref, out_ref):
    rows, width = rows_ref.shape
    pick = (lax.broadcasted_iota(jnp.int32, (index_ref.shape[0], rows), 1) == index_ref[...])
    pick = pick.astype(jnp.float32).astype(jnp.bfloat16)
    for h in range(2):
        part = jnp.dot(
            pick,
            rows_ref[:, h * (width // 2) : (h + 1) * (width // 2)],
            preferred_element_type=jnp.float32,
        )
        slots = part.shape[0] // out_ref.shape[0]
        out_ref[:, h * slots : (h + 1) * slots, :] = part.astype(jnp.bfloat16).reshape(
            out_ref.shape[0], slots, width // 2
        )


def receive_kernel(index_ref, arrived_ref, upstream_ref, out_ref, last_ref, first_ref):
    slots, half = arrived_ref.shape
    slabs, frames, _ = upstream_ref.shape
    reach = 2 * EDGE
    columns = lax.broadcasted_iota(jnp.int32, (index_ref.shape[0], slots), 1)
    for h in range(2):
        pick = (columns == index_ref[:, h : h + 1]).astype(jnp.float32).astype(jnp.bfloat16)
        rows = jnp.dot(pick, arrived_ref[...], preferred_element_type=jnp.float32)
        rows = rows.astype(jnp.bfloat16)
        cols = slice(h * half, (h + 1) * half)
        out_ref[:, cols] = rows
        for s in range(slabs):
            last_ref[s, :reach, cols] = rows[(s + 1) * frames - reach : (s + 1) * frames]
            first_ref[s, :reach, cols] = rows[s * frames : s * frames + reach]
    for s in range(slabs):
        last_ref[s, reach:, :] = upstream_ref[s, frames - EDGE :, :]
        first_ref[s, reach:, :] = upstream_ref[s, :EDGE, :]


def total_kernel(parts_ref, out_sum_ref, weight_ref, gain_ref, total_ref, sum_ref, *, tap, scale):
    count, share, width = parts_ref.shape
    in_width = weight_ref.shape[1]
    grad_gain = jnp.zeros((share, 1), jnp.float32)
    for at in range(0, width, SMALL):
        cols = slice(at, at + SMALL)
        part = jnp.zeros((share, SMALL), jnp.float32)
        for j in range(0, count, 16):
            part = part + jnp.sum(parts_ref[j : j + 16, :, cols].astype(jnp.float32), axis=0)
        sum_ref[:, cols] = part
        if at < in_width:
            grad_gain = grad_gain + jnp.sum(part * weight_ref[:, cols], axis=1, keepdims=True)
    small = sum_ref[:, in_width:]
    column = lax.broadcasted_iota(jnp.int32, small.shape, 1)
    sum_ref[:, in_width:] = jnp.where(column == tap, grad_gain / gain_ref[...], small)
    for i in range(total_ref.shape[0]):
        total_ref[i, :, :width] = (sum_ref[...] * scale).astype(jnp.bfloat16)
        total_ref[i, :, width:] = (out_sum_ref[...] * scale).astype(jnp.bfloat16)


def finish_kernel(final_ref, grad_in_ref, grad_out_ref, grad_taps_ref, grad_gains_ref):
    in_width, taps_count = grad_in_ref.shape[1], grad_taps_ref.shape[0]
    grad_in_ref[...] = final_ref[:, :in_width].astype(jnp.float32)
    grad_out_ref[...] = final_ref[:, in_width + SMALL :].astype(jnp.float32)
    small = final_ref[:, in_width : in_width + LANES].astype(jnp.float32).T
    grad_taps_ref[...] = small[:taps_count]
    grad_gains_ref[...] = small[taps_count : taps_count + 2]


def product_kernel(core_ref, left_ref, left_other_ref, right_ref, right_other_ref, *rest):
    small_refs, out_ref, turned_ref = rest[:-2], rest[-2], rest[-1]
    rows, channels = left_ref.shape
    width = right_ref.shape[1]
    step = 1024
    picks = [
        pl.ds(pl.multiple_of((2 * z + core_ref[0]) * LANES, LANES), LANES)
        for z in range(channels // LANES // 2)
    ]
    for z, pick in enumerate(picks):
        for h, ref in enumerate((left_ref, left_other_ref)):
            turned_ref[z * LANES : (z + 1) * LANES, h * rows : (h + 1) * rows] = ref[:, pick].T
    for at in range(0, width, step):
        right = jnp.concatenate(
            [right_ref[:, at : at + step], right_other_ref[:, at : at + step]], axis=0
        )
        out_ref[:, at : at + step] = jnp.dot(
            turned_ref[...], right, preferred_element_type=jnp.float32
        ).astype(out_ref.dtype)
    if small_refs:
        for z, pick in enumerate(picks):
            small = small_refs[0][:, pick] + small_refs[1][:, pick]
            filled = jnp.concatenate(
                [small, jnp.zeros((LANES - small.shape[0], LANES), jnp.float32)], axis=0
            )
            block = slice(z * LANES, (z + 1) * LANES)
            out_ref[block, width : width + LANES] = filled.T.astype(out_ref.dtype)


def weight_part(core, left, left_other, right, right_other, *small):
    rows, channels = left.shape
    mine = channels // LANES // 2
    width = right.shape[1]
    out_width = width + (SMALL if small else 0)
    vmem = pl.BlockSpec(memory_space=pltpu.VMEM)
    return pl.pallas_call(
        product_kernel,
        out_shape=jax.ShapeDtypeStruct((mine * LANES, out_width), jnp.bfloat16),
        in_specs=[pl.BlockSpec(memory_space=pltpu.SMEM)] + [vmem] * (4 + len(small)),
        out_specs=vmem,
        scratch_shapes=[pltpu.VMEM((mine * LANES, 2 * rows), jnp.bfloat16)],
        name="weight_part",
        compiler_params=pltpu.CompilerParams(vmem_limit_bytes=VMEM_GRANT),
        cost_estimate=pl.CostEstimate(
            flops=4 * rows * mine * LANES * width,
            bytes_accessed=4 * rows * (channels + width),
            transcendentals=0,
        ),
    )(core, left, left_other, right, right_other, *small)


def norm_kernel(
    frames_ref, low_ref, high_ref, upstream_ref, gain_ref, wide_ref, own_ref, up_wide_ref
):
    slabs, padded, _ = wide_ref.shape
    reach = 2 * EDGE
    own = padded - 2 * reach

    def normed_rows(rows):
        values = rows.astype(jnp.float32)
        centered = values - jnp.mean(values, axis=-1, keepdims=True)
        spread_ = jnp.mean(centered * centered, axis=-1, keepdims=True)
        return (centered * lax.rsqrt(spread_ + EPS) * gain_ref[0:1, :]).astype(jnp.bfloat16)

    for s in range(slabs):
        for at in range(0, reach, 16):
            wide_ref[s, at : at + 16, :] = normed_rows(low_ref[s, at : at + 16, :])
            high_at = reach + own + at
            wide_ref[s, high_at : high_at + 16, :] = normed_rows(high_ref[s, at : at + 16, :])

    def step(i, carry):
        row = pl.multiple_of(i * 16, 16)
        rows = normed_rows(frames_ref[pl.ds(row, 16), :])
        own_ref[pl.ds(row, 16), :] = rows
        steps = own // 16
        wide_ref[i // steps, pl.ds(pl.multiple_of(reach + (i % steps) * 16, 16), 16), :] = rows
        return carry

    lax.fori_loop(0, slabs * own // 16, step, 0, unroll=4)
    for s in range(slabs):
        base = s * (own + 2 * EDGE)
        up_wide_ref[base : base + EDGE, :] = low_ref[s, reach:, :]
        up_wide_ref[base + EDGE : base + EDGE + own, :] = upstream_ref[s]
        up_wide_ref[base + EDGE + own : base + 2 * EDGE + own, :] = high_ref[s, reach:, :]


def project_kernel(normed_ref, lin_w_ref, gate_w_ref, lin_ref, sig_ref, gated_ref):
    lin = jnp.dot(normed_ref[...], lin_w_ref[...], preferred_element_type=jnp.float32)
    gate = jnp.dot(normed_ref[...], gate_w_ref[...], preferred_element_type=jnp.float32)
    sig = jax.nn.sigmoid(gate)
    lin_ref[...] = lin
    sig_ref[...] = sig
    gated_ref[...] = (lin * sig).astype(jnp.bfloat16)


def project(normed, weight):
    rows, width = normed.shape
    cols = 256
    steps = width // cols
    out = pl.BlockSpec((rows, cols), lambda j: (0, j))
    return pl.pallas_call(
        project_kernel,
        out_shape=(
            jax.ShapeDtypeStruct((rows, width), jnp.float32),
            jax.ShapeDtypeStruct((rows, width), jnp.float32),
            jax.ShapeDtypeStruct((rows, width), jnp.bfloat16),
        ),
        grid=(steps,),
        in_specs=[
            pl.BlockSpec((rows, width), lambda j: (0, 0)),
            pl.BlockSpec((width, cols), lambda j: (0, j)),
            pl.BlockSpec((width, cols), lambda j: (0, j + steps)),
        ],
        out_specs=(out, out, out),
        name="project",
        compiler_params=pltpu.CompilerParams(vmem_limit_bytes=VMEM_GRANT),
        cost_estimate=pl.CostEstimate(
            flops=4 * rows * width * width,
            bytes_accessed=4 * width * width,
            transcendentals=rows * width,
        ),
    )(normed, weight, weight)


def kernel_call(body, outs, scratch, flops, *args):
    moved = sum(a.size * a.dtype.itemsize for a in args)
    return pl.pallas_call(
        body,
        out_shape=outs,
        scratch_shapes=scratch,
        compiler_params=pltpu.CompilerParams(vmem_limit_bytes=VMEM_GRANT),
        cost_estimate=pl.CostEstimate(flops=flops, bytes_accessed=moved, transcendentals=0),
    )(*args)


def to_neighbours(last, first, count):
    forward = [(i, i + 1) for i in range(count - 1)]
    backward = [(i + 1, i) for i in range(count - 1)]
    return lax.ppermute(last, SEQ, forward), lax.ppermute(first, SEQ, backward)


def norm_rows(values, gain):
    average = jnp.mean(values, axis=-1, keepdims=True)
    centered = values - average
    spread_ = jnp.mean(centered * centered, axis=-1, keepdims=True)
    return centered * lax.rsqrt(spread_ + EPS) * gain


def per_device(
    loaded, plan, segment_ids, in_weight, out_weight, depth_kernel, norm_gains, upstream
):
    rows_dev, width = loaded.shape
    devices = plan.shape[0]
    capacity = 2 * rows_dev // devices
    slabs, slab_len = segment_ids.shape
    n_seq = lax.axis_size(SEQ)
    n_z = lax.axis_size("z")
    frames_dev = slab_len // n_seq
    kernel_len = depth_kernel.shape[1]
    core = lax.axis_index("core")
    sender = lax.axis_index((*DP, *SEQ))
    swap = [(0, 1), (1, 0)]

    in_full = lax.all_gather(in_weight, DP, axis=0, tiled=True)
    out_full = lax.all_gather(out_weight, DP, axis=0, tiled=True)

    send_plan = lax.dynamic_index_in_dim(plan, sender, 0, keepdims=False)
    send_start = jnp.cumsum(send_plan) - send_plan
    slot_index = jnp.arange(capacity, dtype=jnp.int32)
    source_rows = jnp.minimum(send_start[:, None] + slot_index[None, :], rows_dev - 1)
    outgoing = kernel_call(
        send_kernel,
        jax.ShapeDtypeStruct((devices, 2 * capacity, width // 2), jnp.bfloat16),
        [],
        4 * devices * capacity * rows_dev * width,
        source_rows.reshape(-1, 1), loaded,
    )
    arrived = lax.all_to_all(
        outgoing, (*DP, *SEQ), split_axis=0, concat_axis=0, tiled=True
    ).reshape(devices * 2 * capacity, width // 2)
    extras = jnp.pad(
        jnp.concatenate([depth_kernel, norm_gains], axis=1), ((0, 0), (0, LANES - kernel_len - 2))
    )
    upstream_rows = upstream.reshape(rows_dev, width)
    extras_other = lax.ppermute(extras, "core", swap)
    pair = jnp.where(
        core == 0, jnp.stack([extras, extras_other]), jnp.stack([extras_other, extras])
    )
    from_z = [
        lax.ppermute(pair, "z", [(i, (i + d) % n_z) for i in range(n_z)])
        for d in range(1, n_z)
    ]
    upstream_other = lax.ppermute(upstream_rows, "core", swap)
    arrived, upstream_other, pair = lax.optimization_barrier((arrived, upstream_other, pair))
    by_z = jnp.stack([*from_z[::-1], pair])
    side_all = lax.dynamic_slice_in_dim(
        jnp.concatenate([by_z, by_z]), n_z - 1 - lax.axis_index("z"), n_z, 0
    )
    recv_plan = lax.dynamic_index_in_dim(plan, sender, 1, keepdims=False)
    recv_end = jnp.cumsum(recv_plan)
    frame_index = jnp.arange(rows_dev, dtype=jnp.int32)
    before = recv_end[None, :] <= frame_index[:, None]
    source_dev = jnp.sum(before.astype(jnp.int32), axis=1)
    start_of = jnp.sum(jnp.where(before, recv_plan[None, :], 0), axis=1)
    place = source_dev * 2 * capacity + frame_index - start_of
    frames, last, first = kernel_call(
        receive_kernel,
        (
            jax.ShapeDtypeStruct((rows_dev, width), jnp.bfloat16),
            jax.ShapeDtypeStruct((slabs, 3 * EDGE, width), jnp.bfloat16),
            jax.ShapeDtypeStruct((slabs, 3 * EDGE, width), jnp.bfloat16),
        ),
        [],
        4 * devices * capacity * rows_dev * width,
        jnp.stack([place, place + capacity], axis=1), arrived, upstream,
    )
    low, high = to_neighbours(last, first, n_seq)
    side = side_all.reshape(width, LANES)[:, : kernel_len + 2].astype(jnp.float32).T
    gain_pre, gain_mid = side[kernel_len], side[kernel_len + 1]
    taps = jnp.pad(side[:kernel_len], ((0, 1), (0, 0)))
    taps = taps.reshape(kernel_len + 1, width // LANES, LANES).transpose(1, 0, 2)

    id_pad = jnp.pad(segment_ids, ((0, 0), (2 * EDGE, 2 * EDGE)), constant_values=-1)
    window = lax.dynamic_slice_in_dim(
        id_pad, lax.axis_index(SEQ) * frames_dev, frames_dev + 4 * EDGE, 1
    )
    ids = jnp.broadcast_to(window[:, :, None], (*window.shape, LANES))

    frame_rows = frames.astype(jnp.float32)
    _, pull_pre = jax.vjp(norm_rows, frame_rows, gain_pre)
    padded = frames_dev + 4 * EDGE
    normed_wide, normed, upstream_wide = kernel_call(
        norm_kernel,
        (
            jax.ShapeDtypeStruct((slabs, padded, width), jnp.bfloat16),
            jax.ShapeDtypeStruct((rows_dev, width), jnp.bfloat16),
            jax.ShapeDtypeStruct((slabs * (frames_dev + 2 * EDGE), width), jnp.bfloat16),
        ),
        [],
        rows_dev * width * 10,
        frames, low, high, upstream, gain_pre[None],
    )
    normed_other = lax.ppermute(normed, "core", swap)
    lin, sig, gated = project(normed_wide.reshape(-1, width), in_full)
    gated, normed_other = lax.optimization_barrier((gated, normed_other))
    gated = gated.reshape(slabs, padded, width)
    elements = rows_dev * width
    wide = frames_dev + 2 * EDGE
    blocks = width // LANES
    activated, normed_mid = kernel_call(
        forward_kernel,
        (
            jax.ShapeDtypeStruct((rows_dev, width), jnp.bfloat16),
            jax.ShapeDtypeStruct((slabs * wide, width + LANES), jnp.float32),
        ),
        [
            pltpu.VMEM((blocks, padded, LANES), jnp.float32),
            pltpu.VMEM((blocks, wide, LANES), jnp.float32),
        ],
        elements * 3 * kernel_len,
        gated, ids, taps, gain_mid[None],
    )
    act_other = lax.ppermute(activated, "core", swap)
    grad_mixing, grad_gain_mid = kernel_call(
        middle_kernel,
        (
            jax.ShapeDtypeStruct((slabs, wide, width), jnp.float32),
            jax.ShapeDtypeStruct((8, width), jnp.float32),
        ),
        [pltpu.VMEM((slabs * wide, width), jnp.float32)],
        2 * slabs * wide * width * width,
        normed_mid, upstream_wide, out_full, gain_mid[None],
    )

    def exchanged(part):
        return lax.all_to_all(
            part.reshape(n_z * n_seq, LANES // n_seq, part.shape[1]), ZXY, 0, 0, tiled=True
        )

    core_ref = core[None].astype(jnp.int32)
    out_part = weight_part(core_ref, activated, act_other, upstream_rows, upstream_other)
    out_parts = exchanged(out_part)
    out_sum = jnp.sum(out_parts.astype(jnp.float32), axis=0)
    projected = jnp.dot(activated, out_full, preferred_element_type=jnp.float32)
    encoded = (frame_rows + projected).astype(jnp.bfloat16).reshape(slabs, frames_dev, width)

    grad_hidden, grad_taps = kernel_call(
        backward_kernel,
        (
            jax.ShapeDtypeStruct((rows_dev, 2 * width), jnp.bfloat16),
            jax.ShapeDtypeStruct((kernel_len + 9, width), jnp.float32),
        ),
        [
            pltpu.VMEM((blocks, wide, LANES), jnp.float32),
            pltpu.VMEM((blocks, kernel_len, 8, LANES), jnp.float32),
        ],
        elements * 5 * kernel_len,
        grad_mixing, gated, ids, taps, lin, sig, grad_gain_mid,
    )
    hidden_other = lax.ppermute(grad_hidden, "core", swap)
    small_other = lax.ppermute(grad_taps, "core", swap)
    in_part = weight_part(
        core_ref, normed, normed_other, grad_hidden, hidden_other, grad_taps, small_other
    )
    in_parts = exchanged(in_part)
    grad_normed = lax.dot_general(
        grad_hidden, in_full, (((1,), (1,)), ((), ())), preferred_element_type=jnp.float32
    )
    grad_rows, _ = pull_pre(grad_normed)
    grad_frames = (
        (upstream_rows.astype(jnp.float32) + grad_rows)
        .astype(jnp.bfloat16)
        .reshape(slabs, frames_dev, width)
    )
    share = LANES // n_seq
    start = lax.axis_index(SEQ) * share
    own_weight = lax.dynamic_slice_in_dim(in_weight, start, share, 0).astype(jnp.float32)
    own_gain = lax.dynamic_slice_in_dim(norm_gains, start, share, 0)[:, :1].astype(jnp.float32)
    total = kernel_call(
        functools.partial(
            total_kernel, tap=kernel_len, scale=1.0 / math.sqrt(devices * rows_dev)
        ),
        jax.ShapeDtypeStruct((n_seq, share, 3 * width + SMALL), jnp.bfloat16),
        [pltpu.VMEM((share, 2 * width + SMALL), jnp.float32)],
        in_parts.size,
        in_parts, out_sum, own_weight, own_gain,
    )
    final = lax.all_to_all(total, SEQ, 0, 0, tiled=True).reshape(LANES, -1)
    grad_in, grad_out, grad_kernel, grad_gains = kernel_call(
        finish_kernel,
        (
            jax.ShapeDtypeStruct((LANES, 2 * width), jnp.float32),
            jax.ShapeDtypeStruct((LANES, width), jnp.float32),
            jax.ShapeDtypeStruct((kernel_len, LANES), jnp.float32),
            jax.ShapeDtypeStruct((2, LANES), jnp.float32),
        ),
        [],
        LANES * width,
        final,
    )
    return encoded, grad_frames, grad_in, grad_out, grad_kernel.T, grad_gains.T


def solution(mesh):
    n_dp, n_seq = mesh.devices.shape
    side = math.isqrt(n_seq)
    split = Mesh(mesh.devices.reshape(n_dp // 2, 2, side, side), ("z", "core", "x", "y"))
    placed = (
        P((*DP, *SEQ), None),
        P(),
        P(DP, None),
        P(DP, None),
        P(DP, None),
        P(DP, None),
        P(DP, None),
        P(DP, SEQ, None),
    )
    return jax.shard_map(
        per_device,
        mesh=split,
        in_specs=placed,
        out_specs=(
            P(DP, SEQ, None),
            P(DP, SEQ, None),
            P(DP, None),
            P(DP, None),
            P(DP, None),
            P(DP, None),
        ),
        check_vma=False,
    )
```
